32 devices in a mesh: gx: 4 (over y, core), gy: 8 (over z, x).
Axes of the slice: x: 2, y: 2, z: 4, core: 2. Of those that a mesh axis runs over, the one named last changes fastest.
Arguments:
- forcing: float32 [16, 256, 1024], P(None, 'gy', 'gx'), may hold values from -6 to 6
- damping: float32 [16, 256, 1024], P(None, 'gy', 'gx'), may hold values from 0.5 to 4
- coupling: float32 [16, 16], replicated, may hold values from -1.5 to 1.5
- wind_lon: float32 [256, 1024], P('gy', 'gx'), may hold values from -0.5 to 0.5
- wind_lat: float32 [256, 1024], P('gy', 'gx'), may hold values from -0.5 to 0.5
Outputs:
- solution: float32 [16, 256, 1024], P(None, 'gy', 'gx')
- residual: float32 [16, 256, 1024], P(None, 'gy', 'gx')
The draws below stay inside these ranges and needn't reach their ends.
All inputs are finite; a program needn't handle non-finite values.
Results may differ from the reference program's by a relative error of at most 0.0003.
Values sent between devices are 32-bit elements; how exact they have to be, the bound alone decides.
A program may use at most 64 MiB of HBM per device.

```python
import math
import jax
import jax.numpy as jnp
from jax import lax

CH = 16
ITERS = 8
NLAT = 256
NLON = 1024


def block_scale(stream_key, dims, cuts, smallest, high):
    def one(position, parts):
        steps = jax.random.uniform(jax.random.fold_in(jax.random.fold_in(stream_key, 6), position), (parts,), jnp.float32, smallest / len(cuts), high / len(cuts))
        return jnp.repeat(jnp.exp(steps), dims[position] // parts).reshape((-1,) + (1,) * (len(dims) - position - 1))

    factor_of = one(*cuts[0])
    for cut in cuts[1:]:
        factor_of = factor_of * one(*cut)
    return factor_of


def scatter_about(own_key, extent, scale, limit, pieces=(), held_as=jnp.bfloat16):
    factor_of = block_scale(own_key, extent, pieces, -0.22, 0.18) if pieces else 1.0
    drawn = jax.random.normal(own_key, extent, jnp.float32) * scale * factor_of
    return jnp.minimum(jnp.maximum(drawn, -limit), limit).astype(held_as)


def setup_inputs(seed: int = 0) -> dict:
    seeds = jax.random.split(jax.random.key(seed), 6)
    return {
        "forcing": scatter_about(seeds[0], (CH, NLAT, NLON), 1.0, 6.0, ((1, 8), (2, 4)), jnp.float32),
        "damping": jnp.clip(jnp.exp(math.log(4.0) - 2.0794415 * jax.random.uniform(seeds[1], (CH, NLAT, NLON), jnp.float32) ** block_scale(seeds[1], (CH, NLAT, NLON), ((1, 8), (2, 4)), -0.2, 0.2)), 0.5, 4.0),
        "coupling": scatter_about(seeds[2], (CH, CH), CH ** -0.5, 1.5, (), jnp.float32),
        "wind_lon": jnp.clip(jax.random.uniform(seeds[3], (NLAT, NLON), jnp.float32, -0.5, 0.5) * block_scale(seeds[3], (NLAT, NLON), ((0, 8), (1, 4)), -0.4, 0.0), -0.5, 0.5),
        "wind_lat": jnp.clip(jax.random.uniform(seeds[4], (NLAT, NLON), jnp.float32, -0.5, 0.5) * block_scale(seeds[4], (NLAT, NLON), ((0, 8), (1, 4)), -0.4, 0.0), -0.5, 0.5),
    }


COUPLE = 0.25
DIFF_LAT = 0.5
DIFF_LON = 0.5
GUARD = 1.0

def apply_core(padded, damping, coupling, wind_lon, wind_lat, diffuse_lon):
    centre = padded[:, 2:-2, 2:-2]
    east_one = padded[:, 2:-2, 3:-1]
    west_one = padded[:, 2:-2, 1:-3]
    east_two = padded[:, 2:-2, 4:]
    west_two = padded[:, 2:-2, :-4]
    north_one = padded[:, 3:-1, 2:-2]
    south_one = padded[:, 1:-3, 2:-2]
    north_two = padded[:, 4:, 2:-2]
    south_two = padded[:, :-4, 2:-2]
    slope_lon = (8.0 * (east_one - west_one) - (east_two - west_two)) / 12.0
    slope_lat = (8.0 * (north_one - south_one) - (north_two - south_two)) / 12.0
    coupled = COUPLE * jnp.einsum('ij,jab->iab', coupling, centre, precision=lax.Precision.HIGHEST)
    return (1.0 + damping) * centre + coupled + diffuse_lon * (2.0 * centre - east_one - west_one) + DIFF_LAT * (2.0 * centre - north_one - south_one) + wind_lon * slope_lon + wind_lat * slope_lat

def lon_diffusion(row_pos, lat_total):
    phi = -math.pi / 2 + (row_pos + 0.5) * (math.pi / lat_total)
    return DIFF_LON / (jnp.cos(phi) ** 2 + 0.1)

def operate(source, damping, coupling, wind_lon, wind_lat):
    padded = jnp.pad(source, ((0, 0), (2, 2), (0, 0)))
    padded = jnp.concatenate([padded[:, :, -2:], padded, padded[:, :, :2]], axis=2)
    row_pos = jnp.arange(NLAT).astype(jnp.float32)
    diffuse = lon_diffusion(row_pos, NLAT)[:, None]
    return apply_core(padded, damping, coupling, wind_lon, wind_lat, diffuse)

def least_squares(heights, first):
    num_steps = heights.shape[1]
    target = jnp.zeros((num_steps + 1,), jnp.float32).at[0].set(first)
    rotated = heights
    cosines = []
    sines = []
    for column in range(num_steps):
        column_vec = rotated[:, column]
        for earlier in range(column):
            upper_val = column_vec[earlier]
            lower_val = column_vec[earlier + 1]
            column_vec = column_vec.at[earlier].set(cosines[earlier] * upper_val + sines[earlier] * lower_val)
            column_vec = column_vec.at[earlier + 1].set(-sines[earlier] * upper_val + cosines[earlier] * lower_val)
        upper_val = column_vec[column]
        lower_val = column_vec[column + 1]
        radius = jnp.sqrt(upper_val * upper_val + lower_val * lower_val)
        cosine = upper_val / radius
        sine_val = lower_val / radius
        column_vec = column_vec.at[column].set(radius).at[column + 1].set(0.0)
        rotated = rotated.at[:, column].set(column_vec)
        upper_val = target[column]
        lower_val = target[column + 1]
        target = target.at[column].set(cosine * upper_val + sine_val * lower_val)
        target = target.at[column + 1].set(-sine_val * upper_val + cosine * lower_val)
        cosines.append(cosine)
        sines.append(sine_val)
    weights = [None] * num_steps
    for column in reversed(range(num_steps)):
        partial_value = target[column]
        for later_col in range(column + 1, num_steps):
            partial_value = partial_value - rotated[column, later_col] * weights[later_col]
        weights[column] = partial_value / rotated[column, column]
    return weights

def reference(forcing, damping, coupling, wind_lon, wind_lat):
    scale_first = jnp.sqrt(jnp.sum(forcing * forcing) + GUARD)
    krylov = [forcing / scale_first]
    heights = jnp.zeros((ITERS + 1, ITERS), jnp.float32)
    for column in range(ITERS):
        applied = operate(krylov[column], damping, coupling, wind_lon, wind_lat)
        coeffs = jnp.stack([jnp.sum(vector * applied) for vector in krylov])
        for earlier in range(len(krylov)):
            applied = applied - coeffs[earlier] * krylov[earlier]
        subdiag = jnp.sqrt(jnp.sum(applied * applied) + GUARD)
        heights = heights.at[:column + 1, column].set(coeffs).at[column + 1, column].set(subdiag)
        if column + 1 < ITERS:
            krylov.append(applied / subdiag)
    weights = least_squares(heights, scale_first)
    solution = weights[0] * krylov[0]
    for column in range(1, ITERS):
        solution = solution + weights[column] * krylov[column]
    residual = forcing - operate(solution, damping, coupling, wind_lon, wind_lat)
    return (solution, residual)
```

```python
import functools
import math

import jax
import jax.numpy as jnp
from jax import lax
from jax.experimental import pallas as pl
from jax.experimental.pallas import tpu as pltpu
from jax.sharding import PartitionSpec as P

ITERS = 8
COUPLE = 0.25
DIFF_LAT = 0.5
DIFF_LON = 0.5
GUARD = 1.0
MESH = pl.DeviceIdType.MESH
HI = lax.Precision.HIGHEST

MIDDLE = 9.0
RADIUS = 6.0
WIDTH = 3.0
THETA = [MIDDLE + RADIUS * math.cos(math.pi * (2 * k + 1) / (2 * ITERS)) for k in (7, 0, 4, 2, 6, 1, 5, 3)]
PAIRS = [(k, i) for k in range(ITERS + 1) for i in range(k + 1)]
GROUP = 4
HALO = 4
BLOCKS = ITERS // 2


def apply_to(coords):
    out = [None] * (len(coords) + 1)
    for k, value in enumerate(coords):
        low = THETA[k] * value if k < ITERS else value
        out[k] = low if out[k] is None else out[k] + low
        out[k + 1] = WIDTH * value
    return out


def small_solve(gram):
    first = jnp.sqrt(gram[0][0] + GUARD)
    coords = [[1.0 / first]]
    images = [[gram[i][0] * coords[0][0] for i in range(ITERS + 1)]]
    heights = []
    for j in range(ITERS):
        moved = apply_to(coords[j])
        column = []
        for i in range(j + 1):
            column.append(functools.reduce(lambda a, b: a + b, [images[i][k] * moved[k] for k in range(j + 2)]))
        left = list(moved)
        for i in range(j + 1):
            for k in range(i + 1):
                left[k] = left[k] - column[i] * coords[i][k]
        image = [
            functools.reduce(lambda a, b: a + b, [gram[r][k] * left[k] for k in range(j + 2)])
            for r in range(ITERS + 1)
        ]
        norm_sq = functools.reduce(lambda a, b: a + b, [image[k] * left[k] for k in range(j + 2)])
        subdiag = jnp.sqrt(jnp.maximum(norm_sq, 0.0) + GUARD)
        column.append(subdiag)
        heights.append(column)
        inverse = 1.0 / subdiag
        coords.append([v * inverse for v in left])
        images.append([v * inverse for v in image])
    cosines, sines, target, rotated = [], [], [first], []
    for j in range(ITERS):
        column = list(heights[j])
        for e in range(j):
            upper, lower = column[e], column[e + 1]
            column[e] = cosines[e] * upper + sines[e] * lower
            column[e + 1] = cosines[e] * lower - sines[e] * upper
        upper, lower = column[j], column[j + 1]
        radius = jnp.sqrt(upper * upper + lower * lower)
        inverse = 1.0 / radius
        cosine, sine = upper * inverse, lower * inverse
        column[j] = radius
        kept = target[j]
        target[j] = cosine * kept
        target.append(-sine * kept)
        cosines.append(cosine)
        sines.append(sine)
        rotated.append(column)
    weights = [None] * ITERS
    for j in reversed(range(ITERS)):
        value = target[j]
        for later in range(j + 1, ITERS):
            value = value - rotated[later][j] * weights[later]
        weights[j] = value / rotated[j][j]
    answer = [None] * ITERS
    for j in range(ITERS):
        for k in range(j + 1):
            term = weights[j] * coords[j][k]
            answer[k] = term if answer[k] is None else answer[k] + term
    return answer, apply_to(answer)


def kernel(nx, ny, f_hbm, d_hbm, c_ref, wl_hbm, wa_hbm, basis, splats,
           diag, coef, block, single, side_in, side_out, band, fixed_in, fixed_out, corner_in, corner_out,
           gram_acc, mine, slots, wl_ref, wa_ref,
           in_sem, wind_sem, lat_send, lat_recv, lon_send, lon_recv, turn_send, turn_recv, fix_send, fix_recv, red_send, red_recv):
    channels, lat, lon = f_hbm.shape
    tiles = lon // 128
    total = nx * ny
    ix, iy = lax.axis_index("gx"), lax.axis_index("gy")
    me = ix * ny + iy
    east, west = lax.rem(ix + 1, nx), lax.rem(ix + nx - 1, nx)

    winds = [pltpu.make_async_copy(wl_hbm, wl_ref, wind_sem.at[0]), pltpu.make_async_copy(wa_hbm, wa_ref, wind_sem.at[1])]
    for copy in winds:
        copy.start()
    loads = []
    for q, (src, dst, off) in enumerate(((f_hbm, basis.at[0], HALO), (d_hbm, diag, 2))):
        for c in range(channels):
            copy = pltpu.make_async_copy(src.at[c], dst.at[pl.ds(off, lat), c, :], in_sem.at[q, c])
            copy.start()
            loads.append(copy)

    barrier = pltpu.get_barrier_semaphore()

    def greet(o, _):
        other = lax.rem(me + o, total)
        pl.semaphore_signal(barrier, inc=1, device_id=(other // ny, lax.rem(other, ny)), device_id_type=MESH)
        return 0

    lax.fori_loop(1, total, greet, 0)

    scale = 1.0 / WIDTH
    size = GROUP * channels

    def spread(n):
        row = lax.broadcasted_iota(jnp.int32, (n, channels), 0)
        col = lax.broadcasted_iota(jnp.int32, (n, channels), 1)
        return jnp.where(lax.rem(row, channels) == col, 1.0, 0.0).astype(jnp.float32)

    def widen(tall, n):
        wide = lax.dot_general(tall, spread(3 * n), (((1,), (1,)), ((), ())), precision=HI,
                               preferred_element_type=jnp.float32) * (COUPLE * scale)
        across = lax.broadcasted_iota(jnp.int32, wide.shape, 1)
        high = wide.astype(jnp.bfloat16).astype(jnp.float32)
        return jnp.where(across < 2 * n, high, wide - high), across

    single[...] = widen(c_ref[...], channels)[0].astype(jnp.bfloat16)
    tall = lax.dot_general(spread(size), c_ref[...], (((1,), (0,)), ((), ())), precision=HI,
                           preferred_element_type=jnp.float32)
    wide, across = widen(tall, size)
    down = lax.broadcasted_iota(jnp.int32, (size, 3 * size), 0)
    block[...] = jnp.where(down // channels == lax.rem(across, size) // channels, wide, 0.0).astype(jnp.bfloat16)

    def blank(at):
        for b in range(BLOCKS):
            basis[2 * b, pl.ds(HALO + lat if at else 0, HALO)] = jnp.zeros((HALO, channels, lon), jnp.float32)
        diag[pl.ds(lat + 2 if at else 0, 2)] = jnp.zeros((2, channels, lon), jnp.float32)
        coef[pl.ds(lat + 2 if at else 0, 2)] = jnp.zeros((2, 8, lon), jnp.float32)
        corner_in[:, 0 if at else 2] = jnp.zeros((BLOCKS, 2, 128), jnp.float32)
        corner_in[:, 1 if at else 3] = jnp.zeros((BLOCKS, 2, 128), jnp.float32)

    @pl.when(iy == 0)
    def _():
        blank(0)

    @pl.when(iy == ny - 1)
    def _():
        blank(1)

    for copy in winds:
        copy.wait()
    place = (lax.broadcasted_iota(jnp.int32, (lat, 128), 0) + iy * lat).astype(jnp.float32)
    phi = -math.pi / 2 + (place + 0.5) * (math.pi / (lat * ny))
    kx = (DIFF_LON * scale) / (jnp.cos(phi) ** 2 + 0.1)
    wl = wl_ref[...] * (scale / 12.0)
    wa = wa_ref[...] * (scale / 12.0)
    kx = jnp.concatenate([kx] * tiles, axis=1)
    planes = (8.0 * wl - kx, -8.0 * wl - kx, wl, 8.0 * wa - DIFF_LAT * scale, -8.0 * wa - DIFF_LAT * scale, wa,
              2.0 * kx + (1.0 + 2.0 * DIFF_LAT) * scale)
    for q, plane in enumerate(planes + (jnp.zeros_like(kx),)):
        for r in range(lat):
            coef[r + 2, q:q + 1, :] = plane[r:r + 1, :]

    for copy in loads:
        copy.wait()

    def prepare(r, _):
        diag[r + 2] = diag[r + 2] * scale + coef[r + 2, 6:7, :]
        return 0

    lax.fori_loop(0, lat, prepare, 0)

    def pack(read, far, n):
        lane = lax.broadcasted_iota(jnp.int32, (n, 128), 1)
        to_west = to_east = jnp.zeros((n, 128), jnp.float32)
        for r in range(lat):
            head = read(r, slice(0, 128))
            tail = read(r, slice(lon - 128, lon))
            here = (lane >= 2 * r) & (lane < 2 * r + 2)
            to_west = jnp.where(here, pltpu.roll(head, 2 * r, 1) if r else head, to_west)
            to_east = jnp.where(here, pltpu.roll(tail, (2 * r + 2) % 128, 1), to_east)
            if far:
                here = (lane >= 64 + 2 * r) & (lane < 64 + 2 * r + 2)
                to_west = jnp.where(here, pltpu.roll(head, (62 + 2 * r) % 128, 1), to_west)
                to_east = jnp.where(here, pltpu.roll(tail, (68 + 2 * r) % 128, 1), to_east)
        return to_west, to_east

    fixed = [pack(lambda r, cut: diag[r + 2, :, cut], False, channels), pack(lambda r, cut: coef[r + 2, :, cut], False, 8)]
    for way in range(2):
        fixed_out[way, 0:channels, :] = fixed[0][way]
        fixed_out[way, channels:channels + 8, :] = fixed[1][way]

    lane = lax.broadcasted_iota(jnp.int32, (channels, 128), 1)
    spot = lax.broadcasted_iota(jnp.int32, (8, 128), 1)
    deep = lax.broadcasted_iota(jnp.int32, (8, 128), 0)

    def copy_to(src, dst, send, recv, to):
        return pltpu.make_async_remote_copy(src_ref=src, dst_ref=dst, send_sem=send, recv_sem=recv,
                                            device_id=to, device_id_type=MESH)

    def lat_to(way):
        return iy + 1 if way else iy - 1

    def lat_copy(b, way):
        src = pl.ds(lat, HALO) if way else pl.ds(HALO, HALO)
        dst = pl.ds(0, HALO) if way else pl.ds(lat + HALO, HALO)
        return copy_to(basis.at[2 * b, src], basis.at[2 * b, dst], lat_send.at[b, way], lat_recv.at[b, way], (ix, lat_to(way)))

    def fix_copies(way):
        src = pl.ds(lat, 2) if way else pl.ds(2, 2)
        dst = pl.ds(0, 2) if way else pl.ds(lat + 2, 2)
        return [copy_to(ref.at[src], ref.at[dst], fix_send.at[n, way], fix_recv.at[n, way], (ix, lat_to(way)))
                for n, ref in enumerate((diag, coef))]

    def fix_side(way):
        return copy_to(fixed_out.at[way], fixed_in.at[way], fix_send.at[2, way], fix_recv.at[2, way],
                       (east if way else west, iy))

    def lon_copy(b, way):
        return copy_to(side_out.at[b, way], side_in.at[b, way], lon_send.at[b, way], lon_recv.at[b, way],
                       (east if way else west, iy))

    def turn_copy(b, up, way):
        n = 2 * up + way
        return copy_to(corner_out.at[b], corner_in.at[b, n], turn_send.at[b, n], turn_recv.at[b, n],
                       (east if way else west, lat_to(up)))

    def each_lat(act):
        @pl.when(iy < ny - 1)
        def _():
            act(1)

        @pl.when(iy > 0)
        def _():
            act(0)

    def arrive_lat(act):
        @pl.when(iy > 0)
        def _():
            act(1)

        @pl.when(iy < ny - 1)
        def _():
            act(0)

    def send_side(b):
        k = 2 * b
        to_west, to_east = pack(lambda r, cut: basis[k, r + HALO, :, cut], True, channels)
        side_out[b, 0] = to_west
        side_out[b, 1] = to_east
        lon_copy(b, 0).start()
        lon_copy(b, 1).start()
        small = jnp.zeros((8, 128), jnp.float32)
        for up in range(2):
            for way, ref in enumerate((to_west, to_east)):
                for h in range(channels // 8):
                    at = 16 * up + 8 * way + 4 * h
                    here = (spot >= at) & (spot < at + 4)
                    start = 2 * lat - 4 if up else 0
                    part = ref[8 * h:8 * h + 8, :]
                    small = jnp.where(here, pltpu.roll(part, (at - start) % 128, 1) if at != start else part, small)
        dense = small
        for g in range(1, 4):
            moved = pltpu.roll(pltpu.roll(small, 8 - 2 * g, 0), 32 * g, 1)
            dense = jnp.where(spot // 32 == g, moved, dense)
        corner_out[b] = dense[0:2, :]

        def go(up):
            turn_copy(b, up, 0).start()
            turn_copy(b, up, 1).start()

        each_lat(go)

    def take_corners(b):
        got = jnp.zeros((2, 128), jnp.float32)
        sub = lax.rem(lax.broadcasted_iota(jnp.int32, (2, 128), 1), 32) // 8
        for n in range(4):
            got = jnp.where(sub == n, corner_in[b, n], got)
        got = jnp.concatenate([got] * 4, axis=0)
        small = got
        for g in range(1, 4):
            small = jnp.where(deep // 2 == g, pltpu.roll(got, 128 - 32 * g, 1), small)
        parts = []
        for h in range(channels // 8):
            part = jnp.zeros((8, 128), jnp.float32)
            for up in range(2):
                for way in range(2):
                    at = 16 * up + 8 * way + 4 * h
                    want = (64 if way else 0) + (2 * lat - 4 if up else 0)
                    here = (spot >= want) & (spot < want + 4)
                    part = jnp.where(here, pltpu.roll(small, (want - at) % 128, 1) if want != at else small, part)
            parts.append(part)
        return jnp.concatenate(parts, axis=0)

    def theta_of(k):
        theta = jnp.float32(THETA[0] * scale)
        for i in range(1, ITERS):
            theta = jnp.where(k == i, jnp.float32(THETA[i] * scale), theta)
        return theta

    def dots(k, first, count):
        def one(i, _):
            def part(b, acc):
                acc = list(acc)
                for j in range(8):
                    r = b * 8 + j + HALO + first
                    prod = basis[k, r] * basis[i, r]
                    n = 0
                    for h in range(channels // 8):
                        for t in range(tiles):
                            acc[n % 4] = acc[n % 4] + prod[8 * h:8 * h + 8, 128 * t:128 * t + 128]
                            n += 1
                return tuple(acc)

            zero = jnp.zeros((8, 128), jnp.float32)
            acc = lax.fori_loop(0, count // 8, part, (zero,) * 4)
            gram_acc[lax.div(k * (k + 1), 2) + i] = (acc[0] + acc[1]) + (acc[2] + acc[3])
            return 0

        lax.fori_loop(0, k + 1, one, 0)

    def split(stack):
        high = stack.astype(jnp.bfloat16)
        low = (stack - high.astype(jnp.float32)).astype(jnp.bfloat16)
        return jnp.concatenate([high, low, high], axis=0)

    def rows(k, picked, theta, beside, bare=False):
        stack = jnp.concatenate([basis[k, r + HALO] for r in picked], axis=0)
        mixed = lax.dot_general(block[...], split(stack), (((1,), (0,)), ((), ())), preferred_element_type=jnp.float32)
        for j, r in enumerate(picked):
            inside = 0 <= r < lat
            source = beside[0] if inside else beside[1]
            left = 2 * r if inside else 64 + 2 * (r % lat)
            right = 64 + 2 * r if inside else 2 * (r % lat)

            def turn(v, shift):
                return pltpu.roll(v, shift % 128, 1) if shift % 128 else v

            x = [basis[k, r + HALO, :, 128 * t:128 * t + 128] for t in range(tiles)]
            fwd1 = [pltpu.roll(v, 127, 1) for v in x] + [turn(source, 127 - right)]
            fwd2 = [pltpu.roll(v, 126, 1) for v in x] + [turn(source, 126 - right)]
            bwd1 = [turn(source, -left - 1)] + [pltpu.roll(v, 1, 1) for v in x]
            bwd2 = [turn(source, -left)] + [pltpu.roll(v, 2, 1) for v in x]
            for t in range(tiles):
                cut = slice(128 * t, 128 * t + 128)
                e1 = jnp.where(lane < 127, fwd1[t], fwd1[t + 1])
                e2 = jnp.where(lane < 126, fwd2[t], fwd2[t + 1])
                w1 = jnp.where(lane >= 1, bwd1[t + 1], bwd1[t])
                w2 = jnp.where(lane >= 2, bwd2[t + 1], bwd2[t])

                def weight(q):
                    return coef[r + 2, q:q + 1, cut]

                def near(d):
                    return basis[k, r + HALO + d, :, cut]

                def has(d):
                    return not bare or 0 <= r + d < lat

                value = (diag[r + 2, :, cut] - theta) * x[t] + mixed[channels * j:channels * (j + 1), cut]
                value = value + (weight(0) * e1 + weight(1) * w1 + weight(2) * (w2 - e2))
                if has(1):
                    value = value + weight(3) * near(1)
                if has(-1):
                    value = value + weight(4) * near(-1)
                if has(2) and has(-2):
                    value = value + weight(5) * (near(-2) - near(2))
                elif has(2):
                    value = value - weight(5) * near(2)
                else:
                    value = value + weight(5) * near(-2)
                basis[k + 1, r + HALO, :, cut] = value

    def middle(b):
        from_east, from_west = side_in[b, 0], side_in[b, 1]
        return jnp.where(lane < 64, from_west, pltpu.roll(from_east, 64, 1))

    def edge_band(b, theta, centre, corners):
        from_east, from_west = side_in[b, 0], side_in[b, 1]
        to_west, to_east = side_out[b, 0], side_out[b, 1]
        low = jnp.where(lane < 64, pltpu.roll(from_west, 64, 1), pltpu.roll(to_east, 64, 1))
        high = jnp.where(lane < 64, to_west, from_east)
        even = lax.rem(lane, 2) == 0
        e1 = jnp.where(even, pltpu.roll(centre, 127, 1), pltpu.roll(high, 1, 1))
        w1 = jnp.where(even, pltpu.roll(low, 127, 1), pltpu.roll(centre, 1, 1))
        row = lax.rem(lane, 64) // 2
        n1 = jnp.where(row < lat - 1, pltpu.roll(centre, 126, 1), pltpu.roll(corners, 126, 1))
        n2 = jnp.where(row < lat - 2, pltpu.roll(centre, 124, 1), pltpu.roll(corners, 124, 1))
        s1 = jnp.where(row >= 1, pltpu.roll(centre, 2, 1), pltpu.roll(corners, 2, 1))
        s2 = jnp.where(row >= 2, pltpu.roll(centre, 4, 1), pltpu.roll(corners, 4, 1))
        mixed = lax.dot_general(single[...], split(centre), (((1,), (0,)), ((), ())), preferred_element_type=jnp.float32)
        own = jnp.where(lane < 64, fixed_in[1, 0:channels, :], pltpu.roll(fixed_in[0, 0:channels, :], 64, 1))
        tail = jnp.where(spot < 64, fixed_in[1, channels:channels + 8, :],
                         pltpu.roll(fixed_in[0, channels:channels + 8, :], 64, 1))

        def weight(q):
            return tail[q:q + 1, :]

        value = (own - theta) * centre + mixed
        value = value + (weight(0) * e1 + weight(1) * w1 + weight(2) * (low - high))
        value = value + weight(3) * n1 + weight(4) * s1 + weight(5) * (s2 - n2)
        band[...] = value

    def stage(b, _):
        k = 2 * b
        theta, after = theta_of(k), theta_of(k + 1)

        @pl.when(b > 0)
        def _():
            dots(k - 1, 0, lat)

        dots(k, 0, lat)
        lon_copy(b, 0).wait()
        lon_copy(b, 1).wait()
        centre = middle(b)
        for g in range((lat - 4) // GROUP):
            rows(k, [2 + GROUP * g + j for j in range(GROUP)], theta, (centre, None))
        rows(k, (0, 1, lat - 2, lat - 1), theta, (centre, None), bare=True)

        @pl.when(b == 0)
        def _():
            fix_side(0).wait()
            fix_side(1).wait()

        def corners_in(up):
            turn_copy(b, up, 0).wait_recv()
            turn_copy(b, up, 1).wait_recv()

        arrive_lat(corners_in)
        corners = take_corners(b)
        edge_band(b, theta, centre, corners)
        beside = band[...]
        for g in range((lat - 8) // GROUP):
            rows(k + 1, [4 + GROUP * g + j for j in range(GROUP)], after, (beside, None))

        def halo_in(way):
            lat_copy(b, way).wait_recv()

            @pl.when(b == 0)
            def _():
                for copy in fix_copies(way):
                    copy.wait_recv()

        arrive_lat(halo_in)
        rows(k, (-2, -1, lat, lat + 1), theta, (None, corners))
        south, north = basis[k, HALO - 1], basis[k, HALO + lat]
        basis[k + 1, HALO] += coef[2, 4:5, :] * south + coef[2, 5:6, :] * basis[k, HALO - 2]
        basis[k + 1, HALO + 1] += coef[3, 5:6, :] * south
        basis[k + 1, HALO + lat - 1] += coef[lat + 1, 3:4, :] * north - coef[lat + 1, 5:6, :] * basis[k, HALO + lat + 1]
        basis[k + 1, HALO + lat - 2] -= coef[lat, 5:6, :] * north
        rows(k + 1, tuple(range(4)), after, (beside, None))
        rows(k + 1, tuple(range(lat - 4, lat)), after, (beside, None))

        @pl.when(b + 1 < BLOCKS)
        def _():
            each_lat(lambda way: lat_copy(b + 1, way).start())
            send_side(b + 1)

        def sent(way):
            lat_copy(b, way).wait_send()
            turn_copy(b, way, 0).wait_send()
            turn_copy(b, way, 1).wait_send()

            @pl.when(b == 0)
            def _():
                for copy in fix_copies(way):
                    copy.wait_send()

        each_lat(sent)
        return 0

    pl.semaphore_wait(barrier, total - 1)
    each_lat(lambda way: lat_copy(0, way).start())
    send_side(0)
    fix_side(0).start()
    fix_side(1).start()

    def give_fixed(way):
        for copy in fix_copies(way):
            copy.start()

    each_lat(give_fixed)
    lax.fori_loop(0, BLOCKS, stage, 0)
    dots(ITERS - 1, 0, lat)
    dots(ITERS, 0, lat)

    sums = jnp.concatenate(
        [jnp.sum(gram_acc[n], axis=0, keepdims=True) for n in range(len(PAIRS))]
        + [jnp.zeros((128 - len(PAIRS), 128), jnp.float32)], axis=0)
    flat = lax.dot_general(jnp.ones((8, 128), jnp.float32), sums, (((1,), (1,)), ((), ())), precision=HI,
                           preferred_element_type=jnp.float32)
    mine[...] = flat[0:1, :]
    slots[me] = flat[0:1, :]

    def share(o):
        other = lax.rem(me + o, total)
        return pltpu.make_async_remote_copy(
            src_ref=mine, dst_ref=slots.at[me], send_sem=red_send.at[o], recv_sem=red_recv.at[me],
            device_id=(other // ny, lax.rem(other, ny)), device_id_type=MESH)

    def take(o):
        other = lax.rem(me + total - o, total)
        return pltpu.make_async_remote_copy(
            src_ref=mine, dst_ref=slots.at[other], send_sem=red_send.at[o], recv_sem=red_recv.at[other],
            device_id=(other // ny, lax.rem(other, ny)), device_id_type=MESH)

    def give(o, _):
        share(o).start()
        return 0

    def get(o, _):
        take(o).wait_recv()
        share(o).wait_send()
        return 0

    lax.fori_loop(1, total, give, 0)
    lax.fori_loop(1, total, get, 0)
    whole = slots[0]
    for n in range(1, total):
        whole = whole + slots[n]
    gram = [[None] * (ITERS + 1) for _ in range(ITERS + 1)]
    for n, (k, i) in enumerate(PAIRS):
        gram[k][i] = gram[i][k] = jnp.broadcast_to(whole[:, n:n + 1], (8, 128))
    answer, applied = small_solve(gram)
    for k in range(ITERS):
        splats[k] = answer[k]
    for k in range(ITERS + 1):
        splats[ITERS + k] = applied[k]


def finish(b_ref, w_ref, sol_hbm, res_hbm, outs, out_sem):
    channels, lat, lon = sol_hbm.shape
    stores = []
    for part in range(lat // 8):
        def one(j, _):
            r = 8 * part + j
            for h in range(channels // 8):
                for t in range(lon // 128):
                    at = (slice(8 * h, 8 * h + 8), slice(128 * t, 128 * t + 128))
                    x = b_ref[0, r + HALO, at[0], at[1]]
                    best = w_ref[0] * x
                    rest = x - w_ref[ITERS] * x
                    for k in range(1, ITERS + 1):
                        x = b_ref[k, r + HALO, at[0], at[1]]
                        if k < ITERS:
                            best = best + w_ref[k] * x
                        rest = rest - w_ref[ITERS + k] * x
                    outs[0, r, at[0], at[1]] = best
                    outs[1, r, at[0], at[1]] = rest
            return 0

        lax.fori_loop(0, 8, one, 0)
        for q, dst in enumerate((sol_hbm, res_hbm)):
            for c in range(channels):
                copy = pltpu.make_async_copy(outs.at[q, pl.ds(8 * part, 8), c, :], dst.at[c, pl.ds(8 * part, 8), :],
                                             out_sem.at[part, q, c])
                copy.start()
                stores.append(copy)
    for copy in stores:
        copy.wait()


def solution(mesh):
    nx, ny = mesh.shape["gx"], mesh.shape["gy"]

    def per_device(forcing, damping, coupling, wind_lon, wind_lat):
        channels, lat, lon = forcing.shape
        f32 = jnp.float32
        vmem = pl.BlockSpec(memory_space=pltpu.VMEM)
        hbm = pl.BlockSpec(memory_space=pltpu.HBM)
        dma = pltpu.SemaphoreType.DMA

        def keep(v):
            return pltpu.with_memory_space_constraint(v, pltpu.HBM)

        basis, weights = pl.pallas_call(
            functools.partial(kernel, nx, ny),
            out_shape=(pltpu.VMEM((ITERS + 1, lat + 2 * HALO, channels, lon), f32), pltpu.VMEM((2 * ITERS + 1, 8, 128), f32)),
            in_specs=[hbm, hbm, vmem, hbm, hbm],
            out_specs=(vmem, vmem),
            scratch_shapes=[
                pltpu.VMEM((lat + 4, channels, lon), f32),
                pltpu.VMEM((lat + 4, 8, lon), f32),
                pltpu.VMEM((GROUP * channels, 3 * GROUP * channels), jnp.bfloat16),
                pltpu.VMEM((channels, 3 * channels), jnp.bfloat16),
                pltpu.VMEM((BLOCKS, 2, channels, 128), f32),
                pltpu.VMEM((BLOCKS, 2, channels, 128), f32),
                pltpu.VMEM((channels, 128), f32),
                pltpu.VMEM((2, channels + 8, 128), f32),
                pltpu.VMEM((2, channels + 8, 128), f32),
                pltpu.VMEM((BLOCKS, 4, 2, 128), f32),
                pltpu.VMEM((BLOCKS, 2, 128), f32),
                pltpu.VMEM((len(PAIRS), 8, 128), f32),
                pltpu.VMEM((1, 128), f32),
                pltpu.VMEM((nx * ny, 1, 128), f32),
                pltpu.VMEM((lat, lon), f32), pltpu.VMEM((lat, lon), f32),
                dma((2, channels)), dma((2,)),
                dma((BLOCKS, 2)), dma((BLOCKS, 2)), dma((BLOCKS, 2)), dma((BLOCKS, 2)),
                dma((BLOCKS, 4)), dma((BLOCKS, 4)), dma((3, 2)), dma((3, 2)),
                dma((nx * ny,)), dma((nx * ny,)),
            ],
            compiler_params=pltpu.CompilerParams(
                collective_id=0, has_side_effects=True, vmem_limit_bytes=24 * 1024 * 1024),
        )(keep(forcing), keep(damping), coupling, keep(wind_lon), keep(wind_lat))
        shape = jax.ShapeDtypeStruct((channels, lat, lon), f32)
        return pl.pallas_call(
            finish,
            out_shape=(shape, shape),
            in_specs=[vmem, vmem],
            out_specs=(hbm, hbm),
            scratch_shapes=[pltpu.VMEM((2, lat, channels, lon), f32), dma((lat // 8, 2, channels))],
            compiler_params=pltpu.CompilerParams(vmem_limit_bytes=24 * 1024 * 1024),
        )(basis, weights)

    return jax.shard_map(
        per_device,
        mesh=mesh,
        in_specs=(P(None, "gy", "gx"), P(None, "gy", "gx"), P(), P("gy", "gx"), P("gy", "gx")),
        out_specs=(P(None, "gy", "gx"), P(None, "gy", "gx")),
        check_vma=False,
    )
```

```python
import functools
import math

import jax
import jax.numpy as jnp
from jax import lax
from jax.experimental import pallas as pl
from jax.experimental.pallas import tpu as pltpu
from jax.sharding import PartitionSpec as P

ITERS = 8
COUPLE = 0.25
DIFF_LAT = 0.5
DIFF_LON = 0.5
GUARD = 1.0
MESH = pl.DeviceIdType.MESH
HI = lax.Precision.HIGHEST

MIDDLE = 9.0
RADIUS = 6.0
WIDTH = 3.0
THETA = [MIDDLE + RADIUS * math.cos(math.pi * (2 * k + 1) / (2 * ITERS)) for k in (7, 0, 4, 2, 6, 1, 5, 3)]
PAIRS = [(k, i) for k in range(ITERS + 1) for i in range(k + 1)]
GROUP = 4
HALO = 4
BLOCKS = ITERS // 2


def apply_to(coords):
    out = [None] * (len(coords) + 1)
    for k, value in enumerate(coords):
        low = THETA[k] * value if k < ITERS else value
        out[k] = low if out[k] is None else out[k] + low
        out[k + 1] = WIDTH * value
    return out


def small_solve(gram):
    first = jnp.sqrt(gram[0][0] + GUARD)
    coords = [[1.0 / first]]
    images = [[gram[i][0] * coords[0][0] for i in range(ITERS + 1)]]
    heights = []
    for j in range(ITERS):
        moved = apply_to(coords[j])
        column = []
        for i in range(j + 1):
            column.append(functools.reduce(lambda a, b: a + b, [images[i][k] * moved[k] for k in range(j + 2)]))
        left = list(moved)
        for i in range(j + 1):
            for k in range(i + 1):
                left[k] = left[k] - column[i] * coords[i][k]
        image = [
            functools.reduce(lambda a, b: a + b, [gram[r][k] * left[k] for k in range(j + 2)])
            for r in range(ITERS + 1)
        ]
        norm_sq = functools.reduce(lambda a, b: a + b, [image[k] * left[k] for k in range(j + 2)])
        subdiag = jnp.sqrt(jnp.maximum(norm_sq, 0.0) + GUARD)
        column.append(subdiag)
        heights.append(column)
        inverse = 1.0 / subdiag
        coords.append([v * inverse for v in left])
        images.append([v * inverse for v in image])
    cosines, sines, target, rotated = [], [], [first], []
    for j in range(ITERS):
        column = list(heights[j])
        for e in range(j):
            upper, lower = column[e], column[e + 1]
            column[e] = cosines[e] * upper + sines[e] * lower
            column[e + 1] = cosines[e] * lower - sines[e] * upper
        upper, lower = column[j], column[j + 1]
        radius = jnp.sqrt(upper * upper + lower * lower)
        inverse = 1.0 / radius
        cosine, sine = upper * inverse, lower * inverse
        column[j] = radius
        kept = target[j]
        target[j] = cosine * kept
        target.append(-sine * kept)
        cosines.append(cosine)
        sines.append(sine)
        rotated.append(column)
    weights = [None] * ITERS
    for j in reversed(range(ITERS)):
        value = target[j]
        for later in range(j + 1, ITERS):
            value = value - rotated[later][j] * weights[later]
        weights[j] = value / rotated[j][j]
    answer = [None] * ITERS
    for j in range(ITERS):
        for k in range(j + 1):
            term = weights[j] * coords[j][k]
            answer[k] = term if answer[k] is None else answer[k] + term
    return answer, apply_to(answer)


def kernel(nx, ny, f_hbm, d_hbm, c_hbm, wl_hbm, wa_hbm, basis, splats,
           diag, coef, block, single, side_in, side_out, band, fixed_in, fixed_out, corner_in, corner_out,
           gram_acc, mine, slots, c_ref, wl_ref, wa_ref,
           in_sem, wind_sem, lat_send, lat_recv, lon_send, lon_recv, turn_send, turn_recv, fix_send, fix_recv, red_send, red_recv):
    channels, lat, lon = f_hbm.shape
    tiles = lon // 128
    total = nx * ny
    ix, iy = lax.axis_index("gx"), lax.axis_index("gy")
    me = ix * ny + iy
    east, west = lax.rem(ix + 1, nx), lax.rem(ix + nx - 1, nx)

    loads = [[], []]
    for q, (src, dst, off) in enumerate(((f_hbm, basis.at[0], HALO), (d_hbm, diag, 2))):
        for c in range(channels):
            copy = pltpu.make_async_copy(src.at[c], dst.at[pl.ds(off, lat), c, :], in_sem.at[q, c])
            copy.start()
            loads[q].append(copy)
    small = [pltpu.make_async_copy(src, dst, wind_sem.at[n])
             for n, (src, dst) in enumerate(((wl_hbm, wl_ref), (wa_hbm, wa_ref), (c_hbm, c_ref)))]
    for copy in small:
        copy.start()

    barrier = pltpu.get_barrier_semaphore()

    def greet(o, _):
        other = lax.rem(me + o, total)
        pl.semaphore_signal(barrier, inc=1, device_id=(other // ny, lax.rem(other, ny)), device_id_type=MESH)
        return 0

    lax.fori_loop(1, total, greet, 0)

    scale = 1.0 / WIDTH
    size = GROUP * channels

    def spread(n):
        row = lax.broadcasted_iota(jnp.int32, (n, channels), 0)
        col = lax.broadcasted_iota(jnp.int32, (n, channels), 1)
        return jnp.where(lax.rem(row, channels) == col, 1.0, 0.0).astype(jnp.float32)

    def widen(tall, n):
        wide = lax.dot_general(tall, spread(3 * n), (((1,), (1,)), ((), ())), precision=HI,
                               preferred_element_type=jnp.float32) * (COUPLE * scale)
        across = lax.broadcasted_iota(jnp.int32, wide.shape, 1)
        high = wide.astype(jnp.bfloat16).astype(jnp.float32)
        return jnp.where(across < 2 * n, high, wide - high), across

    def blank(at):
        for b in range(BLOCKS):
            basis[2 * b, pl.ds(HALO + lat if at else 0, HALO)] = jnp.zeros((HALO, channels, lon), jnp.float32)
        diag[pl.ds(lat + 2 if at else 0, 2)] = jnp.zeros((2, channels, lon), jnp.float32)
        coef[pl.ds(lat + 2 if at else 0, 2)] = jnp.zeros((2, 8, lon), jnp.float32)
        corner_in[:, 0 if at else 2] = jnp.zeros((BLOCKS, 2, 128), jnp.float32)
        corner_in[:, 1 if at else 3] = jnp.zeros((BLOCKS, 2, 128), jnp.float32)

    @pl.when(iy == 0)
    def _():
        blank(0)

    @pl.when(iy == ny - 1)
    def _():
        blank(1)

    def pack(read, far, n):
        lane = lax.broadcasted_iota(jnp.int32, (n, 128), 1)
        to_west = to_east = jnp.zeros((n, 128), jnp.float32)
        for r in range(lat):
            head = read(r, slice(0, 128))
            tail = read(r, slice(lon - 128, lon))
            here = (lane >= 2 * r) & (lane < 2 * r + 2)
            to_west = jnp.where(here, pltpu.roll(head, 2 * r, 1) if r else head, to_west)
            to_east = jnp.where(here, pltpu.roll(tail, (2 * r + 2) % 128, 1), to_east)
            if far:
                here = (lane >= 64 + 2 * r) & (lane < 64 + 2 * r + 2)
                to_west = jnp.where(here, pltpu.roll(head, (62 + 2 * r) % 128, 1), to_west)
                to_east = jnp.where(here, pltpu.roll(tail, (68 + 2 * r) % 128, 1), to_east)
        return to_west, to_east

    lane = lax.broadcasted_iota(jnp.int32, (channels, 128), 1)
    spot = lax.broadcasted_iota(jnp.int32, (8, 128), 1)
    deep = lax.broadcasted_iota(jnp.int32, (8, 128), 0)

    def copy_to(src, dst, send, recv, to):
        return pltpu.make_async_remote_copy(src_ref=src, dst_ref=dst, send_sem=send, recv_sem=recv,
                                            device_id=to, device_id_type=MESH)

    def lat_to(way):
        return iy + 1 if way else iy - 1

    def lat_copy(b, way):
        src = pl.ds(lat, HALO) if way else pl.ds(HALO, HALO)
        dst = pl.ds(0, HALO) if way else pl.ds(lat + HALO, HALO)
        return copy_to(basis.at[2 * b, src], basis.at[2 * b, dst], lat_send.at[b, way], lat_recv.at[b, way], (ix, lat_to(way)))

    def fix_copies(way):
        src = pl.ds(lat, 2) if way else pl.ds(2, 2)
        dst = pl.ds(0, 2) if way else pl.ds(lat + 2, 2)
        return [copy_to(ref.at[src], ref.at[dst], fix_send.at[n, way], fix_recv.at[n, way], (ix, lat_to(way)))
                for n, ref in enumerate((diag, coef))]

    def fix_side(way):
        return copy_to(fixed_out.at[way], fixed_in.at[way], fix_send.at[2, way], fix_recv.at[2, way],
                       (east if way else west, iy))

    def lon_copy(b, way):
        return copy_to(side_out.at[b, way], side_in.at[b, way], lon_send.at[b, way], lon_recv.at[b, way],
                       (east if way else west, iy))

    def turn_copy(b, up, way):
        n = 2 * up + way
        return copy_to(corner_out.at[b], corner_in.at[b, n], turn_send.at[b, n], turn_recv.at[b, n],
                       (east if way else west, lat_to(up)))

    def each_lat(act):
        @pl.when(iy < ny - 1)
        def _():
            act(1)

        @pl.when(iy > 0)
        def _():
            act(0)

    def arrive_lat(act):
        @pl.when(iy > 0)
        def _():
            act(1)

        @pl.when(iy < ny - 1)
        def _():
            act(0)

    def send_all(b):
        k = 2 * b
        small = jnp.zeros((8, 128), jnp.float32)
        for up in range(2):
            for way in range(2):
                for h in range(channels // 8):
                    for j in range(2):
                        at = 16 * up + 8 * way + 4 * h + 2 * j
                        here = (spot >= at) & (spot < at + 2)
                        cut = slice(lon - 128, lon) if way else slice(0, 128)
                        part = basis[k, HALO + (lat - 2 if up else 0) + j, 8 * h:8 * h + 8, cut]
                        move = (at - (126 if way else 0)) % 128
                        small = jnp.where(here, pltpu.roll(part, move, 1) if move else part, small)
        dense = small
        for g in range(1, 4):
            moved = pltpu.roll(pltpu.roll(small, 8 - 2 * g, 0), 32 * g, 1)
            dense = jnp.where(spot // 32 == g, moved, dense)
        corner_out[b] = dense[0:2, :]

        def go(up):
            turn_copy(b, up, 0).start()
            turn_copy(b, up, 1).start()
            lat_copy(b, up).start()

        each_lat(go)
        to_west, to_east = pack(lambda r, cut: basis[k, r + HALO, :, cut], True, channels)
        side_out[b, 0] = to_west
        side_out[b, 1] = to_east
        lon_copy(b, 0).start()
        lon_copy(b, 1).start()

    def take_corners(b):
        got = jnp.zeros((2, 128), jnp.float32)
        sub = lax.rem(lax.broadcasted_iota(jnp.int32, (2, 128), 1), 32) // 8
        for n in range(4):
            got = jnp.where(sub == n, corner_in[b, n], got)
        got = jnp.concatenate([got] * 4, axis=0)
        small = got
        for g in range(1, 4):
            small = jnp.where(deep // 2 == g, pltpu.roll(got, 128 - 32 * g, 1), small)
        parts = []
        for h in range(channels // 8):
            part = jnp.zeros((8, 128), jnp.float32)
            for up in range(2):
                for way in range(2):
                    at = 16 * up + 8 * way + 4 * h
                    want = (64 if way else 0) + (2 * lat - 4 if up else 0)
                    here = (spot >= want) & (spot < want + 4)
                    part = jnp.where(here, pltpu.roll(small, (want - at) % 128, 1) if want != at else small, part)
            parts.append(part)
        return jnp.concatenate(parts, axis=0)

    def theta_of(k):
        theta = jnp.float32(THETA[0] * scale)
        for i in range(1, ITERS):
            theta = jnp.where(k == i, jnp.float32(THETA[i] * scale), theta)
        return theta

    def products(k, i, places, acc):
        n = 0
        for r in places:
            prod = basis[k, r + HALO] * basis[i, r + HALO]
            for h in range(channels // 8):
                for t in range(tiles):
                    acc[n % 4] = acc[n % 4] + prod[8 * h:8 * h + 8, 128 * t:128 * t + 128]
                    n += 1
        return acc

    def dots(k, first, count):
        def one(i, _):
            def part(b, acc):
                return tuple(products(k, i, [b * 8 + j + first for j in range(8)], list(acc)))

            zero = jnp.zeros((8, 128), jnp.float32)
            acc = lax.fori_loop(0, count // 8, part, (zero,) * 4)
            gram_acc[lax.div(k * (k + 1), 2) + i] = (acc[0] + acc[1]) + (acc[2] + acc[3])
            return 0

        lax.fori_loop(0, k + 1, one, 0)

    def dots_rest(k):
        def one(i, _):
            zero = jnp.zeros((8, 128), jnp.float32)
            acc = products(k, i, list(range(4)) + list(range(lat - 4, lat)), [zero] * 4)
            gram_acc[lax.div(k * (k + 1), 2) + i] += (acc[0] + acc[1]) + (acc[2] + acc[3])
            return 0

        lax.fori_loop(0, k + 1, one, 0)

    def split(stack):
        high = stack.astype(jnp.bfloat16)
        low = (stack - high.astype(jnp.float32)).astype(jnp.bfloat16)
        return jnp.concatenate([high, low, high], axis=0)

    def rows(k, picked, theta, beside, bare=False):
        stack = jnp.concatenate([basis[k, r + HALO] for r in picked], axis=0)
        mixed = lax.dot_general(block[...], split(stack), (((1,), (0,)), ((), ())), preferred_element_type=jnp.float32)
        for j, r in enumerate(picked):
            inside = 0 <= r < lat
            source = beside
            left = 2 * r if inside else 64 + 2 * (r % lat)
            right = 64 + 2 * r if inside else 2 * (r % lat)

            def turn(v, shift):
                return pltpu.roll(v, shift % 128, 1) if shift % 128 else v

            x = [basis[k, r + HALO, :, 128 * t:128 * t + 128] for t in range(tiles)]
            if source is None:
                ends = [jnp.zeros_like(lane, jnp.float32)] * 4
            else:
                ends = [turn(source, shift) for shift in (127 - right, 126 - right, -left - 1, -left)]
            fwd1 = [pltpu.roll(v, 127, 1) for v in x] + [ends[0]]
            fwd2 = [pltpu.roll(v, 126, 1) for v in x] + [ends[1]]
            bwd1 = [ends[2]] + [pltpu.roll(v, 1, 1) for v in x]
            bwd2 = [ends[3]] + [pltpu.roll(v, 2, 1) for v in x]
            for t in range(tiles):
                cut = slice(128 * t, 128 * t + 128)
                e1 = jnp.where(lane < 127, fwd1[t], fwd1[t + 1])
                e2 = jnp.where(lane < 126, fwd2[t], fwd2[t + 1])
                w1 = jnp.where(lane >= 1, bwd1[t + 1], bwd1[t])
                w2 = jnp.where(lane >= 2, bwd2[t + 1], bwd2[t])

                def weight(q):
                    return coef[r + 2, q:q + 1, cut]

                def near(d):
                    return basis[k, r + HALO + d, :, cut]

                def has(d):
                    return not bare or 0 <= r + d < lat

                value = (diag[r + 2, :, cut] - theta) * x[t] + mixed[channels * j:channels * (j + 1), cut]
                value = value + (weight(0) * e1 + weight(1) * w1 + weight(2) * (w2 - e2))
                if has(1):
                    value = value + weight(3) * near(1)
                if has(-1):
                    value = value + weight(4) * near(-1)
                if has(2) and has(-2):
                    value = value + weight(5) * (near(-2) - near(2))
                elif has(2):
                    value = value - weight(5) * near(2)
                else:
                    value = value + weight(5) * near(-2)
                basis[k + 1, r + HALO, :, cut] = value

    def middle(b):
        from_east, from_west = side_in[b, 0], side_in[b, 1]
        return jnp.where(lane < 64, from_west, pltpu.roll(from_east, 64, 1))

    row = lax.rem(lane, 64) // 2
    even = lax.rem(lane, 2) == 0

    def edge_coef(q):
        return jnp.where(spot[0:1] < 64, fixed_in[1, channels + q:channels + q + 1, :],
                         pltpu.roll(fixed_in[0, channels + q:channels + q + 1, :], 64, 1))

    def edge_band(b, theta, centre):
        from_east, from_west = side_in[b, 0], side_in[b, 1]
        to_west, to_east = side_out[b, 0], side_out[b, 1]
        low = jnp.where(lane < 64, pltpu.roll(from_west, 64, 1), pltpu.roll(to_east, 64, 1))
        high = jnp.where(lane < 64, to_west, from_east)
        e1 = jnp.where(even, pltpu.roll(centre, 127, 1), pltpu.roll(high, 1, 1))
        w1 = jnp.where(even, pltpu.roll(low, 127, 1), pltpu.roll(centre, 1, 1))
        n1 = jnp.where(row < lat - 1, pltpu.roll(centre, 126, 1), 0.0)
        n2 = jnp.where(row < lat - 2, pltpu.roll(centre, 124, 1), 0.0)
        s1 = jnp.where(row >= 1, pltpu.roll(centre, 2, 1), 0.0)
        s2 = jnp.where(row >= 2, pltpu.roll(centre, 4, 1), 0.0)
        mixed = lax.dot_general(single[...], split(centre), (((1,), (0,)), ((), ())), preferred_element_type=jnp.float32)
        own = jnp.where(lane < 64, fixed_in[1, 0:channels, :], pltpu.roll(fixed_in[0, 0:channels, :], 64, 1))
        value = (own - theta) * centre + mixed
        value = value + (edge_coef(0) * e1 + edge_coef(1) * w1 + edge_coef(2) * (low - high))
        return value + (edge_coef(3) * n1 + edge_coef(4) * s1 + edge_coef(5) * (s2 - n2))

    def edge_turn(corners):
        n1 = jnp.where(row < lat - 1, 0.0, pltpu.roll(corners, 126, 1))
        n2 = jnp.where(row < lat - 2, 0.0, pltpu.roll(corners, 124, 1))
        s1 = jnp.where(row >= 1, 0.0, pltpu.roll(corners, 2, 1))
        s2 = jnp.where(row >= 2, 0.0, pltpu.roll(corners, 4, 1))
        return edge_coef(3) * n1 + edge_coef(4) * s1 + edge_coef(5) * (s2 - n2)

    def add_sides(k, centre):
        def own(q):
            return jnp.where(spot[0:1] < 64, fixed_out[0, channels + q:channels + q + 1, :],
                             pltpu.roll(fixed_out[1, channels + q:channels + q + 1, :], 64, 1))

        from_west = own(2) * centre + jnp.where(even, own(1) * pltpu.roll(centre, 127, 1), 0.0)
        from_east = jnp.where(even, 0.0, own(0) * pltpu.roll(centre, 1, 1)) - own(2) * centre
        for r in range(lat):
            left = pltpu.roll(from_west, (128 - 2 * r) % 128, 1) if r else from_west
            right = pltpu.roll(from_east, (62 - 2 * r) % 128, 1) if 2 * r != 62 else from_east
            basis[k + 1, r + HALO, :, 0:128] += jnp.where(lane < 2, left, 0.0)
            basis[k + 1, r + HALO, :, lon - 128:lon] += jnp.where(lane >= 126, right, 0.0)

    def stage(b, _):
        k = 2 * b
        theta, after = theta_of(k), theta_of(k + 1)
        for g in range((lat - 4) // GROUP):
            rows(k, [2 + GROUP * g + j for j in range(GROUP)], theta, None)
        rows(k, (0, 1, lat - 2, lat - 1), theta, None, bare=True)

        @pl.when(b > 0)
        def _():
            dots(k - 1, 0, lat)

        dots(k, 0, lat)
        lon_copy(b, 0).wait()
        lon_copy(b, 1).wait()

        @pl.when(b == 0)
        def _():
            fix_side(0).wait()
            fix_side(1).wait()

        centre = middle(b)
        add_sides(k, centre)
        band[...] = edge_band(b, theta, centre)
        beside = band[...]
        for g in range((lat - 8) // GROUP):
            rows(k + 1, [4 + GROUP * g + j for j in range(GROUP)], after, beside)

        @pl.when(b + 1 == BLOCKS)
        def _():
            dots(k + 1, 4, lat - 8)
            dots(k + 2, 4, lat - 8)

        def halo_in(way):
            turn_copy(b, way, 0).wait_recv()
            turn_copy(b, way, 1).wait_recv()
            lat_copy(b, way).wait_recv()

            @pl.when(b == 0)
            def _():
                for copy in fix_copies(way):
                    copy.wait_recv()

        arrive_lat(halo_in)
        corners = take_corners(b)
        beside = band[...] + edge_turn(corners)
        rows(k, (-2, -1, lat, lat + 1), theta, corners)
        south, north = basis[k, HALO - 1], basis[k, HALO + lat]
        basis[k + 1, HALO] += coef[2, 4:5, :] * south + coef[2, 5:6, :] * basis[k, HALO - 2]
        basis[k + 1, HALO + 1] += coef[3, 5:6, :] * south
        basis[k + 1, HALO + lat - 1] += coef[lat + 1, 3:4, :] * north - coef[lat + 1, 5:6, :] * basis[k, HALO + lat + 1]
        basis[k + 1, HALO + lat - 2] -= coef[lat, 5:6, :] * north
        rows(k + 1, tuple(range(4)), after, beside)
        rows(k + 1, tuple(range(lat - 4, lat)), after, beside)

        @pl.when(b + 1 < BLOCKS)
        def _():
            send_all(b + 1)

        def sent(way):
            lat_copy(b, way).wait_send()
            turn_copy(b, way, 0).wait_send()
            turn_copy(b, way, 1).wait_send()

            @pl.when(b == 0)
            def _():
                for copy in fix_copies(way):
                    copy.wait_send()

        each_lat(sent)
        return 0

    for copy in loads[0]:
        copy.wait()
    pl.semaphore_wait(barrier, total - 1)
    send_all(0)
    for copy in small:
        copy.wait()
    place = (lax.broadcasted_iota(jnp.int32, (lat, 128), 0) + iy * lat).astype(jnp.float32)
    phi = -math.pi / 2 + (place + 0.5) * (math.pi / (lat * ny))
    kx = (DIFF_LON * scale) / (jnp.cos(phi) ** 2 + 0.1)
    wl = wl_ref[...] * (scale / 12.0)
    wa = wa_ref[...] * (scale / 12.0)
    kx = jnp.concatenate([kx] * tiles, axis=1)
    planes = (8.0 * wl - kx, -8.0 * wl - kx, wl, 8.0 * wa - DIFF_LAT * scale, -8.0 * wa - DIFF_LAT * scale, wa,
              2.0 * kx + (1.0 + 2.0 * DIFF_LAT) * scale)
    for q, plane in enumerate(planes + (jnp.zeros_like(kx),)):
        for r in range(lat):
            coef[r + 2, q:q + 1, :] = plane[r:r + 1, :]

    for copy in loads[1]:
        copy.wait()

    def prepare(r, _):
        diag[r + 2] = diag[r + 2] * scale + coef[r + 2, 6:7, :]
        return 0

    lax.fori_loop(0, lat, prepare, 0)

    def give_fixed(way):
        for copy in fix_copies(way):
            copy.start()

    each_lat(give_fixed)
    fixed = [pack(lambda r, cut: diag[r + 2, :, cut], False, channels), pack(lambda r, cut: coef[r + 2, :, cut], False, 8)]
    for way in range(2):
        fixed_out[way, 0:channels, :] = fixed[0][way]
        fixed_out[way, channels:channels + 8, :] = fixed[1][way]
    fix_side(0).start()
    fix_side(1).start()
    single[...] = widen(c_ref[...], channels)[0].astype(jnp.bfloat16)
    tall = lax.dot_general(spread(size), c_ref[...], (((1,), (0,)), ((), ())), precision=HI,
                           preferred_element_type=jnp.float32)
    wide, across = widen(tall, size)
    down = lax.broadcasted_iota(jnp.int32, (size, 3 * size), 0)
    block[...] = jnp.where(down // channels == lax.rem(across, size) // channels, wide, 0.0).astype(jnp.bfloat16)
    lax.fori_loop(0, BLOCKS, stage, 0)
    dots_rest(ITERS - 1)
    dots_rest(ITERS)

    sums = jnp.concatenate(
        [jnp.sum(gram_acc[n], axis=0, keepdims=True) for n in range(len(PAIRS))]
        + [jnp.zeros((128 - len(PAIRS), 128), jnp.float32)], axis=0)
    flat = lax.dot_general(jnp.ones((8, 128), jnp.float32), sums, (((1,), (1,)), ((), ())), precision=HI,
                           preferred_element_type=jnp.float32)
    mine[...] = flat[0:1, :]
    slots[me] = flat[0:1, :]

    def share(o):
        other = lax.rem(me + o, total)
        return pltpu.make_async_remote_copy(
            src_ref=mine, dst_ref=slots.at[me], send_sem=red_send.at[o], recv_sem=red_recv.at[me],
            device_id=(other // ny, lax.rem(other, ny)), device_id_type=MESH)

    def take(o):
        other = lax.rem(me + total - o, total)
        return pltpu.make_async_remote_copy(
            src_ref=mine, dst_ref=slots.at[other], send_sem=red_send.at[o], recv_sem=red_recv.at[other],
            device_id=(other // ny, lax.rem(other, ny)), device_id_type=MESH)

    def give(o, _):
        share(o).start()
        return 0

    def get(o, _):
        take(o).wait_recv()
        share(o).wait_send()
        return 0

    lax.fori_loop(1, total, give, 0)
    lax.fori_loop(1, total, get, 0)
    whole = slots[0]
    for n in range(1, total):
        whole = whole + slots[n]
    gram = [[None] * (ITERS + 1) for _ in range(ITERS + 1)]
    for n, (k, i) in enumerate(PAIRS):
        gram[k][i] = gram[i][k] = jnp.broadcast_to(whole[:, n:n + 1], (8, 128))
    answer, applied = small_solve(gram)
    for k in range(ITERS):
        splats[k] = answer[k]
    for k in range(ITERS + 1):
        splats[ITERS + k] = applied[k]


def finish(b_ref, w_ref, sol_hbm, res_hbm, outs, out_sem):
    channels, lat, lon = sol_hbm.shape
    stores = []
    for part in range(lat // 8):
        def one(j, _):
            r = 8 * part + j
            for h in range(channels // 8):
                for t in range(lon // 128):
                    at = (slice(8 * h, 8 * h + 8), slice(128 * t, 128 * t + 128))
                    x = b_ref[0, r + HALO, at[0], at[1]]
                    best = w_ref[0] * x
                    rest = x - w_ref[ITERS] * x
                    for k in range(1, ITERS + 1):
                        x = b_ref[k, r + HALO, at[0], at[1]]
                        if k < ITERS:
                            best = best + w_ref[k] * x
                        rest = rest - w_ref[ITERS + k] * x
                    outs[0, r, at[0], at[1]] = best
                    outs[1, r, at[0], at[1]] = rest
            return 0

        lax.fori_loop(0, 8, one, 0)
        for q, dst in enumerate((sol_hbm, res_hbm)):
            for c in range(channels):
                copy = pltpu.make_async_copy(outs.at[q, pl.ds(8 * part, 8), c, :], dst.at[c, pl.ds(8 * part, 8), :],
                                             out_sem.at[part, q, c])
                copy.start()
                stores.append(copy)
    for copy in stores:
        copy.wait()


def solution(mesh):
    nx, ny = mesh.shape["gx"], mesh.shape["gy"]

    def per_device(forcing, damping, coupling, wind_lon, wind_lat):
        channels, lat, lon = forcing.shape
        f32 = jnp.float32
        vmem = pl.BlockSpec(memory_space=pltpu.VMEM)
        hbm = pl.BlockSpec(memory_space=pltpu.HBM)
        dma = pltpu.SemaphoreType.DMA

        def keep(v):
            return pltpu.with_memory_space_constraint(v, pltpu.HBM)

        basis, weights = pl.pallas_call(
            functools.partial(kernel, nx, ny),
            out_shape=(pltpu.VMEM((ITERS + 1, lat + 2 * HALO, channels, lon), f32), pltpu.VMEM((2 * ITERS + 1, 8, 128), f32)),
            in_specs=[hbm] * 5,
            out_specs=(vmem, vmem),
            scratch_shapes=[
                pltpu.VMEM((lat + 4, channels, lon), f32),
                pltpu.VMEM((lat + 4, 8, lon), f32),
                pltpu.VMEM((GROUP * channels, 3 * GROUP * channels), jnp.bfloat16),
                pltpu.VMEM((channels, 3 * channels), jnp.bfloat16),
                pltpu.VMEM((BLOCKS, 2, channels, 128), f32),
                pltpu.VMEM((BLOCKS, 2, channels, 128), f32),
                pltpu.VMEM((channels, 128), f32),
                pltpu.VMEM((2, channels + 8, 128), f32),
                pltpu.VMEM((2, channels + 8, 128), f32),
                pltpu.VMEM((BLOCKS, 4, 2, 128), f32),
                pltpu.VMEM((BLOCKS, 2, 128), f32),
                pltpu.VMEM((len(PAIRS), 8, 128), f32),
                pltpu.VMEM((1, 128), f32),
                pltpu.VMEM((nx * ny, 1, 128), f32),
                pltpu.VMEM((channels, channels), f32), pltpu.VMEM((lat, lon), f32), pltpu.VMEM((lat, lon), f32),
                dma((2, channels)), dma((3,)),
                dma((BLOCKS, 2)), dma((BLOCKS, 2)), dma((BLOCKS, 2)), dma((BLOCKS, 2)),
                dma((BLOCKS, 4)), dma((BLOCKS, 4)), dma((3, 2)), dma((3, 2)),
                dma((nx * ny,)), dma((nx * ny,)),
            ],
            compiler_params=pltpu.CompilerParams(
                collective_id=0, has_side_effects=True, vmem_limit_bytes=24 * 1024 * 1024),
        )(*map(keep, (forcing, damping, coupling, wind_lon, wind_lat)))
        shape = jax.ShapeDtypeStruct((channels, lat, lon), f32)
        return pl.pallas_call(
            finish,
            out_shape=(shape, shape),
            in_specs=[vmem, vmem],
            out_specs=(hbm, hbm),
            scratch_shapes=[pltpu.VMEM((2, lat, channels, lon), f32), dma((lat // 8, 2, channels))],
            compiler_params=pltpu.CompilerParams(vmem_limit_bytes=24 * 1024 * 1024),
        )(basis, weights)

    return jax.shard_map(
        per_device,
        mesh=mesh,
        in_specs=(P(None, "gy", "gx"), P(None, "gy", "gx"), P(), P("gy", "gx"), P("gy", "gx")),
        out_specs=(P(None, "gy", "gx"), P(None, "gy", "gx")),
        check_vma=False,
    )
```

```python
import functools
import math

import jax
import jax.numpy as jnp
from jax import lax
from jax.experimental import pallas as pl
from jax.experimental.pallas import tpu as pltpu
from jax.sharding import PartitionSpec as P

ITERS = 8
COUPLE = 0.25
DIFF_LAT = 0.5
DIFF_LON = 0.5
GUARD = 1.0
MESH = pl.DeviceIdType.MESH
HI = lax.Precision.HIGHEST

MIDDLE = 9.0
RADIUS = 6.0
WIDTH = 3.0
THETA = [MIDDLE + RADIUS * math.cos(math.pi * (2 * k + 1) / (2 * ITERS)) for k in (7, 0, 4, 2, 6, 1, 5, 3)]
PAIRS = [(k, i) for k in range(ITERS + 1) for i in range(k + 1)]
GROUP = 4
HALO = 4
BLOCKS = ITERS // 2


def apply_to(coords):
    out = [None] * (len(coords) + 1)
    for k, value in enumerate(coords):
        low = THETA[k] * value if k < ITERS else value
        out[k] = low if out[k] is None else out[k] + low
        out[k + 1] = WIDTH * value
    return out


def small_solve(gram):
    first = jnp.sqrt(gram[0][0] + GUARD)
    coords = [[1.0 / first]]
    images = [[gram[i][0] * coords[0][0] for i in range(ITERS + 1)]]
    heights = []
    for j in range(ITERS):
        moved = apply_to(coords[j])
        column = []
        for i in range(j + 1):
            column.append(functools.reduce(lambda a, b: a + b, [images[i][k] * moved[k] for k in range(j + 2)]))
        left = list(moved)
        for i in range(j + 1):
            for k in range(i + 1):
                left[k] = left[k] - column[i] * coords[i][k]
        image = [
            functools.reduce(lambda a, b: a + b, [gram[r][k] * left[k] for k in range(j + 2)])
            for r in range(ITERS + 1)
        ]
        norm_sq = functools.reduce(lambda a, b: a + b, [image[k] * left[k] for k in range(j + 2)])
        subdiag = jnp.sqrt(jnp.maximum(norm_sq, 0.0) + GUARD)
        column.append(subdiag)
        heights.append(column)
        inverse = 1.0 / subdiag
        coords.append([v * inverse for v in left])
        images.append([v * inverse for v in image])
    cosines, sines, target, rotated = [], [], [first], []
    for j in range(ITERS):
        column = list(heights[j])
        for e in range(j):
            upper, lower = column[e], column[e + 1]
            column[e] = cosines[e] * upper + sines[e] * lower
            column[e + 1] = cosines[e] * lower - sines[e] * upper
        upper, lower = column[j], column[j + 1]
        radius = jnp.sqrt(upper * upper + lower * lower)
        inverse = 1.0 / radius
        cosine, sine = upper * inverse, lower * inverse
        column[j] = radius
        kept = target[j]
        target[j] = cosine * kept
        target.append(-sine * kept)
        cosines.append(cosine)
        sines.append(sine)
        rotated.append(column)
    weights = [None] * ITERS
    for j in reversed(range(ITERS)):
        value = target[j]
        for later in range(j + 1, ITERS):
            value = value - rotated[later][j] * weights[later]
        weights[j] = value / rotated[j][j]
    answer = [None] * ITERS
    for j in range(ITERS):
        for k in range(j + 1):
            term = weights[j] * coords[j][k]
            answer[k] = term if answer[k] is None else answer[k] + term
    return answer, apply_to(answer)


def word_plan(nx, ny):
    def doubled(n):
        out = [2]
        while out[-1] < n:
            out.append(2 * out[-1])
        return out[:-1]

    far_lat, far_lon = doubled(ny), doubled(nx // 2 + 1)
    words = max(len(far_lat), len(far_lon))
    reach = {}
    for x in range(nx):
        for y in range(ny):
            reach[x, y] = {((x + dx) % nx, y + dy) for dx in (-1, 0, 1) for dy in (-1, 0, 1) if 0 <= y + dy < ny}
    near = {place: set(known) for place, known in reach.items()}

    def peers(x, y, n):
        out = []
        if n < len(far_lat):
            out += [(x, y + d) for d in (-far_lat[n], far_lat[n]) if 0 <= y + d < ny]
        if n < len(far_lon):
            out += [((x + d) % nx, y) for d in (-far_lon[n], far_lon[n])]
        return out

    told = None
    for n in range(BLOCKS):
        before = reach
        reach = {place: set().union(*(before[other] for other in near[place])) for place in before}
        if told is not None:
            reach = {place: known.union(*(told[other] for other in peers(*place, n - 1))) for place, known in reach.items()}
        told = reach
    if any(len(known) < nx * ny for known in reach.values()):
        far_lon = far_lon + [nx // 2] * (max(BLOCKS, words + 1) - len(far_lon))
    return far_lat, far_lon


def kernel(nx, ny, f_hbm, d_hbm, c_hbm, wl_hbm, wa_hbm, basis, splats,
           diag, coef, block, single, side_in, side_out, band, fixed_in, fixed_out, corner_in, corner_out,
           gram_acc, mine, slots, c_ref, wl_ref, wa_ref, wind_in, kx_in, turned,
           in_sem, wind_sem, lat_send, lat_recv, lon_send, lon_recv, turn_send, turn_recv, fix_send, fix_recv, red_send, red_recv, word):
    channels, lat, lon = f_hbm.shape
    tiles = lon // 128
    total = nx * ny
    ix, iy = lax.axis_index("gx"), lax.axis_index("gy")
    me = ix * ny + iy
    east, west = lax.rem(ix + 1, nx), lax.rem(ix + nx - 1, nx)

    small = [pltpu.make_async_copy(src, dst, wind_sem.at[n])
             for n, (src, dst) in enumerate(((wl_hbm, wl_ref), (wa_hbm, wa_ref), (c_hbm, c_ref)))]
    for copy in small:
        copy.start()
    loads = [[], []]
    for q, (src, dst, off) in enumerate(((f_hbm, basis.at[0], HALO), (d_hbm, diag, 2))):
        for c in range(channels):
            copy = pltpu.make_async_copy(src.at[c], dst.at[pl.ds(off, lat), c, :], in_sem.at[q, c])
            copy.start()
            loads[q].append(copy)

    barrier = pltpu.get_barrier_semaphore()

    def greet(to, sem=barrier):
        pl.semaphore_signal(sem, inc=1, device_id=to, device_id_type=MESH)

    greet((east, iy))
    greet((west, iy))

    def greet_lat(to):
        greet((ix, to))
        greet((east, to))
        greet((west, to))

    @pl.when(iy > 0)
    def _():
        greet_lat(iy - 1)

    @pl.when(iy < ny - 1)
    def _():
        greet_lat(iy + 1)

    far_lat, far_lon = word_plan(nx, ny)

    def spread_word(n):
        if n < len(far_lat):
            d = far_lat[n]

            @pl.when(iy >= d)
            def _():
                greet((ix, iy - d), word.at[n])

            @pl.when(iy + d < ny)
            def _():
                greet((ix, iy + d), word.at[n])

        if n < len(far_lon):
            greet((lax.rem(ix + far_lon[n], nx), iy), word.at[n])
            greet((lax.rem(ix + nx - far_lon[n], nx), iy), word.at[n])

    def hear_word(n):
        count = 2 if n < len(far_lon) else 0
        if n < len(far_lat):
            d = far_lat[n]
            count = count + jnp.where(iy >= d, 1, 0) + jnp.where(iy + d < ny, 1, 0)
        pl.semaphore_wait(word.at[n], count)

    words = max(len(far_lat), len(far_lon))

    scale = 1.0 / WIDTH
    size = GROUP * channels

    def spread(n):
        row = lax.broadcasted_iota(jnp.int32, (n, channels), 0)
        col = lax.broadcasted_iota(jnp.int32, (n, channels), 1)
        return jnp.where(lax.rem(row, channels) == col, 1.0, 0.0).astype(jnp.float32)

    def widen(tall, n):
        wide = lax.dot_general(tall, spread(3 * n), (((1,), (1,)), ((), ())), precision=HI,
                               preferred_element_type=jnp.float32) * (COUPLE * scale)
        across = lax.broadcasted_iota(jnp.int32, wide.shape, 1)
        high = wide.astype(jnp.bfloat16).astype(jnp.float32)
        return jnp.where(across < 2 * n, high, wide - high), across

    def blank(at):
        for b in range(BLOCKS):
            basis[2 * b, pl.ds(HALO + lat if at else 0, HALO)] = jnp.zeros((HALO, channels, lon), jnp.float32)
        diag[pl.ds(lat + 2 if at else 0, 2)] = jnp.zeros((2, channels, lon), jnp.float32)
        coef[pl.ds(lat + 2 if at else 0, 2)] = jnp.zeros((2, 8, lon), jnp.float32)
        corner_in[:, 0 if at else 2] = jnp.zeros((BLOCKS, 2, 128), jnp.float32)
        corner_in[:, 1 if at else 3] = jnp.zeros((BLOCKS, 2, 128), jnp.float32)

    @pl.when(iy == 0)
    def _():
        blank(0)

    @pl.when(iy == ny - 1)
    def _():
        blank(1)

    def fill_coef(wl, wa, kx, at):
        wl, wa = wl * (scale / 12.0), wa * (scale / 12.0)
        kx = jnp.concatenate([kx] * tiles, axis=1)
        planes = (8.0 * wl - kx, -8.0 * wl - kx, wl, 8.0 * wa - DIFF_LAT * scale, -8.0 * wa - DIFF_LAT * scale, wa,
                  2.0 * kx + (1.0 + 2.0 * DIFF_LAT) * scale, jnp.zeros_like(kx))
        for q, plane in enumerate(planes):
            for r in range(wl.shape[0]):
                coef[r + at, q:q + 1, :] = plane[r:r + 1, :]

    def pack(read, far, n):
        lane = lax.broadcasted_iota(jnp.int32, (n, 128), 1)
        to_west = to_east = jnp.zeros((n, 128), jnp.float32)
        for r in range(lat):
            head = read(r, slice(0, 128))
            tail = read(r, slice(lon - 128, lon))
            here = (lane >= 2 * r) & (lane < 2 * r + 2)
            to_west = jnp.where(here, pltpu.roll(head, 2 * r, 1) if r else head, to_west)
            to_east = jnp.where(here, pltpu.roll(tail, (2 * r + 2) % 128, 1), to_east)
            if far:
                here = (lane >= 64 + 2 * r) & (lane < 64 + 2 * r + 2)
                to_west = jnp.where(here, pltpu.roll(head, (62 + 2 * r) % 128, 1), to_west)
                to_east = jnp.where(here, pltpu.roll(tail, (68 + 2 * r) % 128, 1), to_east)
        return to_west, to_east

    lane = lax.broadcasted_iota(jnp.int32, (channels, 128), 1)
    spot = lax.broadcasted_iota(jnp.int32, (8, 128), 1)
    deep = lax.broadcasted_iota(jnp.int32, (8, 128), 0)

    def copy_to(src, dst, send, recv, to):
        return pltpu.make_async_remote_copy(src_ref=src, dst_ref=dst, send_sem=send, recv_sem=recv,
                                            device_id=to, device_id_type=MESH)

    def lat_to(way):
        return iy + 1 if way else iy - 1

    def lat_copy(b, way, near):
        if way:
            src, dst = HALO + lat - (2 if near else 4), 2 if near else 0
        else:
            src, dst = HALO + (0 if near else 2), HALO + lat + (0 if near else 2)
        return copy_to(basis.at[2 * b, pl.ds(src, 2)], basis.at[2 * b, pl.ds(dst, 2)], lat_send.at[b, way, near],
                       lat_recv.at[b, way, near], (ix, lat_to(way)))

    def diag_copy(way):
        src = pl.ds(lat, 2) if way else pl.ds(2, 2)
        dst = pl.ds(0, 2) if way else pl.ds(lat + 2, 2)
        return copy_to(diag.at[src], diag.at[dst], fix_send.at[0, way], fix_recv.at[0, way], (ix, lat_to(way)))

    def wind_copies(way):
        src = pl.ds(lat - 2, 2) if way else pl.ds(0, 2)
        return [copy_to(ref.at[src], wind_in.at[n, way], fix_send.at[1 + n, way], fix_recv.at[1 + n, way], (ix, lat_to(way)))
                for n, ref in enumerate((wl_ref, wa_ref))]

    def fix_side(way):
        return copy_to(fixed_out.at[way], fixed_in.at[way], fix_send.at[3, way], fix_recv.at[3, way],
                       (east if way else west, iy))

    def lon_copy(b, way):
        return copy_to(side_out.at[b, way], side_in.at[b, way], lon_send.at[b, way], lon_recv.at[b, way],
                       (east if way else west, iy))

    def turn_copy(b, up, way):
        n = 2 * up + way
        return copy_to(corner_out.at[b], corner_in.at[b, n], turn_send.at[b, n], turn_recv.at[b, n],
                       (east if way else west, lat_to(up)))

    def each_lat(act):
        @pl.when(iy < ny - 1)
        def _():
            act(1)

        @pl.when(iy > 0)
        def _():
            act(0)

    def arrive_lat(act):
        @pl.when(iy > 0)
        def _():
            act(1)

        @pl.when(iy < ny - 1)
        def _():
            act(0)

    def send_corners(b):
        k = 2 * b
        small = jnp.zeros((8, 128), jnp.float32)
        for up in range(2):
            for way in range(2):
                for h in range(channels // 8):
                    for j in range(2):
                        at = 16 * up + 8 * way + 4 * h + 2 * j
                        here = (spot >= at) & (spot < at + 2)
                        cut = slice(lon - 128, lon) if way else slice(0, 128)
                        part = basis[k, HALO + (lat - 2 if up else 0) + j, 8 * h:8 * h + 8, cut]
                        move = (at - (126 if way else 0)) % 128
                        small = jnp.where(here, pltpu.roll(part, move, 1) if move else part, small)
        dense = small
        for g in range(1, 4):
            moved = pltpu.roll(pltpu.roll(small, 8 - 2 * g, 0), 32 * g, 1)
            dense = jnp.where(spot // 32 == g, moved, dense)
        corner_out[b] = dense[0:2, :]

        def go(up):
            turn_copy(b, up, 0).start()
            turn_copy(b, up, 1).start()

        each_lat(go)

    def send_sides(b):
        k = 2 * b
        to_west, to_east = pack(lambda r, cut: basis[k, r + HALO, :, cut], True, channels)
        side_out[b, 0] = to_west
        side_out[b, 1] = to_east
        lon_copy(b, 0).start()
        lon_copy(b, 1).start()

    def take_corners(b):
        got = jnp.zeros((2, 128), jnp.float32)
        sub = lax.rem(lax.broadcasted_iota(jnp.int32, (2, 128), 1), 32) // 8
        for n in range(4):
            got = jnp.where(sub == n, corner_in[b, n], got)
        got = jnp.concatenate([got] * 4, axis=0)
        small = got
        for g in range(1, 4):
            small = jnp.where(deep // 2 == g, pltpu.roll(got, 128 - 32 * g, 1), small)
        parts = []
        for h in range(channels // 8):
            part = jnp.zeros((8, 128), jnp.float32)
            for up in range(2):
                for way in range(2):
                    at = 16 * up + 8 * way + 4 * h
                    want = (64 if way else 0) + (2 * lat - 4 if up else 0)
                    here = (spot >= want) & (spot < want + 4)
                    part = jnp.where(here, pltpu.roll(small, (want - at) % 128, 1) if want != at else small, part)
            parts.append(part)
        return jnp.concatenate(parts, axis=0)

    def theta_of(k):
        theta = jnp.float32(THETA[0] * scale)
        for i in range(1, ITERS):
            theta = jnp.where(k == i, jnp.float32(THETA[i] * scale), theta)
        return theta

    def products(k, i, places, acc):
        n = 0
        for r in places:
            prod = basis[k, r + HALO] * basis[i, r + HALO]
            for h in range(channels // 8):
                for t in range(tiles):
                    acc[n % 4] = acc[n % 4] + prod[8 * h:8 * h + 8, 128 * t:128 * t + 128]
                    n += 1
        return acc

    def dots(k, first, count):
        def one(i, _):
            def part(b, acc):
                return tuple(products(k, i, [b * 8 + j + first for j in range(8)], list(acc)))

            zero = jnp.zeros((8, 128), jnp.float32)
            acc = lax.fori_loop(0, count // 8, part, (zero,) * 4)
            gram_acc[lax.div(k * (k + 1), 2) + i] = (acc[0] + acc[1]) + (acc[2] + acc[3])
            return 0

        lax.fori_loop(0, k + 1, one, 0)

    def dots_rest():
        picked = list(range(4)) + list(range(lat - 4, lat))
        zero = jnp.zeros((8, 128), jnp.float32)

        def save(k, i, acc):
            gram_acc[k * (k + 1) // 2 + i] += (acc[0] + acc[1]) + (acc[2] + acc[3])

        def one(i, _):
            for k in (ITERS - 1, ITERS):
                save(k, i, products(k, i, picked, [zero] * 4))
            return 0

        lax.fori_loop(0, ITERS, one, 0)
        save(ITERS, ITERS, products(ITERS, ITERS, picked, [zero] * 4))

    def split(stack):
        high = stack.astype(jnp.bfloat16)
        low = (stack - high.astype(jnp.float32)).astype(jnp.bfloat16)
        return jnp.concatenate([high, low, high], axis=0)

    def rows(k, picked, theta, beside, bare=False):
        stack = jnp.concatenate([basis[k, r + HALO] for r in picked], axis=0)
        mixed = lax.dot_general(block[...], split(stack), (((1,), (0,)), ((), ())), preferred_element_type=jnp.float32)
        for j, r in enumerate(picked):
            inside = 0 <= r < lat
            source = beside
            left = 2 * r if inside else 64 + 2 * (r % lat)
            right = 64 + 2 * r if inside else 2 * (r % lat)

            def turn(v, shift):
                return pltpu.roll(v, shift % 128, 1) if shift % 128 else v

            x = [basis[k, r + HALO, :, 128 * t:128 * t + 128] for t in range(tiles)]
            if source is None:
                ends = [jnp.zeros_like(lane, jnp.float32)] * 4
            else:
                ends = [turn(source, shift) for shift in (127 - right, 126 - right, -left - 1, -left)]
            fwd1 = [pltpu.roll(v, 127, 1) for v in x] + [ends[0]]
            fwd2 = [pltpu.roll(v, 126, 1) for v in x] + [ends[1]]
            bwd1 = [ends[2]] + [pltpu.roll(v, 1, 1) for v in x]
            bwd2 = [ends[3]] + [pltpu.roll(v, 2, 1) for v in x]
            for t in range(tiles):
                cut = slice(128 * t, 128 * t + 128)
                e1 = jnp.where(lane < 127, fwd1[t], fwd1[t + 1])
                e2 = jnp.where(lane < 126, fwd2[t], fwd2[t + 1])
                w1 = jnp.where(lane >= 1, bwd1[t + 1], bwd1[t])
                w2 = jnp.where(lane >= 2, bwd2[t + 1], bwd2[t])

                def weight(q):
                    return coef[r + 2, q:q + 1, cut]

                def near(d):
                    return basis[k, r + HALO + d, :, cut]

                def has(d):
                    return not bare or 0 <= r + d < lat

                value = (diag[r + 2, :, cut] - theta) * x[t] + mixed[channels * j:channels * (j + 1), cut]
                value = value + (weight(0) * e1 + weight(1) * w1 + weight(2) * (w2 - e2))
                if has(1):
                    value = value + weight(3) * near(1)
                if has(-1):
                    value = value + weight(4) * near(-1)
                if has(2) and has(-2):
                    value = value + weight(5) * (near(-2) - near(2))
                elif has(2):
                    value = value - weight(5) * near(2)
                else:
                    value = value + weight(5) * near(-2)
                basis[k + 1, r + HALO, :, cut] = value

    def middle(b):
        from_east, from_west = side_in[b, 0], side_in[b, 1]
        return jnp.where(lane < 64, from_west, pltpu.roll(from_east, 64, 1))

    row = lax.rem(lane, 64) // 2
    even = lax.rem(lane, 2) == 0

    def edge_coef(q):
        return jnp.where(spot[0:1] < 64, fixed_in[1, channels + q:channels + q + 1, :],
                         pltpu.roll(fixed_in[0, channels + q:channels + q + 1, :], 64, 1))

    def edge_band(b, theta, centre):
        from_east, from_west = side_in[b, 0], side_in[b, 1]
        to_west, to_east = side_out[b, 0], side_out[b, 1]
        low = jnp.where(lane < 64, pltpu.roll(from_west, 64, 1), pltpu.roll(to_east, 64, 1))
        high = jnp.where(lane < 64, to_west, from_east)
        e1 = jnp.where(even, pltpu.roll(centre, 127, 1), pltpu.roll(high, 1, 1))
        w1 = jnp.where(even, pltpu.roll(low, 127, 1), pltpu.roll(centre, 1, 1))
        n1 = jnp.where(row < lat - 1, pltpu.roll(centre, 126, 1), 0.0)
        n2 = jnp.where(row < lat - 2, pltpu.roll(centre, 124, 1), 0.0)
        s1 = jnp.where(row >= 1, pltpu.roll(centre, 2, 1), 0.0)
        s2 = jnp.where(row >= 2, pltpu.roll(centre, 4, 1), 0.0)
        mixed = lax.dot_general(single[...], split(centre), (((1,), (0,)), ((), ())), preferred_element_type=jnp.float32)
        own = jnp.where(lane < 64, fixed_in[1, 0:channels, :], pltpu.roll(fixed_in[0, 0:channels, :], 64, 1))
        value = (own - theta) * centre + mixed
        value = value + (edge_coef(0) * e1 + edge_coef(1) * w1 + edge_coef(2) * (low - high))
        return value + (edge_coef(3) * n1 + edge_coef(4) * s1 + edge_coef(5) * (s2 - n2))

    def edge_turn(corners):
        n1 = jnp.where(row < lat - 1, 0.0, pltpu.roll(corners, 126, 1))
        n2 = jnp.where(row < lat - 2, 0.0, pltpu.roll(corners, 124, 1))
        s1 = jnp.where(row >= 1, 0.0, pltpu.roll(corners, 2, 1))
        s2 = jnp.where(row >= 2, 0.0, pltpu.roll(corners, 4, 1))
        return edge_coef(3) * n1 + edge_coef(4) * s1 + edge_coef(5) * (s2 - n2)

    def add_sides(k, centre):
        def own(q):
            return jnp.where(spot[0:1] < 64, fixed_out[0, channels + q:channels + q + 1, :],
                             pltpu.roll(fixed_out[1, channels + q:channels + q + 1, :], 64, 1))

        from_west = own(2) * centre + jnp.where(even, own(1) * pltpu.roll(centre, 127, 1), 0.0)
        from_east = jnp.where(even, 0.0, own(0) * pltpu.roll(centre, 1, 1)) - own(2) * centre
        for r in range(lat):
            left = pltpu.roll(from_west, (128 - 2 * r) % 128, 1) if r else from_west
            right = pltpu.roll(from_east, (62 - 2 * r) % 128, 1) if 2 * r != 62 else from_east
            basis[k + 1, r + HALO, :, 0:128] += jnp.where(lane < 2, left, 0.0)
            basis[k + 1, r + HALO, :, lon - 128:lon] += jnp.where(lane >= 126, right, 0.0)

    def stage(b, _):
        k = 2 * b
        theta, after = theta_of(k), theta_of(k + 1)
        for g in range((lat - 4) // GROUP):
            rows(k, [2 + GROUP * g + j for j in range(GROUP)], theta, None)
        rows(k, (0, 1, lat - 2, lat - 1), theta, None, bare=True)

        @pl.when(b > 0)
        def _():
            dots(k - 1, 0, lat)

        dots(k, 0, lat)
        lon_copy(b, 0).wait()
        lon_copy(b, 1).wait()

        @pl.when(b == 0)
        def _():
            fix_side(0).wait()
            fix_side(1).wait()

        centre = middle(b)
        add_sides(k, centre)
        band[...] = edge_band(b, theta, centre)
        beside = band[...]
        for g in range((lat - 8) // GROUP):
            rows(k + 1, [4 + GROUP * g + j for j in range(GROUP)], after, beside)

        @pl.when(b + 1 == BLOCKS)
        def _():
            dots(k + 1, 4, lat - 8)
            dots(k + 2, 4, lat - 8)

        def corners_in(way):
            turn_copy(b, way, 0).wait_recv()
            turn_copy(b, way, 1).wait_recv()

            @pl.when(b == 0)
            def _():
                for copy in wind_copies(way):
                    copy.wait_recv()
                fill_coef(wind_in[0, way], wind_in[1, way], kx_in[way, 6:8] if way else kx_in[way, 0:2], 0 if way else lat + 2)

        arrive_lat(corners_in)
        turned[0] = take_corners(b)
        turned[1] = band[...] + edge_turn(turned[0])
        arrive_lat(lambda way: lat_copy(b, way, 1).wait_recv())
        beside = turned[1]
        south, north = basis[k, HALO - 1], basis[k, HALO + lat]
        basis[k + 1, HALO] += coef[2, 4:5, :] * south + coef[2, 5:6, :] * basis[k, HALO - 2]
        basis[k + 1, HALO + 1] += coef[3, 5:6, :] * south
        basis[k + 1, HALO + lat - 1] += coef[lat + 1, 3:4, :] * north - coef[lat + 1, 5:6, :] * basis[k, HALO + lat + 1]
        basis[k + 1, HALO + lat - 2] -= coef[lat, 5:6, :] * north
        rows(k + 1, (2, 3, lat - 4, lat - 3), after, beside)
        more = b + 1 < BLOCKS

        @pl.when(more)
        def _():
            each_lat(lambda way: lat_copy(b + 1, way, 0).start())

        def far_in(way):
            lat_copy(b, way, 0).wait_recv()

            @pl.when(b == 0)
            def _():
                diag_copy(way).wait_recv()

        arrive_lat(far_in)
        rows(k, (-2, -1, lat, lat + 1), theta, turned[0])
        rows(k + 1, (0, 1, lat - 2, lat - 1), after, turned[1])

        @pl.when(more)
        def _():
            send_corners(b + 1)
            each_lat(lambda way: lat_copy(b + 1, way, 1).start())
            send_sides(b + 1)

        for n in range(min(words, BLOCKS)):
            @pl.when(b == n)
            def _():
                if n:
                    hear_word(n - 1)
                spread_word(n)

        if words < BLOCKS:
            @pl.when(b == words)
            def _():
                hear_word(words - 1)

        def sent(way):
            lat_copy(b, way, 0).wait_send()
            lat_copy(b, way, 1).wait_send()
            turn_copy(b, way, 0).wait_send()
            turn_copy(b, way, 1).wait_send()

            @pl.when(b == 0)
            def _():
                for copy in wind_copies(way) + [diag_copy(way)]:
                    copy.wait_send()

        each_lat(sent)
        return 0

    for copy in loads[0]:
        copy.wait()
    pl.semaphore_wait(barrier, 2 + jnp.where(iy > 0, 3, 0) + jnp.where(iy < ny - 1, 3, 0))
    send_corners(0)

    def first_rows(way):
        lat_copy(0, way, 1).start()
        lat_copy(0, way, 0).start()

    each_lat(first_rows)
    send_sides(0)
    for copy in small:
        copy.wait()

    def first_winds(way):
        for copy in wind_copies(way):
            copy.start()

    each_lat(first_winds)
    place = (lax.broadcasted_iota(jnp.int32, (lat + 16, 128), 0) + iy * lat - 8).astype(jnp.float32)
    phi = -math.pi / 2 + (place + 0.5) * (math.pi / (lat * ny))
    kx = (DIFF_LON * scale) / (jnp.cos(phi) ** 2 + 0.1)
    kx_in[0] = kx[lat + 8:lat + 16]
    kx_in[1] = kx[0:8]
    fill_coef(wl_ref[...], wa_ref[...], kx[8:lat + 8], 2)
    for copy in loads[1]:
        copy.wait()

    def prepare(r, _):
        diag[r + 2] = diag[r + 2] * scale + coef[r + 2, 6:7, :]
        return 0

    for r in (0, 1, lat - 2, lat - 1):
        prepare(r, 0)
    each_lat(lambda way: diag_copy(way).start())
    lax.fori_loop(2, lat - 2, prepare, 0)
    fixed = [pack(lambda r, cut: diag[r + 2, :, cut], False, channels), pack(lambda r, cut: coef[r + 2, :, cut], False, 8)]
    for way in range(2):
        fixed_out[way, 0:channels, :] = fixed[0][way]
        fixed_out[way, channels:channels + 8, :] = fixed[1][way]
    fix_side(0).start()
    fix_side(1).start()
    single[...] = widen(c_ref[...], channels)[0].astype(jnp.bfloat16)
    tall = lax.dot_general(spread(size), c_ref[...], (((1,), (0,)), ((), ())), precision=HI,
                           preferred_element_type=jnp.float32)
    wide, across = widen(tall, size)
    down = lax.broadcasted_iota(jnp.int32, (size, 3 * size), 0)
    block[...] = jnp.where(down // channels == lax.rem(across, size) // channels, wide, 0.0).astype(jnp.bfloat16)
    lax.fori_loop(0, BLOCKS, stage, 0)
    for n in range(BLOCKS, words + 1):
        hear_word(n - 1)
        if n < words:
            spread_word(n)
    dots_rest()

    sums = jnp.concatenate(
        [jnp.sum(gram_acc[n], axis=0, keepdims=True) for n in range(len(PAIRS))]
        + [jnp.zeros((128 - len(PAIRS), 128), jnp.float32)], axis=0)
    flat = lax.dot_general(jnp.ones((8, 128), jnp.float32), sums, (((1,), (1,)), ((), ())), precision=HI,
                           preferred_element_type=jnp.float32)
    mine[...] = flat[0:1, :]
    slots[me] = flat[0:1, :]

    def share(o):
        other = lax.rem(me + o, total)
        return pltpu.make_async_remote_copy(
            src_ref=mine, dst_ref=slots.at[me], send_sem=red_send.at[o], recv_sem=red_recv.at[me],
            device_id=(other // ny, lax.rem(other, ny)), device_id_type=MESH)

    def take(o):
        other = lax.rem(me + total - o, total)
        return pltpu.make_async_remote_copy(
            src_ref=mine, dst_ref=slots.at[other], send_sem=red_send.at[o], recv_sem=red_recv.at[other],
            device_id=(other // ny, lax.rem(other, ny)), device_id_type=MESH)

    def give(o, _):
        share(o).start()
        return 0

    def get(o, _):
        take(o).wait_recv()
        share(o).wait_send()
        return 0

    lax.fori_loop(1, total, give, 0)
    lax.fori_loop(1, total, get, 0)
    whole = slots[0]
    for n in range(1, total):
        whole = whole + slots[n]
    gram = [[None] * (ITERS + 1) for _ in range(ITERS + 1)]
    for n, (k, i) in enumerate(PAIRS):
        gram[k][i] = gram[i][k] = jnp.broadcast_to(whole[:, n:n + 1], (8, 128))
    answer, applied = small_solve(gram)
    for k in range(ITERS):
        splats[k] = answer[k]
    for k in range(ITERS + 1):
        splats[ITERS + k] = applied[k]


def finish(b_ref, w_ref, sol_hbm, res_hbm, outs, out_sem):
    channels, lat, lon = sol_hbm.shape
    stores = []
    for part in range(lat // 8):
        def one(j, _):
            r = 8 * part + j
            for h in range(channels // 8):
                for t in range(lon // 128):
                    at = (slice(8 * h, 8 * h + 8), slice(128 * t, 128 * t + 128))
                    x = b_ref[0, r + HALO, at[0], at[1]]
                    best = w_ref[0] * x
                    rest = x - w_ref[ITERS] * x
                    for k in range(1, ITERS + 1):
                        x = b_ref[k, r + HALO, at[0], at[1]]
                        if k < ITERS:
                            best = best + w_ref[k] * x
                        rest = rest - w_ref[ITERS + k] * x
                    outs[0, r, at[0], at[1]] = best
                    outs[1, r, at[0], at[1]] = rest
            return 0

        lax.fori_loop(0, 8, one, 0)
        for q, dst in enumerate((sol_hbm, res_hbm)):
            for c in range(channels):
                copy = pltpu.make_async_copy(outs.at[q, pl.ds(8 * part, 8), c, :], dst.at[c, pl.ds(8 * part, 8), :],
                                             out_sem.at[part, q, c])
                copy.start()
                stores.append(copy)
    for copy in stores:
        copy.wait()


def solution(mesh):
    nx, ny = mesh.shape["gx"], mesh.shape["gy"]

    def per_device(forcing, damping, coupling, wind_lon, wind_lat):
        channels, lat, lon = forcing.shape
        f32 = jnp.float32
        vmem = pl.BlockSpec(memory_space=pltpu.VMEM)
        hbm = pl.BlockSpec(memory_space=pltpu.HBM)
        dma = pltpu.SemaphoreType.DMA

        def keep(v):
            return pltpu.with_memory_space_constraint(v, pltpu.HBM)

        basis, weights = pl.pallas_call(
            functools.partial(kernel, nx, ny),
            out_shape=(pltpu.VMEM((ITERS + 1, lat + 2 * HALO, channels, lon), f32), pltpu.VMEM((2 * ITERS + 1, 8, 128), f32)),
            in_specs=[hbm] * 5,
            out_specs=(vmem, vmem),
            scratch_shapes=[
                pltpu.VMEM((lat + 4, channels, lon), f32),
                pltpu.VMEM((lat + 4, 8, lon), f32),
                pltpu.VMEM((GROUP * channels, 3 * GROUP * channels), jnp.bfloat16),
                pltpu.VMEM((channels, 3 * channels), jnp.bfloat16),
                pltpu.VMEM((BLOCKS, 2, channels, 128), f32),
                pltpu.VMEM((BLOCKS, 2, channels, 128), f32),
                pltpu.VMEM((channels, 128), f32),
                pltpu.VMEM((2, channels + 8, 128), f32),
                pltpu.VMEM((2, channels + 8, 128), f32),
                pltpu.VMEM((BLOCKS, 4, 2, 128), f32),
                pltpu.VMEM((BLOCKS, 2, 128), f32),
                pltpu.VMEM((len(PAIRS), 8, 128), f32),
                pltpu.VMEM((1, 128), f32),
                pltpu.VMEM((nx * ny, 1, 128), f32),
                pltpu.VMEM((channels, channels), f32), pltpu.VMEM((lat, lon), f32), pltpu.VMEM((lat, lon), f32),
                pltpu.VMEM((2, 2, 2, lon), f32), pltpu.VMEM((2, 8, 128), f32), pltpu.VMEM((2, channels, 128), f32),
                dma((2, channels)), dma((3,)),
                dma((BLOCKS, 2, 2)), dma((BLOCKS, 2, 2)), dma((BLOCKS, 2)), dma((BLOCKS, 2)),
                dma((BLOCKS, 4)), dma((BLOCKS, 4)), dma((4, 2)), dma((4, 2)),
                dma((nx * ny,)), dma((nx * ny,)), pltpu.SemaphoreType.REGULAR((8,)),
            ],
            compiler_params=pltpu.CompilerParams(
                collective_id=0, has_side_effects=True, vmem_limit_bytes=24 * 1024 * 1024),
        )(*map(keep, (forcing, damping, coupling, wind_lon, wind_lat)))
        shape = jax.ShapeDtypeStruct((channels, lat, lon), f32)
        return pl.pallas_call(
            finish,
            out_shape=(shape, shape),
            in_specs=[vmem, vmem],
            out_specs=(hbm, hbm),
            scratch_shapes=[pltpu.VMEM((2, lat, channels, lon), f32), dma((lat // 8, 2, channels))],
            compiler_params=pltpu.CompilerParams(vmem_limit_bytes=24 * 1024 * 1024),
        )(basis, weights)

    return jax.shard_map(
        per_device,
        mesh=mesh,
        in_specs=(P(None, "gy", "gx"), P(None, "gy", "gx"), P(), P("gy", "gx"), P("gy", "gx")),
        out_specs=(P(None, "gy", "gx"), P(None, "gy", "gx")),
        check_vma=False,
    )
```

```python
import functools
import math

import jax
import jax.numpy as jnp
from jax import lax
from jax.experimental import pallas as pl
from jax.experimental.pallas import tpu as pltpu
from jax.sharding import PartitionSpec as P

ITERS = 8
COUPLE = 0.25
DIFF_LAT = 0.5
DIFF_LON = 0.5
GUARD = 1.0
MESH = pl.DeviceIdType.MESH
HI = lax.Precision.HIGHEST

MIDDLE = 9.0
RADIUS = 6.0
WIDTH = 3.0
THETA = [MIDDLE + RADIUS * math.cos(math.pi * (2 * k + 1) / (2 * ITERS)) for k in (7, 0, 4, 2, 6, 1, 5, 3)]
PAIRS = [(k, i) for k in range(ITERS + 1) for i in range(k + 1)]
GROUP = 4
HALO = 4
BLOCKS = ITERS // 2


def apply_to(coords):
    out = [None] * (len(coords) + 1)
    for k, value in enumerate(coords):
        low = THETA[k] * value if k < ITERS else value
        out[k] = low if out[k] is None else out[k] + low
        out[k + 1] = WIDTH * value
    return out


def tree(terms):
    while len(terms) > 1:
        terms = [a + b for a, b in zip(terms[::2], terms[1::2])] + ([terms[-1]] if len(terms) % 2 else [])
    return terms[0]


def small_solve(gram):
    first = jnp.sqrt(gram[0][0] + GUARD)
    coords = [[1.0 / first]]
    images = [[gram[i][0] * coords[0][0] for i in range(ITERS + 1)]]
    heights = []
    for j in range(ITERS):
        moved = apply_to(coords[j])
        column = []
        for i in range(j + 1):
            column.append(functools.reduce(lambda a, b: a + b, [images[i][k] * moved[k] for k in range(j + 2)]))
        left = list(moved)
        for i in range(j + 1):
            for k in range(i + 1):
                left[k] = left[k] - column[i] * coords[i][k]
        image = [
            functools.reduce(lambda a, b: a + b, [gram[r][k] * left[k] for k in range(j + 2)])
            for r in range(ITERS + 1)
        ]
        norm_sq = functools.reduce(lambda a, b: a + b, [image[k] * left[k] for k in range(j + 2)])
        subdiag = jnp.sqrt(jnp.maximum(norm_sq, 0.0) + GUARD)
        column.append(subdiag)
        heights.append(column)
        inverse = 1.0 / subdiag
        coords.append([v * inverse for v in left])
        images.append([v * inverse for v in image])
    cosines, sines, target, rotated = [], [], [first], []
    for j in range(ITERS):
        column = list(heights[j])
        for e in range(j):
            upper, lower = column[e], column[e + 1]
            column[e] = cosines[e] * upper + sines[e] * lower
            column[e + 1] = cosines[e] * lower - sines[e] * upper
        upper, lower = column[j], column[j + 1]
        radius = jnp.sqrt(upper * upper + lower * lower)
        inverse = 1.0 / radius
        cosine, sine = upper * inverse, lower * inverse
        column[j] = radius
        kept = target[j]
        target[j] = cosine * kept
        target.append(-sine * kept)
        cosines.append(cosine)
        sines.append(sine)
        rotated.append(column)
    weights = [None] * ITERS
    for j in reversed(range(ITERS)):
        value = target[j]
        for later in range(j + 1, ITERS):
            value = value - rotated[later][j] * weights[later]
        weights[j] = value / rotated[j][j]
    answer = [None] * ITERS
    for j in range(ITERS):
        for k in range(j + 1):
            term = weights[j] * coords[j][k]
            answer[k] = term if answer[k] is None else answer[k] + term
    return answer, apply_to(answer)


def word_plan(nx, ny):
    def doubled(n):
        out = [2]
        while out[-1] < n:
            out.append(2 * out[-1])
        return out[:-1]

    far_lat, far_lon = doubled(ny), doubled(nx // 2 + 1)
    words = max(len(far_lat), len(far_lon))
    reach = {}
    for x in range(nx):
        for y in range(ny):
            reach[x, y] = {((x + dx) % nx, y + dy) for dx in (-1, 0, 1) for dy in (-1, 0, 1) if 0 <= y + dy < ny}
    near = {place: set(known) for place, known in reach.items()}

    def peers(x, y, n):
        out = []
        if n < len(far_lat):
            out += [(x, y + d) for d in (-far_lat[n], far_lat[n]) if 0 <= y + d < ny]
        if n < len(far_lon):
            out += [((x + d) % nx, y) for d in (-far_lon[n], far_lon[n])]
        return out

    told = None
    for n in range(BLOCKS):
        before = reach
        reach = {place: set().union(*(before[other] for other in near[place])) for place in before}
        if told is not None:
            reach = {place: known.union(*(told[other] for other in peers(*place, n - 1))) for place, known in reach.items()}
        told = reach
    if any(len(known) < nx * ny for known in reach.values()):
        far_lon = far_lon + [nx // 2] * (max(BLOCKS, words + 1) - len(far_lon))
    return far_lat, far_lon


def kernel(nx, ny, f_hbm, d_hbm, c_hbm, wl_hbm, wa_hbm, basis, splats,
           diag, coef, block, single, side_in, side_out, band, fixed_in, fixed_out, corner_in, corner_out,
           gram_acc, slots, c_ref, wl_ref, wa_ref, wind_in, kx_in, turned,
           in_sem, wind_sem, lat_send, lat_recv, lon_send, lon_recv, turn_send, turn_recv, fix_send, fix_recv, red_send, red_recv, word):
    channels, lat, lon = f_hbm.shape
    tiles = lon // 128
    total = nx * ny
    ix, iy = lax.axis_index("gx"), lax.axis_index("gy")
    me = ix * ny + iy
    east, west = lax.rem(ix + 1, nx), lax.rem(ix + nx - 1, nx)

    small = [pltpu.make_async_copy(src, dst, wind_sem.at[n])
             for n, (src, dst) in enumerate(((wl_hbm, wl_ref), (wa_hbm, wa_ref), (c_hbm, c_ref)))]
    for copy in small:
        copy.start()
    loads = [[], []]
    for q, (src, dst, off) in enumerate(((f_hbm, basis.at[0], HALO), (d_hbm, diag, 2))):
        for c in range(channels):
            copy = pltpu.make_async_copy(src.at[c], dst.at[pl.ds(off, lat), c, :], in_sem.at[q, c])
            copy.start()
            loads[q].append(copy)

    barrier = pltpu.get_barrier_semaphore()

    def greet(to, sem=barrier):
        pl.semaphore_signal(sem, inc=1, device_id=to, device_id_type=MESH)

    greet((east, iy))
    greet((west, iy))

    def greet_lat(to):
        greet((ix, to))
        greet((east, to))
        greet((west, to))

    @pl.when(iy > 0)
    def _():
        greet_lat(iy - 1)

    @pl.when(iy < ny - 1)
    def _():
        greet_lat(iy + 1)

    far_lat, far_lon = word_plan(nx, ny)

    def spread_word(n):
        if n < len(far_lat):
            d = far_lat[n]

            @pl.when(iy >= d)
            def _():
                greet((ix, iy - d), word.at[n])

            @pl.when(iy + d < ny)
            def _():
                greet((ix, iy + d), word.at[n])

        if n < len(far_lon):
            greet((lax.rem(ix + far_lon[n], nx), iy), word.at[n])
            greet((lax.rem(ix + nx - far_lon[n], nx), iy), word.at[n])

    def hear_word(n):
        count = 2 if n < len(far_lon) else 0
        if n < len(far_lat):
            d = far_lat[n]
            count = count + jnp.where(iy >= d, 1, 0) + jnp.where(iy + d < ny, 1, 0)
        pl.semaphore_wait(word.at[n], count)

    words = max(len(far_lat), len(far_lon))

    scale = 1.0 / WIDTH
    size = GROUP * channels

    def spread(n):
        row = lax.broadcasted_iota(jnp.int32, (n, channels), 0)
        col = lax.broadcasted_iota(jnp.int32, (n, channels), 1)
        return jnp.where(lax.rem(row, channels) == col, 1.0, 0.0).astype(jnp.float32)

    def widen(tall, n):
        wide = lax.dot_general(tall, spread(3 * n), (((1,), (1,)), ((), ())), precision=HI,
                               preferred_element_type=jnp.float32) * (COUPLE * scale)
        across = lax.broadcasted_iota(jnp.int32, wide.shape, 1)
        high = wide.astype(jnp.bfloat16).astype(jnp.float32)
        return jnp.where(across < 2 * n, high, wide - high), across

    def blank(at):
        for b in range(BLOCKS):
            basis[2 * b, pl.ds(HALO + lat if at else 0, HALO)] = jnp.zeros((HALO, channels, lon), jnp.float32)
        diag[pl.ds(lat + 2 if at else 0, 2)] = jnp.zeros((2, channels, lon), jnp.float32)
        coef[pl.ds(lat + 2 if at else 0, 2)] = jnp.zeros((2, 8, lon), jnp.float32)
        corner_in[:, 0 if at else 2] = jnp.zeros((BLOCKS, 2, 128), jnp.float32)
        corner_in[:, 1 if at else 3] = jnp.zeros((BLOCKS, 2, 128), jnp.float32)

    @pl.when(iy == 0)
    def _():
        blank(0)

    @pl.when(iy == ny - 1)
    def _():
        blank(1)

    def fill_coef(wl, wa, kx, at):
        wl, wa = wl * (scale / 12.0), wa * (scale / 12.0)
        kx = jnp.concatenate([kx] * tiles, axis=1)
        planes = (8.0 * wl - kx, -8.0 * wl - kx, wl, 8.0 * wa - DIFF_LAT * scale, -8.0 * wa - DIFF_LAT * scale, wa,
                  2.0 * kx + (1.0 + 2.0 * DIFF_LAT) * scale, jnp.zeros_like(kx))
        for q, plane in enumerate(planes):
            for r in range(wl.shape[0]):
                coef[r + at, q:q + 1, :] = plane[r:r + 1, :]

    def pack(read, far, n, picked=None):
        lane = lax.broadcasted_iota(jnp.int32, (n, 128), 1)
        to_west = to_east = jnp.zeros((n, 128), jnp.float32)
        for r in picked or range(lat):
            head = read(r, slice(0, 128))
            tail = read(r, slice(lon - 128, lon))
            here = (lane >= 2 * r) & (lane < 2 * r + 2)
            to_west = jnp.where(here, pltpu.roll(head, 2 * r, 1) if r else head, to_west)
            to_east = jnp.where(here, pltpu.roll(tail, (2 * r + 2) % 128, 1), to_east)
            if far:
                here = (lane >= 64 + 2 * r) & (lane < 64 + 2 * r + 2)
                to_west = jnp.where(here, pltpu.roll(head, (62 + 2 * r) % 128, 1), to_west)
                to_east = jnp.where(here, pltpu.roll(tail, (68 + 2 * r) % 128, 1), to_east)
        return to_west, to_east

    lane = lax.broadcasted_iota(jnp.int32, (channels, 128), 1)
    spot = lax.broadcasted_iota(jnp.int32, (8, 128), 1)
    deep = lax.broadcasted_iota(jnp.int32, (8, 128), 0)

    def copy_to(src, dst, send, recv, to):
        return pltpu.make_async_remote_copy(src_ref=src, dst_ref=dst, send_sem=send, recv_sem=recv,
                                            device_id=to, device_id_type=MESH)

    def lat_to(way):
        return iy + 1 if way else iy - 1

    def lat_copy(b, way, near):
        if way:
            src, dst = HALO + lat - (2 if near else 4), 2 if near else 0
        else:
            src, dst = HALO + (0 if near else 2), HALO + lat + (0 if near else 2)
        return copy_to(basis.at[2 * b, pl.ds(src, 2)], basis.at[2 * b, pl.ds(dst, 2)], lat_send.at[b, way, near],
                       lat_recv.at[b, way, near], (ix, lat_to(way)))

    def diag_copy(way):
        src = pl.ds(lat, 2) if way else pl.ds(2, 2)
        dst = pl.ds(0, 2) if way else pl.ds(lat + 2, 2)
        return copy_to(diag.at[src], diag.at[dst], fix_send.at[0, way], fix_recv.at[0, way], (ix, lat_to(way)))

    def wind_copies(way):
        src = pl.ds(lat - 2, 2) if way else pl.ds(0, 2)
        return [copy_to(ref.at[src], wind_in.at[n, way], fix_send.at[1 + n, way], fix_recv.at[1 + n, way], (ix, lat_to(way)))
                for n, ref in enumerate((wl_ref, wa_ref))]

    def fix_side(way):
        return copy_to(fixed_out.at[way], fixed_in.at[way], fix_send.at[3, way], fix_recv.at[3, way],
                       (east if way else west, iy))

    def lon_copy(b, part, way):
        return copy_to(side_out.at[b, part, way], side_in.at[b, part, way], lon_send.at[b, part, way],
                       lon_recv.at[b, part, way], (east if way else west, iy))

    sided = (list(range(4, lat - 4)), list(range(4)) + list(range(lat - 4, lat)))

    def turn_copy(b, up, way):
        n = 2 * up + way
        return copy_to(corner_out.at[b], corner_in.at[b, n], turn_send.at[b, n], turn_recv.at[b, n],
                       (east if way else west, lat_to(up)))

    def each_lat(act):
        @pl.when(iy < ny - 1)
        def _():
            act(1)

        @pl.when(iy > 0)
        def _():
            act(0)

    def arrive_lat(act):
        @pl.when(iy > 0)
        def _():
            act(1)

        @pl.when(iy < ny - 1)
        def _():
            act(0)

    def send_corners(b):
        k = 2 * b
        small = jnp.zeros((8, 128), jnp.float32)
        for up in range(2):
            for way in range(2):
                for h in range(channels // 8):
                    for j in range(2):
                        at = 16 * up + 8 * way + 4 * h + 2 * j
                        here = (spot >= at) & (spot < at + 2)
                        cut = slice(lon - 128, lon) if way else slice(0, 128)
                        part = basis[k, HALO + (lat - 2 if up else 0) + j, 8 * h:8 * h + 8, cut]
                        move = (at - (126 if way else 0)) % 128
                        small = jnp.where(here, pltpu.roll(part, move, 1) if move else part, small)
        dense = small
        for g in range(1, 4):
            moved = pltpu.roll(pltpu.roll(small, 8 - 2 * g, 0), 32 * g, 1)
            dense = jnp.where(spot // 32 == g, moved, dense)
        corner_out[b] = dense[0:2, :]

        def go(up):
            turn_copy(b, up, 0).start()
            turn_copy(b, up, 1).start()

        each_lat(go)

    def send_sides(b, part):
        k = 2 * b
        to_west, to_east = pack(lambda r, cut: basis[k, r + HALO, :, cut], True, channels, sided[part])
        side_out[b, part, 0] = to_west
        side_out[b, part, 1] = to_east
        lon_copy(b, part, 0).start()
        lon_copy(b, part, 1).start()

    def take_corners(b):
        got = jnp.zeros((2, 128), jnp.float32)
        sub = lax.rem(lax.broadcasted_iota(jnp.int32, (2, 128), 1), 32) // 8
        for n in range(4):
            got = jnp.where(sub == n, corner_in[b, n], got)
        got = jnp.concatenate([got] * 4, axis=0)
        small = got
        for g in range(1, 4):
            small = jnp.where(deep // 2 == g, pltpu.roll(got, 128 - 32 * g, 1), small)
        parts = []
        for h in range(channels // 8):
            part = jnp.zeros((8, 128), jnp.float32)
            for up in range(2):
                for way in range(2):
                    at = 16 * up + 8 * way + 4 * h
                    want = (64 if way else 0) + (2 * lat - 4 if up else 0)
                    here = (spot >= want) & (spot < want + 4)
                    part = jnp.where(here, pltpu.roll(small, (want - at) % 128, 1) if want != at else small, part)
            parts.append(part)
        return jnp.concatenate(parts, axis=0)

    def theta_of(k):
        theta = jnp.float32(THETA[0] * scale)
        for i in range(1, ITERS):
            theta = jnp.where(k == i, jnp.float32(THETA[i] * scale), theta)
        return theta

    def products(pairs, places, accs):
        for r in places:
            for h in range(channels // 8):
                for t in range(tiles):
                    at = (r + HALO, slice(8 * h, 8 * h + 8), slice(128 * t, 128 * t + 128))
                    held = {}

                    def read(k):
                        if id(k) not in held:
                            held[id(k)] = basis[(k,) + at]
                        return held[id(k)]

                    for n, (k, i) in enumerate(pairs):
                        m = (2 * h + t) % 2
                        accs[2 * n + m] = accs[2 * n + m] + read(k) * read(i)
        return accs

    def keep(k, i, acc, more):
        at = lax.div(k * (k + 1), 2) + i
        gram_acc[at] = gram_acc[at] + acc if more else acc

    def dots(pairs, first, count, more=False):
        zero = jnp.zeros((8, 128), jnp.float32)
        if count == 8:
            accs = products(pairs, [(j + first) % lat for j in range(8)],
                            [zero] * (2 * len(pairs)))
        else:
            def part(b, accs):
                return tuple(products(pairs, [b * 8 + j + first for j in range(8)], list(accs)))

            accs = lax.fori_loop(0, count // 8, part, (zero,) * (2 * len(pairs)))
        for n, (k, i) in enumerate(pairs):
            keep(k, i, accs[2 * n] + accs[2 * n + 1], more)

    def dots_two(k, first, count, more=False):
        def one(i, _):
            before = k - 1
            dots([(before, i), (k, i)], first, count, more)
            return 0

        lax.fori_loop(0, k, one, 0)
        dots([(k, k)], first, count, more)

    def split(stack):
        high = stack.astype(jnp.bfloat16)
        low = (stack - high.astype(jnp.float32)).astype(jnp.bfloat16)
        return jnp.concatenate([high, low, high], axis=0)

    def rows(k, picked, theta, beside, bare=False):
        stack = jnp.concatenate([basis[k, r + HALO] for r in picked], axis=0)
        mixed = lax.dot_general(block[...], split(stack), (((1,), (0,)), ((), ())), preferred_element_type=jnp.float32)
        for j, r in enumerate(picked):
            inside = 0 <= r < lat
            source = beside
            left = 2 * r if inside else 64 + 2 * (r % lat)
            right = 64 + 2 * r if inside else 2 * (r % lat)

            def turn(v, shift):
                return pltpu.roll(v, shift % 128, 1) if shift % 128 else v

            x = [basis[k, r + HALO, :, 128 * t:128 * t + 128] for t in range(tiles)]
            if source is None:
                ends = [jnp.zeros_like(lane, jnp.float32)] * 4
            else:
                ends = [turn(source, shift) for shift in (127 - right, 126 - right, -left - 1, -left)]
            fwd1 = [pltpu.roll(v, 127, 1) for v in x] + [ends[0]]
            fwd2 = [pltpu.roll(v, 126, 1) for v in x] + [ends[1]]
            bwd1 = [ends[2]] + [pltpu.roll(v, 1, 1) for v in x]
            bwd2 = [ends[3]] + [pltpu.roll(v, 2, 1) for v in x]
            for t in range(tiles):
                cut = slice(128 * t, 128 * t + 128)
                e1 = jnp.where(lane < 127, fwd1[t], fwd1[t + 1])
                e2 = jnp.where(lane < 126, fwd2[t], fwd2[t + 1])
                w1 = jnp.where(lane >= 1, bwd1[t + 1], bwd1[t])
                w2 = jnp.where(lane >= 2, bwd2[t + 1], bwd2[t])

                def weight(q):
                    return coef[r + 2, q:q + 1, cut]

                def near(d):
                    return basis[k, r + HALO + d, :, cut]

                def has(d):
                    return not bare or 0 <= r + d < lat

                value = (diag[r + 2, :, cut] - theta) * x[t] + mixed[channels * j:channels * (j + 1), cut]
                value = value + (weight(0) * e1 + weight(1) * w1 + weight(2) * (w2 - e2))
                if has(1):
                    value = value + weight(3) * near(1)
                if has(-1):
                    value = value + weight(4) * near(-1)
                if has(2) and has(-2):
                    value = value + weight(5) * (near(-2) - near(2))
                elif has(2):
                    value = value - weight(5) * near(2)
                else:
                    value = value + weight(5) * near(-2)
                basis[k + 1, r + HALO, :, cut] = value

    def middle(got):
        return jnp.where(lane < 64, got[1], pltpu.roll(got[0], 64, 1))

    def both(ref, b, part):
        return [ref[b, 0, way] + ref[b, 1, way] if part else ref[b, 0, way] for way in range(2)]

    row = lax.rem(lane, 64) // 2
    even = lax.rem(lane, 2) == 0

    def edge_coef(q):
        return jnp.where(spot[0:1] < 64, fixed_in[1, channels + q:channels + q + 1, :],
                         pltpu.roll(fixed_in[0, channels + q:channels + q + 1, :], 64, 1))

    def edge_band(got, given, theta, centre):
        from_east, from_west = got
        to_west, to_east = given
        low = jnp.where(lane < 64, pltpu.roll(from_west, 64, 1), pltpu.roll(to_east, 64, 1))
        high = jnp.where(lane < 64, to_west, from_east)
        e1 = jnp.where(even, pltpu.roll(centre, 127, 1), pltpu.roll(high, 1, 1))
        w1 = jnp.where(even, pltpu.roll(low, 127, 1), pltpu.roll(centre, 1, 1))
        n1 = jnp.where(row < lat - 1, pltpu.roll(centre, 126, 1), 0.0)
        n2 = jnp.where(row < lat - 2, pltpu.roll(centre, 124, 1), 0.0)
        s1 = jnp.where(row >= 1, pltpu.roll(centre, 2, 1), 0.0)
        s2 = jnp.where(row >= 2, pltpu.roll(centre, 4, 1), 0.0)
        mixed = lax.dot_general(single[...], split(centre), (((1,), (0,)), ((), ())), preferred_element_type=jnp.float32)
        own = jnp.where(lane < 64, fixed_in[1, 0:channels, :], pltpu.roll(fixed_in[0, 0:channels, :], 64, 1))
        value = (own - theta) * centre + mixed
        value = value + (edge_coef(0) * e1 + edge_coef(1) * w1 + edge_coef(2) * (low - high))
        return value + (edge_coef(3) * n1 + edge_coef(4) * s1 + edge_coef(5) * (s2 - n2))

    def edge_turn(corners):
        n1 = jnp.where(row < lat - 1, 0.0, pltpu.roll(corners, 126, 1))
        n2 = jnp.where(row < lat - 2, 0.0, pltpu.roll(corners, 124, 1))
        s1 = jnp.where(row >= 1, 0.0, pltpu.roll(corners, 2, 1))
        s2 = jnp.where(row >= 2, 0.0, pltpu.roll(corners, 4, 1))
        return edge_coef(3) * n1 + edge_coef(4) * s1 + edge_coef(5) * (s2 - n2)

    def add_sides(k, centre, picked):
        def own(q):
            return jnp.where(spot[0:1] < 64, fixed_out[0, channels + q:channels + q + 1, :],
                             pltpu.roll(fixed_out[1, channels + q:channels + q + 1, :], 64, 1))

        from_west = own(2) * centre + jnp.where(even, own(1) * pltpu.roll(centre, 127, 1), 0.0)
        from_east = jnp.where(even, 0.0, own(0) * pltpu.roll(centre, 1, 1)) - own(2) * centre
        for r in picked:
            left = pltpu.roll(from_west, (128 - 2 * r) % 128, 1) if r else from_west
            right = pltpu.roll(from_east, (62 - 2 * r) % 128, 1) if 2 * r != 62 else from_east
            basis[k + 1, r + HALO, :, 0:128] += jnp.where(lane < 2, left, 0.0)
            basis[k + 1, r + HALO, :, lon - 128:lon] += jnp.where(lane >= 126, right, 0.0)

    def stage(b, _):
        k = 2 * b
        theta, after = theta_of(k), theta_of(k + 1)
        for g in range((lat - 4) // GROUP):
            rows(k, [2 + GROUP * g + j for j in range(GROUP)], theta, None)
        rows(k, (0, 1, lat - 2, lat - 1), theta, None, bare=True)

        dots_two(k, 0, lat)
        more = b + 1 < BLOCKS
        for part in range(2):
            lon_copy(b, part, 0).wait()
            lon_copy(b, part, 1).wait()
            if part == 0:
                @pl.when(b == 0)
                def _():
                    fix_side(0).wait()
                    fix_side(1).wait()

            got = both(side_in, b, part)
            centre = middle(got)
            add_sides(k, centre, sided[part])
            band[...] = edge_band(got, both(side_out, b, part), theta, centre)
            beside = band[...]
            if part:
                rows(k + 1, (4, 5, lat - 6, lat - 5), after, beside)
            else:
                for g in range((lat - 12) // GROUP):
                    rows(k + 1, [6 + GROUP * g + j for j in range(GROUP)], after, beside)

        @pl.when(more)
        def _():
            send_sides(b + 1, 0)

        @pl.when(b + 1 == BLOCKS)
        def _():
            dots_two(k + 2, 4, lat - 8)

        def corners_in(way):
            turn_copy(b, way, 0).wait_recv()
            turn_copy(b, way, 1).wait_recv()

            @pl.when(b == 0)
            def _():
                for copy in wind_copies(way):
                    copy.wait_recv()
                fill_coef(wind_in[0, way], wind_in[1, way], kx_in[way, 6:8] if way else kx_in[way, 0:2], 0 if way else lat + 2)

        arrive_lat(corners_in)
        turned[0] = take_corners(b)
        turned[1] = band[...] + edge_turn(turned[0])
        arrive_lat(lambda way: lat_copy(b, way, 1).wait_recv())
        beside = turned[1]
        south, north = basis[k, HALO - 1], basis[k, HALO + lat]
        basis[k + 1, HALO] += coef[2, 4:5, :] * south + coef[2, 5:6, :] * basis[k, HALO - 2]
        basis[k + 1, HALO + 1] += coef[3, 5:6, :] * south
        basis[k + 1, HALO + lat - 1] += coef[lat + 1, 3:4, :] * north - coef[lat + 1, 5:6, :] * basis[k, HALO + lat + 1]
        basis[k + 1, HALO + lat - 2] -= coef[lat, 5:6, :] * north
        rows(k + 1, (2, 3, lat - 4, lat - 3), after, beside)

        @pl.when(more)
        def _():
            each_lat(lambda way: lat_copy(b + 1, way, 0).start())

        def far_in(way):
            lat_copy(b, way, 0).wait_recv()

            @pl.when(b == 0)
            def _():
                diag_copy(way).wait_recv()

        arrive_lat(far_in)
        rows(k, (-2, -1, lat, lat + 1), theta, turned[0])
        rows(k + 1, (0, 1, lat - 2, lat - 1), after, turned[1])

        @pl.when(more)
        def _():
            send_corners(b + 1)
            each_lat(lambda way: lat_copy(b + 1, way, 1).start())
            send_sides(b + 1, 1)

        for n in range(min(words, BLOCKS)):
            @pl.when(b == n)
            def _():
                if n:
                    hear_word(n - 1)
                spread_word(n)

        if words < BLOCKS:
            @pl.when(b == words)
            def _():
                hear_word(words - 1)

        def sent(way):
            lat_copy(b, way, 0).wait_send()
            lat_copy(b, way, 1).wait_send()
            turn_copy(b, way, 0).wait_send()
            turn_copy(b, way, 1).wait_send()

            @pl.when(b == 0)
            def _():
                for copy in wind_copies(way) + [diag_copy(way)]:
                    copy.wait_send()

        each_lat(sent)
        return 0

    for copy in loads[0]:
        copy.wait()
    pl.semaphore_wait(barrier, 2 + jnp.where(iy > 0, 3, 0) + jnp.where(iy < ny - 1, 3, 0))
    send_corners(0)

    def first_rows(way):
        lat_copy(0, way, 1).start()
        lat_copy(0, way, 0).start()

    each_lat(first_rows)
    send_sides(0, 0)
    send_sides(0, 1)
    for copy in small:
        copy.wait()

    def first_winds(way):
        for copy in wind_copies(way):
            copy.start()

    each_lat(first_winds)
    place = (lax.broadcasted_iota(jnp.int32, (lat + 16, 128), 0) + iy * lat - 8).astype(jnp.float32)
    phi = -math.pi / 2 + (place + 0.5) * (math.pi / (lat * ny))
    kx = (DIFF_LON * scale) / (jnp.cos(phi) ** 2 + 0.1)
    kx_in[0] = kx[lat + 8:lat + 16]
    kx_in[1] = kx[0:8]
    fill_coef(wl_ref[...], wa_ref[...], kx[8:lat + 8], 2)
    for copy in loads[1]:
        copy.wait()

    def prepare(r, _):
        diag[r + 2] = diag[r + 2] * scale + coef[r + 2, 6:7, :]
        return 0

    for r in (0, 1, lat - 2, lat - 1):
        prepare(r, 0)
    each_lat(lambda way: diag_copy(way).start())
    lax.fori_loop(2, lat - 2, prepare, 0)
    fixed = [pack(lambda r, cut: diag[r + 2, :, cut], False, channels), pack(lambda r, cut: coef[r + 2, :, cut], False, 8)]
    for way in range(2):
        fixed_out[way, 0:channels, :] = fixed[0][way]
        fixed_out[way, channels:channels + 8, :] = fixed[1][way]
    fix_side(0).start()
    fix_side(1).start()
    single[...] = widen(c_ref[...], channels)[0].astype(jnp.bfloat16)
    tall = lax.dot_general(spread(size), c_ref[...], (((1,), (0,)), ((), ())), precision=HI,
                           preferred_element_type=jnp.float32)
    wide, across = widen(tall, size)
    down = lax.broadcasted_iota(jnp.int32, (size, 3 * size), 0)
    block[...] = jnp.where(down // channels == lax.rem(across, size) // channels, wide, 0.0).astype(jnp.bfloat16)
    lax.fori_loop(0, BLOCKS, stage, 0)
    for n in range(BLOCKS, words + 1):
        hear_word(n - 1)
        if n < words:
            spread_word(n)
    dots_two(ITERS, lat - 4, 8, True)

    sums = jnp.concatenate(
        [jnp.sum(gram_acc[n], axis=0, keepdims=True) for n in range(len(PAIRS))]
        + [jnp.zeros((128 - len(PAIRS), 128), jnp.float32)], axis=0)
    flat = lax.dot_general(jnp.ones((8, 128), jnp.float32), sums, (((1,), (1,)), ((), ())), precision=HI,
                           preferred_element_type=jnp.float32)
    slots[me] = flat[0:1, :]

    def share(to):
        return copy_to(slots.at[me], slots.at[me], red_send.at[0], red_recv.at[0], to)

    def wrap(v, n):
        return jnp.where(v >= n, v - n, v)

    for dx in range(nx):
        for dy in range(ny):
            if dx or dy:
                share((wrap(ix + dx, nx), wrap(iy + dy, ny))).start()
    others = slots.at[pl.ds(0, total - 1)]
    everyone = copy_to(others, others, red_send.at[0], red_recv.at[0], (east, iy))
    everyone.wait_recv()
    everyone.wait_send()
    whole = tree([slots[n] for n in range(total)])
    gram = [[None] * (ITERS + 1) for _ in range(ITERS + 1)]
    for n, (k, i) in enumerate(PAIRS):
        gram[k][i] = gram[i][k] = jnp.broadcast_to(whole[:, n:n + 1], (8, 128))
    answer, applied = small_solve(gram)
    for k in range(ITERS):
        splats[k] = answer[k]
    for k in range(ITERS + 1):
        splats[ITERS + k] = applied[k]


def finish(b_ref, w_ref, sol_hbm, res_hbm, outs, out_sem):
    channels, lat, lon = sol_hbm.shape
    stores = []
    for part in range(lat // 8):
        def one(j, _):
            r = 8 * part + j
            for h in range(channels // 8):
                for t in range(lon // 128):
                    at = (slice(8 * h, 8 * h + 8), slice(128 * t, 128 * t + 128))
                    x = b_ref[0, r + HALO, at[0], at[1]]
                    best = w_ref[0] * x
                    rest = x - w_ref[ITERS] * x
                    for k in range(1, ITERS + 1):
                        x = b_ref[k, r + HALO, at[0], at[1]]
                        if k < ITERS:
                            best = best + w_ref[k] * x
                        rest = rest - w_ref[ITERS + k] * x
                    outs[0, r, at[0], at[1]] = best
                    outs[1, r, at[0], at[1]] = rest
            return 0

        lax.fori_loop(0, 8, one, 0)
        for q, dst in enumerate((sol_hbm, res_hbm)):
            for c in range(channels):
                copy = pltpu.make_async_copy(outs.at[q, pl.ds(8 * part, 8), c, :], dst.at[c, pl.ds(8 * part, 8), :],
                                             out_sem.at[part, q, c])
                copy.start()
                stores.append(copy)
    for copy in stores:
        copy.wait()


def solution(mesh):
    nx, ny = mesh.shape["gx"], mesh.shape["gy"]

    def per_device(forcing, damping, coupling, wind_lon, wind_lat):
        channels, lat, lon = forcing.shape
        f32 = jnp.float32
        vmem = pl.BlockSpec(memory_space=pltpu.VMEM)
        hbm = pl.BlockSpec(memory_space=pltpu.HBM)
        dma = pltpu.SemaphoreType.DMA

        def keep(v):
            return pltpu.with_memory_space_constraint(v, pltpu.HBM)

        basis, weights = pl.pallas_call(
            functools.partial(kernel, nx, ny),
            out_shape=(pltpu.VMEM((ITERS + 1, lat + 2 * HALO, channels, lon), f32), pltpu.VMEM((2 * ITERS + 1, 8, 128), f32)),
            in_specs=[hbm] * 5,
            out_specs=(vmem, vmem),
            scratch_shapes=[
                pltpu.VMEM((lat + 4, channels, lon), f32),
                pltpu.VMEM((lat + 4, 8, lon), f32),
                pltpu.VMEM((GROUP * channels, 3 * GROUP * channels), jnp.bfloat16),
                pltpu.VMEM((channels, 3 * channels), jnp.bfloat16),
                pltpu.VMEM((BLOCKS, 2, 2, channels, 128), f32),
                pltpu.VMEM((BLOCKS, 2, 2, channels, 128), f32),
                pltpu.VMEM((channels, 128), f32),
                pltpu.VMEM((2, channels + 8, 128), f32),
                pltpu.VMEM((2, channels + 8, 128), f32),
                pltpu.VMEM((BLOCKS, 4, 2, 128), f32),
                pltpu.VMEM((BLOCKS, 2, 128), f32),
                pltpu.VMEM((len(PAIRS), 8, 128), f32),
                pltpu.VMEM((nx * ny, 1, 128), f32),
                pltpu.VMEM((channels, channels), f32), pltpu.VMEM((lat, lon), f32), pltpu.VMEM((lat, lon), f32),
                pltpu.VMEM((2, 2, 2, lon), f32), pltpu.VMEM((2, 8, 128), f32), pltpu.VMEM((2, channels, 128), f32),
                dma((2, channels)), dma((3,)),
                dma((BLOCKS, 2, 2)), dma((BLOCKS, 2, 2)), dma((BLOCKS, 2, 2)), dma((BLOCKS, 2, 2)),
                dma((BLOCKS, 4)), dma((BLOCKS, 4)), dma((4, 2)), dma((4, 2)),
                dma((1,)), dma((1,)), pltpu.SemaphoreType.REGULAR((8,)),
            ],
            compiler_params=pltpu.CompilerParams(
                collective_id=0, has_side_effects=True, vmem_limit_bytes=24 * 1024 * 1024),
        )(*map(keep, (forcing, damping, coupling, wind_lon, wind_lat)))
        shape = jax.ShapeDtypeStruct((channels, lat, lon), f32)
        return pl.pallas_call(
            finish,
            out_shape=(shape, shape),
            in_specs=[vmem, vmem],
            out_specs=(hbm, hbm),
            scratch_shapes=[pltpu.VMEM((2, lat, channels, lon), f32), dma((lat // 8, 2, channels))],
            compiler_params=pltpu.CompilerParams(vmem_limit_bytes=24 * 1024 * 1024),
        )(basis, weights)

    return jax.shard_map(
        per_device,
        mesh=mesh,
        in_specs=(P(None, "gy", "gx"), P(None, "gy", "gx"), P(), P("gy", "gx"), P("gy", "gx")),
        out_specs=(P(None, "gy", "gx"), P(None, "gy", "gx")),
        check_vma=False,
    )
```

```python
import functools
import math

import jax
import jax.numpy as jnp
from jax import lax
from jax.experimental import pallas as pl
from jax.experimental.pallas import tpu as pltpu
from jax.sharding import PartitionSpec as P

ITERS = 8
COUPLE = 0.25
DIFF_LAT = 0.5
DIFF_LON = 0.5
GUARD = 1.0
MESH = pl.DeviceIdType.MESH
HI = lax.Precision.HIGHEST

MIDDLE = 9.0
RADIUS = 6.0
WIDTH = 3.0
THETA = [MIDDLE + RADIUS * math.cos(math.pi * (2 * k + 1) / (2 * ITERS)) for k in (7, 0, 4, 2, 6, 1, 5, 3)]
PAIRS = [(k, i) for k in range(ITERS + 1) for i in range(k + 1)]
GROUP = 4
HALO = 4
BLOCKS = ITERS // 2


def apply_to(coords):
    out = [None] * (len(coords) + 1)
    for k, value in enumerate(coords):
        low = THETA[k] * value if k < ITERS else value
        out[k] = low if out[k] is None else out[k] + low
        out[k + 1] = WIDTH * value
    return out


def tree(terms):
    while len(terms) > 1:
        terms = [a + b for a, b in zip(terms[::2], terms[1::2])] + ([terms[-1]] if len(terms) % 2 else [])
    return terms[0]


def small_solve(gram):
    first = jnp.sqrt(gram[0][0] + GUARD)
    coords = [[1.0 / first]]
    images = [[gram[i][0] * coords[0][0] for i in range(ITERS + 1)]]
    heights = []
    for j in range(ITERS):
        moved = apply_to(coords[j])
        column = []
        for i in range(j + 1):
            column.append(functools.reduce(lambda a, b: a + b, [images[i][k] * moved[k] for k in range(j + 2)]))
        left = list(moved)
        for i in range(j + 1):
            for k in range(i + 1):
                left[k] = left[k] - column[i] * coords[i][k]
        image = [
            functools.reduce(lambda a, b: a + b, [gram[r][k] * left[k] for k in range(j + 2)])
            for r in range(ITERS + 1)
        ]
        norm_sq = functools.reduce(lambda a, b: a + b, [image[k] * left[k] for k in range(j + 2)])
        subdiag = jnp.sqrt(jnp.maximum(norm_sq, 0.0) + GUARD)
        column.append(subdiag)
        heights.append(column)
        inverse = 1.0 / subdiag
        coords.append([v * inverse for v in left])
        images.append([v * inverse for v in image])
    cosines, sines, target, rotated = [], [], [first], []
    for j in range(ITERS):
        column = list(heights[j])
        for e in range(j):
            upper, lower = column[e], column[e + 1]
            column[e] = cosines[e] * upper + sines[e] * lower
            column[e + 1] = cosines[e] * lower - sines[e] * upper
        upper, lower = column[j], column[j + 1]
        radius = jnp.sqrt(upper * upper + lower * lower)
        inverse = 1.0 / radius
        cosine, sine = upper * inverse, lower * inverse
        column[j] = radius
        kept = target[j]
        target[j] = cosine * kept
        target.append(-sine * kept)
        cosines.append(cosine)
        sines.append(sine)
        rotated.append(column)
    weights = [None] * ITERS
    for j in reversed(range(ITERS)):
        value = target[j]
        for later in range(j + 1, ITERS):
            value = value - rotated[later][j] * weights[later]
        weights[j] = value / rotated[j][j]
    answer = [None] * ITERS
    for j in range(ITERS):
        for k in range(j + 1):
            term = weights[j] * coords[j][k]
            answer[k] = term if answer[k] is None else answer[k] + term
    return answer, apply_to(answer)


def word_plan(nx, ny):
    def doubled(n):
        out = [2]
        while out[-1] < n:
            out.append(2 * out[-1])
        return out[:-1]

    far_lat, far_lon = doubled(ny), doubled(nx // 2 + 1)
    words = max(len(far_lat), len(far_lon))
    reach = {}
    for x in range(nx):
        for y in range(ny):
            reach[x, y] = {((x + dx) % nx, y + dy) for dx in (-1, 0, 1) for dy in (-1, 0, 1) if 0 <= y + dy < ny}
    near = {place: set(known) for place, known in reach.items()}

    def peers(x, y, n):
        out = []
        if n < len(far_lat):
            out += [(x, y + d) for d in (-far_lat[n], far_lat[n]) if 0 <= y + d < ny]
        if n < len(far_lon):
            out += [((x + d) % nx, y) for d in (-far_lon[n], far_lon[n])]
        return out

    told = None
    for n in range(BLOCKS):
        before = reach
        reach = {place: set().union(*(before[other] for other in near[place])) for place in before}
        if told is not None:
            reach = {place: known.union(*(told[other] for other in peers(*place, n - 1))) for place, known in reach.items()}
        told = reach
    if any(len(known) < nx * ny for known in reach.values()):
        far_lon = far_lon + [nx // 2] * (max(BLOCKS, words + 1) - len(far_lon))
    return far_lat, far_lon


def kernel(nx, ny, f_hbm, d_hbm, c_hbm, wl_hbm, wa_hbm, padded, splats,
           diag, coef, block, single, side_in, side_out, band, fixed_in, fixed_out, corner_in, corner_out,
           gram_acc, slots, c_ref, wl_ref, wa_ref, wind_in, kx_in, turned,
           in_sem, wind_sem, lat_send, lat_recv, lon_send, lon_recv, turn_send, turn_recv, fix_send, fix_recv, red_send, red_recv, word):
    channels, lat, lon = f_hbm.shape
    tiles = lon // 128
    basis = padded.at[:, :, pl.ds(0, channels), :]
    total = nx * ny
    ix, iy = lax.axis_index("gx"), lax.axis_index("gy")
    me = ix * ny + iy
    east, west = lax.rem(ix + 1, nx), lax.rem(ix + nx - 1, nx)

    small = [pltpu.make_async_copy(src, dst, wind_sem.at[n])
             for n, (src, dst) in enumerate(((wl_hbm, wl_ref), (wa_hbm, wa_ref), (c_hbm, c_ref)))]
    for copy in small:
        copy.start()
    loads = [[], []]
    for q, (src, dst, off) in enumerate(((f_hbm, basis.at[0], HALO), (d_hbm, diag, 2))):
        for c in range(channels):
            copy = pltpu.make_async_copy(src.at[c], dst.at[pl.ds(off, lat), c, :], in_sem.at[q, c])
            copy.start()
            loads[q].append(copy)

    barrier = pltpu.get_barrier_semaphore()

    def greet(to, sem=barrier):
        pl.semaphore_signal(sem, inc=1, device_id=to, device_id_type=MESH)

    greet((east, iy))
    greet((west, iy))

    def greet_lat(to):
        greet((ix, to))
        greet((east, to))
        greet((west, to))

    @pl.when(iy > 0)
    def _():
        greet_lat(iy - 1)

    @pl.when(iy < ny - 1)
    def _():
        greet_lat(iy + 1)

    far_lat, far_lon = word_plan(nx, ny)

    def spread_word(n):
        if n < len(far_lat):
            d = far_lat[n]

            @pl.when(iy >= d)
            def _():
                greet((ix, iy - d), word.at[n])

            @pl.when(iy + d < ny)
            def _():
                greet((ix, iy + d), word.at[n])

        if n < len(far_lon):
            greet((lax.rem(ix + far_lon[n], nx), iy), word.at[n])
            greet((lax.rem(ix + nx - far_lon[n], nx), iy), word.at[n])

    def hear_word(n):
        count = 2 if n < len(far_lon) else 0
        if n < len(far_lat):
            d = far_lat[n]
            count = count + jnp.where(iy >= d, 1, 0) + jnp.where(iy + d < ny, 1, 0)
        pl.semaphore_wait(word.at[n], count)

    words = max(len(far_lat), len(far_lon))

    scale = 1.0 / WIDTH
    size = GROUP * channels

    def spread(n):
        row = lax.broadcasted_iota(jnp.int32, (n, channels), 0)
        col = lax.broadcasted_iota(jnp.int32, (n, channels), 1)
        return jnp.where(lax.rem(row, channels) == col, 1.0, 0.0).astype(jnp.float32)

    def widen(tall, n):
        wide = lax.dot_general(tall, spread(3 * n), (((1,), (1,)), ((), ())), precision=HI,
                               preferred_element_type=jnp.float32) * (COUPLE * scale)
        across = lax.broadcasted_iota(jnp.int32, wide.shape, 1)
        high = wide.astype(jnp.bfloat16).astype(jnp.float32)
        return jnp.where(across < 2 * n, high, wide - high), across

    def blank(at):
        for b in range(BLOCKS):
            basis[2 * b, pl.ds(HALO + lat if at else 0, HALO)] = jnp.zeros((HALO, channels, lon), jnp.float32)
        diag[pl.ds(lat + 2 if at else 0, 2)] = jnp.zeros((2, channels, lon), jnp.float32)
        coef[pl.ds(lat + 2 if at else 0, 2)] = jnp.zeros((2, 8, lon), jnp.float32)
        corner_in[:, 0 if at else 2] = jnp.zeros((BLOCKS, 2, 128), jnp.float32)
        corner_in[:, 1 if at else 3] = jnp.zeros((BLOCKS, 2, 128), jnp.float32)

    @pl.when(iy == 0)
    def _():
        blank(0)

    @pl.when(iy == ny - 1)
    def _():
        blank(1)

    def fill_coef(wl, wa, kx, at):
        wl, wa = wl * (scale / 12.0), wa * (scale / 12.0)
        kx = jnp.concatenate([kx] * tiles, axis=1)
        planes = (8.0 * wl - kx, -8.0 * wl - kx, wl, 8.0 * wa - DIFF_LAT * scale, -8.0 * wa - DIFF_LAT * scale, wa,
                  2.0 * kx + (1.0 + 2.0 * DIFF_LAT) * scale, jnp.zeros_like(kx))
        for q, plane in enumerate(planes):
            for r in range(wl.shape[0]):
                coef[r + at, q:q + 1, :] = plane[r:r + 1, :]

    def pack(read, far, n, picked=None):
        lane = lax.broadcasted_iota(jnp.int32, (n, 128), 1)
        to_west = to_east = jnp.zeros((n, 128), jnp.float32)
        for r in picked or range(lat):
            head = read(r, slice(0, 128))
            tail = read(r, slice(lon - 128, lon))
            here = (lane >= 2 * r) & (lane < 2 * r + 2)
            to_west = jnp.where(here, pltpu.roll(head, 2 * r, 1) if r else head, to_west)
            to_east = jnp.where(here, pltpu.roll(tail, (2 * r + 2) % 128, 1), to_east)
            if far:
                here = (lane >= 64 + 2 * r) & (lane < 64 + 2 * r + 2)
                to_west = jnp.where(here, pltpu.roll(head, (62 + 2 * r) % 128, 1), to_west)
                to_east = jnp.where(here, pltpu.roll(tail, (68 + 2 * r) % 128, 1), to_east)
        return to_west, to_east

    lane = lax.broadcasted_iota(jnp.int32, (channels, 128), 1)
    spot = lax.broadcasted_iota(jnp.int32, (8, 128), 1)
    deep = lax.broadcasted_iota(jnp.int32, (8, 128), 0)

    def copy_to(src, dst, send, recv, to):
        return pltpu.make_async_remote_copy(src_ref=src, dst_ref=dst, send_sem=send, recv_sem=recv,
                                            device_id=to, device_id_type=MESH)

    def lat_to(way):
        return iy + 1 if way else iy - 1

    def lat_copy(b, way, near):
        if way:
            src, dst = HALO + lat - (2 if near else 4), 2 if near else 0
        else:
            src, dst = HALO + (0 if near else 2), HALO + lat + (0 if near else 2)
        return copy_to(basis.at[2 * b, pl.ds(src, 2)], basis.at[2 * b, pl.ds(dst, 2)], lat_send.at[b, way, near],
                       lat_recv.at[b, way, near], (ix, lat_to(way)))

    def diag_copy(way):
        src = pl.ds(lat, 2) if way else pl.ds(2, 2)
        dst = pl.ds(0, 2) if way else pl.ds(lat + 2, 2)
        return copy_to(diag.at[src], diag.at[dst], fix_send.at[0, way], fix_recv.at[0, way], (ix, lat_to(way)))

    def wind_copies(way):
        src = pl.ds(lat - 2, 2) if way else pl.ds(0, 2)
        return [copy_to(ref.at[src], wind_in.at[n, way], fix_send.at[1 + n, way], fix_recv.at[1 + n, way], (ix, lat_to(way)))
                for n, ref in enumerate((wl_ref, wa_ref))]

    def fix_side(way):
        return copy_to(fixed_out.at[way], fixed_in.at[way], fix_send.at[3, way], fix_recv.at[3, way],
                       (east if way else west, iy))

    def lon_copy(b, part, way):
        return copy_to(side_out.at[b, part, way], side_in.at[b, part, way], lon_send.at[b, part, way],
                       lon_recv.at[b, part, way], (east if way else west, iy))

    sided = (list(range(4, lat - 4)), list(range(4)) + list(range(lat - 4, lat)))

    def turn_copy(b, up, way):
        n = 2 * up + way
        return copy_to(corner_out.at[b], corner_in.at[b, n], turn_send.at[b, n], turn_recv.at[b, n],
                       (east if way else west, lat_to(up)))

    def each_lat(act):
        @pl.when(iy < ny - 1)
        def _():
            act(1)

        @pl.when(iy > 0)
        def _():
            act(0)

    def arrive_lat(act):
        @pl.when(iy > 0)
        def _():
            act(1)

        @pl.when(iy < ny - 1)
        def _():
            act(0)

    def send_corners(b):
        k = 2 * b
        small = jnp.zeros((8, 128), jnp.float32)
        for up in range(2):
            for way in range(2):
                for h in range(channels // 8):
                    for j in range(2):
                        at = 16 * up + 8 * way + 4 * h + 2 * j
                        here = (spot >= at) & (spot < at + 2)
                        cut = slice(lon - 128, lon) if way else slice(0, 128)
                        part = basis[k, HALO + (lat - 2 if up else 0) + j, 8 * h:8 * h + 8, cut]
                        move = (at - (126 if way else 0)) % 128
                        small = jnp.where(here, pltpu.roll(part, move, 1) if move else part, small)
        dense = small
        for g in range(1, 4):
            moved = pltpu.roll(pltpu.roll(small, 8 - 2 * g, 0), 32 * g, 1)
            dense = jnp.where(spot // 32 == g, moved, dense)
        corner_out[b] = dense[0:2, :]

        def go(up):
            turn_copy(b, up, 0).start()
            turn_copy(b, up, 1).start()

        each_lat(go)

    def send_sides(b, part):
        k = 2 * b
        to_west, to_east = pack(lambda r, cut: basis[k, r + HALO, :, cut], True, channels, sided[part])
        side_out[b, part, 0] = to_west
        side_out[b, part, 1] = to_east
        lon_copy(b, part, 0).start()
        lon_copy(b, part, 1).start()

    def take_corners(b):
        got = jnp.zeros((2, 128), jnp.float32)
        sub = lax.rem(lax.broadcasted_iota(jnp.int32, (2, 128), 1), 32) // 8
        for n in range(4):
            got = jnp.where(sub == n, corner_in[b, n], got)
        got = jnp.concatenate([got] * 4, axis=0)
        small = got
        for g in range(1, 4):
            small = jnp.where(deep // 2 == g, pltpu.roll(got, 128 - 32 * g, 1), small)
        parts = []
        for h in range(channels // 8):
            part = jnp.zeros((8, 128), jnp.float32)
            for up in range(2):
                for way in range(2):
                    at = 16 * up + 8 * way + 4 * h
                    want = (64 if way else 0) + (2 * lat - 4 if up else 0)
                    here = (spot >= want) & (spot < want + 4)
                    part = jnp.where(here, pltpu.roll(small, (want - at) % 128, 1) if want != at else small, part)
            parts.append(part)
        return jnp.concatenate(parts, axis=0)

    def theta_of(k):
        theta = jnp.float32(THETA[0] * scale)
        for i in range(1, ITERS):
            theta = jnp.where(k == i, jnp.float32(THETA[i] * scale), theta)
        return theta

    def products(pairs, places, accs):
        for r in places:
            for h in range(channels // 8):
                for t in range(tiles):
                    at = (r + HALO, slice(8 * h, 8 * h + 8), slice(128 * t, 128 * t + 128))
                    held = {}

                    def read(k):
                        if id(k) not in held:
                            held[id(k)] = basis[(k,) + at]
                        return held[id(k)]

                    for n, (k, i) in enumerate(pairs):
                        m = (2 * h + t) % 2
                        accs[2 * n + m] = accs[2 * n + m] + read(k) * read(i)
        return accs

    def keep(k, i, acc, more):
        at = lax.div(k * (k + 1), 2) + i
        gram_acc[at] = gram_acc[at] + acc if more else acc

    def dots(pairs, first, count, more=False):
        zero = jnp.zeros((8, 128), jnp.float32)
        if count == 8:
            accs = products(pairs, [(j + first) % lat for j in range(8)],
                            [zero] * (2 * len(pairs)))
        else:
            def part(b, accs):
                return tuple(products(pairs, [b * 8 + j + first for j in range(8)], list(accs)))

            accs = lax.fori_loop(0, count // 8, part, (zero,) * (2 * len(pairs)))
        for n, (k, i) in enumerate(pairs):
            keep(k, i, accs[2 * n] + accs[2 * n + 1], more)

    def dots_two(k, first, count, more=False):
        def one(i, _):
            before = k - 1
            dots([(before, i), (k, i)], first, count, more)
            return 0

        lax.fori_loop(0, k, one, 0)
        dots([(k, k)], first, count, more)

    def split(stack):
        high = stack.astype(jnp.bfloat16)
        low = (stack - high.astype(jnp.float32)).astype(jnp.bfloat16)
        return jnp.concatenate([high, low, high], axis=0)

    def rows(k, picked, theta, beside, bare=False):
        stack = jnp.concatenate([basis[k, r + HALO] for r in picked], axis=0)
        mixed = lax.dot_general(block[...], split(stack), (((1,), (0,)), ((), ())), preferred_element_type=jnp.float32)
        for j, r in enumerate(picked):
            inside = 0 <= r < lat
            source = beside
            left = 2 * r if inside else 64 + 2 * (r % lat)
            right = 64 + 2 * r if inside else 2 * (r % lat)

            def turn(v, shift):
                return pltpu.roll(v, shift % 128, 1) if shift % 128 else v

            x = [basis[k, r + HALO, :, 128 * t:128 * t + 128] for t in range(tiles)]
            if source is None:
                ends = [jnp.zeros_like(lane, jnp.float32)] * 4
            else:
                ends = [turn(source, shift) for shift in (127 - right, 126 - right, -left - 1, -left)]
            fwd1 = [pltpu.roll(v, 127, 1) for v in x] + [ends[0]]
            fwd2 = [pltpu.roll(v, 126, 1) for v in x] + [ends[1]]
            bwd1 = [ends[2]] + [pltpu.roll(v, 1, 1) for v in x]
            bwd2 = [ends[3]] + [pltpu.roll(v, 2, 1) for v in x]
            for t in range(tiles):
                cut = slice(128 * t, 128 * t + 128)
                e1 = jnp.where(lane < 127, fwd1[t], fwd1[t + 1])
                e2 = jnp.where(lane < 126, fwd2[t], fwd2[t + 1])
                w1 = jnp.where(lane >= 1, bwd1[t + 1], bwd1[t])
                w2 = jnp.where(lane >= 2, bwd2[t + 1], bwd2[t])

                def weight(q):
                    return coef[r + 2, q:q + 1, cut]

                def near(d):
                    return basis[k, r + HALO + d, :, cut]

                def has(d):
                    return not bare or 0 <= r + d < lat

                value = (diag[r + 2, :, cut] - theta) * x[t] + mixed[channels * j:channels * (j + 1), cut]
                value = value + (weight(0) * e1 + weight(1) * w1 + weight(2) * (w2 - e2))
                if has(1):
                    value = value + weight(3) * near(1)
                if has(-1):
                    value = value + weight(4) * near(-1)
                if has(2) and has(-2):
                    value = value + weight(5) * (near(-2) - near(2))
                elif has(2):
                    value = value - weight(5) * near(2)
                else:
                    value = value + weight(5) * near(-2)
                basis[k + 1, r + HALO, :, cut] = value

    def middle(got):
        return jnp.where(lane < 64, got[1], pltpu.roll(got[0], 64, 1))

    def both(ref, b, part):
        return [ref[b, 0, way] + ref[b, 1, way] if part else ref[b, 0, way] for way in range(2)]

    row = lax.rem(lane, 64) // 2
    even = lax.rem(lane, 2) == 0

    def edge_coef(q):
        return jnp.where(spot[0:1] < 64, fixed_in[1, channels + q:channels + q + 1, :],
                         pltpu.roll(fixed_in[0, channels + q:channels + q + 1, :], 64, 1))

    def edge_band(got, given, theta, centre):
        from_east, from_west = got
        to_west, to_east = given
        low = jnp.where(lane < 64, pltpu.roll(from_west, 64, 1), pltpu.roll(to_east, 64, 1))
        high = jnp.where(lane < 64, to_west, from_east)
        e1 = jnp.where(even, pltpu.roll(centre, 127, 1), pltpu.roll(high, 1, 1))
        w1 = jnp.where(even, pltpu.roll(low, 127, 1), pltpu.roll(centre, 1, 1))
        n1 = jnp.where(row < lat - 1, pltpu.roll(centre, 126, 1), 0.0)
        n2 = jnp.where(row < lat - 2, pltpu.roll(centre, 124, 1), 0.0)
        s1 = jnp.where(row >= 1, pltpu.roll(centre, 2, 1), 0.0)
        s2 = jnp.where(row >= 2, pltpu.roll(centre, 4, 1), 0.0)
        mixed = lax.dot_general(single[...], split(centre), (((1,), (0,)), ((), ())), preferred_element_type=jnp.float32)
        own = jnp.where(lane < 64, fixed_in[1, 0:channels, :], pltpu.roll(fixed_in[0, 0:channels, :], 64, 1))
        value = (own - theta) * centre + mixed
        value = value + (edge_coef(0) * e1 + edge_coef(1) * w1 + edge_coef(2) * (low - high))
        return value + (edge_coef(3) * n1 + edge_coef(4) * s1 + edge_coef(5) * (s2 - n2))

    def edge_turn(corners):
        n1 = jnp.where(row < lat - 1, 0.0, pltpu.roll(corners, 126, 1))
        n2 = jnp.where(row < lat - 2, 0.0, pltpu.roll(corners, 124, 1))
        s1 = jnp.where(row >= 1, 0.0, pltpu.roll(corners, 2, 1))
        s2 = jnp.where(row >= 2, 0.0, pltpu.roll(corners, 4, 1))
        return edge_coef(3) * n1 + edge_coef(4) * s1 + edge_coef(5) * (s2 - n2)

    def add_sides(k, centre, picked):
        def own(q):
            return jnp.where(spot[0:1] < 64, fixed_out[0, channels + q:channels + q + 1, :],
                             pltpu.roll(fixed_out[1, channels + q:channels + q + 1, :], 64, 1))

        from_west = own(2) * centre + jnp.where(even, own(1) * pltpu.roll(centre, 127, 1), 0.0)
        from_east = jnp.where(even, 0.0, own(0) * pltpu.roll(centre, 1, 1)) - own(2) * centre
        for r in picked:
            left = pltpu.roll(from_west, (128 - 2 * r) % 128, 1) if r else from_west
            right = pltpu.roll(from_east, (62 - 2 * r) % 128, 1) if 2 * r != 62 else from_east
            basis[k + 1, r + HALO, :, 0:128] += jnp.where(lane < 2, left, 0.0)
            basis[k + 1, r + HALO, :, lon - 128:lon] += jnp.where(lane >= 126, right, 0.0)

    def stage(b, _):
        k = 2 * b
        theta, after = theta_of(k), theta_of(k + 1)
        for g in range((lat - 4) // GROUP):
            rows(k, [2 + GROUP * g + j for j in range(GROUP)], theta, None)
        rows(k, (0, 1, lat - 2, lat - 1), theta, None, bare=True)

        dots_two(k, 0, lat)
        more = b + 1 < BLOCKS
        for part in range(2):
            lon_copy(b, part, 0).wait()
            lon_copy(b, part, 1).wait()
            if part == 0:
                @pl.when(b == 0)
                def _():
                    fix_side(0).wait()
                    fix_side(1).wait()

            got = both(side_in, b, part)
            centre = middle(got)
            add_sides(k, centre, sided[part])
            band[...] = edge_band(got, both(side_out, b, part), theta, centre)
            beside = band[...]
            if part:
                rows(k + 1, (4, 5, lat - 6, lat - 5), after, beside)
            else:
                for g in range((lat - 12) // GROUP):
                    rows(k + 1, [6 + GROUP * g + j for j in range(GROUP)], after, beside)

        @pl.when(more)
        def _():
            send_sides(b + 1, 0)

        @pl.when(b + 1 == BLOCKS)
        def _():
            dots_two(k + 2, 4, lat - 8)

        def corners_in(way):
            turn_copy(b, way, 0).wait_recv()
            turn_copy(b, way, 1).wait_recv()

            @pl.when(b == 0)
            def _():
                for copy in wind_copies(way):
                    copy.wait_recv()
                fill_coef(wind_in[0, way], wind_in[1, way], kx_in[way, 6:8] if way else kx_in[way, 0:2], 0 if way else lat + 2)

        arrive_lat(lambda way: lat_copy(b, way, 1).wait_recv())
        beside = band[...]
        south, north = basis[k, HALO - 1], basis[k, HALO + lat]
        basis[k + 1, HALO] += coef[2, 4:5, :] * south + coef[2, 5:6, :] * basis[k, HALO - 2]
        basis[k + 1, HALO + 1] += coef[3, 5:6, :] * south
        basis[k + 1, HALO + lat - 1] += coef[lat + 1, 3:4, :] * north - coef[lat + 1, 5:6, :] * basis[k, HALO + lat + 1]
        basis[k + 1, HALO + lat - 2] -= coef[lat, 5:6, :] * north
        rows(k + 1, (2, 3, lat - 4, lat - 3), after, beside)

        @pl.when(more)
        def _():
            each_lat(lambda way: lat_copy(b + 1, way, 0).start())

        arrive_lat(corners_in)
        turned[0] = take_corners(b)
        turned[1] = band[...] + edge_turn(turned[0])

        def far_in(way):
            lat_copy(b, way, 0).wait_recv()

            @pl.when(b == 0)
            def _():
                diag_copy(way).wait_recv()

        arrive_lat(far_in)
        rows(k, (-2, -1, lat, lat + 1), theta, turned[0])
        rows(k + 1, (0, 1, lat - 2, lat - 1), after, turned[1])

        @pl.when(more)
        def _():
            send_corners(b + 1)
            each_lat(lambda way: lat_copy(b + 1, way, 1).start())
            send_sides(b + 1, 1)

        for n in range(min(words, BLOCKS)):
            @pl.when(b == n)
            def _():
                if n:
                    hear_word(n - 1)
                spread_word(n)

        if words < BLOCKS:
            @pl.when(b == words)
            def _():
                hear_word(words - 1)

        def sent(way):
            lat_copy(b, way, 0).wait_send()
            lat_copy(b, way, 1).wait_send()
            turn_copy(b, way, 0).wait_send()
            turn_copy(b, way, 1).wait_send()

            @pl.when(b == 0)
            def _():
                for copy in wind_copies(way) + [diag_copy(way)]:
                    copy.wait_send()

        each_lat(sent)
        return 0

    for copy in loads[0]:
        copy.wait()
    pl.semaphore_wait(barrier, 2 + jnp.where(iy > 0, 3, 0) + jnp.where(iy < ny - 1, 3, 0))
    send_corners(0)

    def first_rows(way):
        lat_copy(0, way, 1).start()
        lat_copy(0, way, 0).start()

    each_lat(first_rows)
    send_sides(0, 0)
    send_sides(0, 1)
    for copy in small:
        copy.wait()

    def first_winds(way):
        for copy in wind_copies(way):
            copy.start()

    each_lat(first_winds)
    place = (lax.broadcasted_iota(jnp.int32, (lat + 16, 128), 0) + iy * lat - 8).astype(jnp.float32)
    phi = -math.pi / 2 + (place + 0.5) * (math.pi / (lat * ny))
    kx = (DIFF_LON * scale) / (jnp.cos(phi) ** 2 + 0.1)
    kx_in[0] = kx[lat + 8:lat + 16]
    kx_in[1] = kx[0:8]
    fill_coef(wl_ref[...], wa_ref[...], kx[8:lat + 8], 2)
    for copy in loads[1]:
        copy.wait()

    def prepare(r, _):
        diag[r + 2] = diag[r + 2] * scale + coef[r + 2, 6:7, :]
        return 0

    for r in (0, 1, lat - 2, lat - 1):
        prepare(r, 0)
    each_lat(lambda way: diag_copy(way).start())
    lax.fori_loop(2, lat - 2, prepare, 0)
    fixed = [pack(lambda r, cut: diag[r + 2, :, cut], False, channels), pack(lambda r, cut: coef[r + 2, :, cut], False, 8)]
    for way in range(2):
        fixed_out[way, 0:channels, :] = fixed[0][way]
        fixed_out[way, channels:channels + 8, :] = fixed[1][way]
    fix_side(0).start()
    fix_side(1).start()
    single[...] = widen(c_ref[...], channels)[0].astype(jnp.bfloat16)
    tall = lax.dot_general(spread(size), c_ref[...], (((1,), (0,)), ((), ())), precision=HI,
                           preferred_element_type=jnp.float32)
    wide, across = widen(tall, size)
    down = lax.broadcasted_iota(jnp.int32, (size, 3 * size), 0)
    block[...] = jnp.where(down // channels == lax.rem(across, size) // channels, wide, 0.0).astype(jnp.bfloat16)
    lax.fori_loop(0, BLOCKS, stage, 0)
    for n in range(BLOCKS, words + 1):
        hear_word(n - 1)
        if n < words:
            spread_word(n)
    dots_two(ITERS, lat - 4, 8, True)

    sums = jnp.concatenate(
        [jnp.sum(gram_acc[n], axis=0, keepdims=True) for n in range(len(PAIRS))]
        + [jnp.zeros((128 - len(PAIRS), 128), jnp.float32)], axis=0)
    flat = lax.dot_general(jnp.ones((8, 128), jnp.float32), sums, (((1,), (1,)), ((), ())), precision=HI,
                           preferred_element_type=jnp.float32)
    slots[me] = flat[0:1, :]

    def share(to):
        return copy_to(slots.at[me], slots.at[me], red_send.at[0], red_recv.at[0], to)

    def wrap(v, n):
        return jnp.where(v >= n, v - n, v)

    for dx in range(nx):
        for dy in range(ny):
            if dx or dy:
                share((wrap(ix + dx, nx), wrap(iy + dy, ny))).start()
    others = slots.at[pl.ds(0, total - 1)]
    everyone = copy_to(others, others, red_send.at[0], red_recv.at[0], (east, iy))
    everyone.wait_recv()
    everyone.wait_send()
    whole = tree([slots[n] for n in range(total)])
    gram = [[None] * (ITERS + 1) for _ in range(ITERS + 1)]
    for n, (k, i) in enumerate(PAIRS):
        gram[k][i] = gram[i][k] = jnp.broadcast_to(whole[:, n:n + 1], (8, 128))
    answer, applied = small_solve(gram)
    for k in range(ITERS):
        splats[k] = answer[k]
    for k in range(ITERS + 1):
        splats[ITERS + k] = applied[k]


def finish(b_ref, w_ref, sol_hbm, res_hbm, outs, out_sem):
    channels, lat, lon = sol_hbm.shape
    stores = []
    for part in range(lat // 8):
        def one(j, _):
            r = 8 * part + j
            for h in range(channels // 8):
                for t in range(lon // 128):
                    at = (slice(8 * h, 8 * h + 8), slice(128 * t, 128 * t + 128))
                    x = b_ref[0, r + HALO, at[0], at[1]]
                    best = w_ref[0] * x
                    rest = x - w_ref[ITERS] * x
                    for k in range(1, ITERS + 1):
                        x = b_ref[k, r + HALO, at[0], at[1]]
                        if k < ITERS:
                            best = best + w_ref[k] * x
                        rest = rest - w_ref[ITERS + k] * x
                    outs[0, r, at[0], at[1]] = best
                    outs[1, r, at[0], at[1]] = rest
            return 0

        lax.fori_loop(0, 8, one, 0)
        for q, dst in enumerate((sol_hbm, res_hbm)):
            for c in range(channels):
                copy = pltpu.make_async_copy(outs.at[q, pl.ds(8 * part, 8), c, :], dst.at[c, pl.ds(8 * part, 8), :],
                                             out_sem.at[part, q, c])
                copy.start()
                stores.append(copy)
    for copy in stores:
        copy.wait()


def solution(mesh):
    nx, ny = mesh.shape["gx"], mesh.shape["gy"]

    def per_device(forcing, damping, coupling, wind_lon, wind_lat):
        channels, lat, lon = forcing.shape
        f32 = jnp.float32
        vmem = pl.BlockSpec(memory_space=pltpu.VMEM)
        hbm = pl.BlockSpec(memory_space=pltpu.HBM)
        dma = pltpu.SemaphoreType.DMA

        def keep(v):
            return pltpu.with_memory_space_constraint(v, pltpu.HBM)

        basis, weights = pl.pallas_call(
            functools.partial(kernel, nx, ny),
            out_shape=(pltpu.VMEM((ITERS + 1, lat + 2 * HALO + 1, channels + 8, lon), f32), pltpu.VMEM((2 * ITERS + 1, 8, 128), f32)),
            in_specs=[hbm] * 5,
            out_specs=(vmem, vmem),
            scratch_shapes=[
                pltpu.VMEM((lat + 4, channels, lon), f32),
                pltpu.VMEM((lat + 4, 8, lon), f32),
                pltpu.VMEM((GROUP * channels, 3 * GROUP * channels), jnp.bfloat16),
                pltpu.VMEM((channels, 3 * channels), jnp.bfloat16),
                pltpu.VMEM((BLOCKS, 2, 2, channels, 128), f32),
                pltpu.VMEM((BLOCKS, 2, 2, channels, 128), f32),
                pltpu.VMEM((channels, 128), f32),
                pltpu.VMEM((2, channels + 8, 128), f32),
                pltpu.VMEM((2, channels + 8, 128), f32),
                pltpu.VMEM((BLOCKS, 4, 2, 128), f32),
                pltpu.VMEM((BLOCKS, 2, 128), f32),
                pltpu.VMEM((len(PAIRS), 8, 128), f32),
                pltpu.VMEM((nx * ny, 1, 128), f32),
                pltpu.VMEM((channels, channels), f32), pltpu.VMEM((lat, lon), f32), pltpu.VMEM((lat, lon), f32),
                pltpu.VMEM((2, 2, 2, lon), f32), pltpu.VMEM((2, 8, 128), f32), pltpu.VMEM((2, channels, 128), f32),
                dma((2, channels)), dma((3,)),
                dma((BLOCKS, 2, 2)), dma((BLOCKS, 2, 2)), dma((BLOCKS, 2, 2)), dma((BLOCKS, 2, 2)),
                dma((BLOCKS, 4)), dma((BLOCKS, 4)), dma((4, 2)), dma((4, 2)),
                dma((1,)), dma((1,)), pltpu.SemaphoreType.REGULAR((8,)),
            ],
            compiler_params=pltpu.CompilerParams(
                collective_id=0, has_side_effects=True, vmem_limit_bytes=24 * 1024 * 1024),
        )(*map(keep, (forcing, damping, coupling, wind_lon, wind_lat)))
        shape = jax.ShapeDtypeStruct((channels, lat, lon), f32)
        return pl.pallas_call(
            finish,
            out_shape=(shape, shape),
            in_specs=[vmem, vmem],
            out_specs=(hbm, hbm),
            scratch_shapes=[pltpu.VMEM((2, lat, channels, lon), f32), dma((lat // 8, 2, channels))],
            compiler_params=pltpu.CompilerParams(vmem_limit_bytes=24 * 1024 * 1024),
        )(basis, weights)

    return jax.shard_map(
        per_device,
        mesh=mesh,
        in_specs=(P(None, "gy", "gx"), P(None, "gy", "gx"), P(), P("gy", "gx"), P("gy", "gx")),
        out_specs=(P(None, "gy", "gx"), P(None, "gy", "gx")),
        check_vma=False,
    )
```

```python
import functools
import math

import jax
import jax.numpy as jnp
from jax import lax
from jax.experimental import pallas as pl
from jax.experimental.pallas import tpu as pltpu
from jax.sharding import PartitionSpec as P

ITERS = 8
COUPLE = 0.25
DIFF_LAT = 0.5
DIFF_LON = 0.5
GUARD = 1.0
MESH = pl.DeviceIdType.MESH
HI = lax.Precision.HIGHEST

MIDDLE = 9.0
RADIUS = 6.0
WIDTH = 3.0
THETA = [MIDDLE + RADIUS * math.cos(math.pi * (2 * k + 1) / (2 * ITERS)) for k in (7, 0, 4, 2, 6, 1, 5, 3)]
PAIRS = [(k, i) for k in range(ITERS + 1) for i in range(k + 1)]
GROUP = 4
HALO = 4
BLOCKS = ITERS // 2


def apply_to(coords):
    out = [None] * (len(coords) + 1)
    for k, value in enumerate(coords):
        low = THETA[k] * value if k < ITERS else value
        out[k] = low if out[k] is None else out[k] + low
        out[k + 1] = WIDTH * value
    return out


def tree(terms):
    while len(terms) > 1:
        terms = [a + b for a, b in zip(terms[::2], terms[1::2])] + ([terms[-1]] if len(terms) % 2 else [])
    return terms[0]


def small_solve(gram):
    first = jnp.sqrt(gram[0][0] + GUARD)
    coords = [[1.0 / first]]
    images = [[gram[i][0] * coords[0][0] for i in range(ITERS + 1)]]
    heights = []
    for j in range(ITERS):
        moved = apply_to(coords[j])
        column = []
        for i in range(j + 1):
            column.append(functools.reduce(lambda a, b: a + b, [images[i][k] * moved[k] for k in range(j + 2)]))
        left = list(moved)
        for i in range(j + 1):
            for k in range(i + 1):
                left[k] = left[k] - column[i] * coords[i][k]
        image = [
            functools.reduce(lambda a, b: a + b, [gram[r][k] * left[k] for k in range(j + 2)])
            for r in range(ITERS + 1)
        ]
        norm_sq = functools.reduce(lambda a, b: a + b, [image[k] * left[k] for k in range(j + 2)])
        subdiag = jnp.sqrt(jnp.maximum(norm_sq, 0.0) + GUARD)
        column.append(subdiag)
        heights.append(column)
        inverse = 1.0 / subdiag
        coords.append([v * inverse for v in left])
        images.append([v * inverse for v in image])
    cosines, sines, target, rotated = [], [], [first], []
    for j in range(ITERS):
        column = list(heights[j])
        for e in range(j):
            upper, lower = column[e], column[e + 1]
            column[e] = cosines[e] * upper + sines[e] * lower
            column[e + 1] = cosines[e] * lower - sines[e] * upper
        upper, lower = column[j], column[j + 1]
        radius = jnp.sqrt(upper * upper + lower * lower)
        inverse = 1.0 / radius
        cosine, sine = upper * inverse, lower * inverse
        column[j] = radius
        kept = target[j]
        target[j] = cosine * kept
        target.append(-sine * kept)
        cosines.append(cosine)
        sines.append(sine)
        rotated.append(column)
    weights = [None] * ITERS
    for j in reversed(range(ITERS)):
        value = target[j]
        for later in range(j + 1, ITERS):
            value = value - rotated[later][j] * weights[later]
        weights[j] = value / rotated[j][j]
    answer = [None] * ITERS
    for j in range(ITERS):
        for k in range(j + 1):
            term = weights[j] * coords[j][k]
            answer[k] = term if answer[k] is None else answer[k] + term
    return answer, apply_to(answer)


def word_plan(nx, ny):
    def doubled(n):
        out = [2]
        while out[-1] < n:
            out.append(2 * out[-1])
        return out[:-1]

    far_lat, far_lon = doubled(ny), doubled(nx // 2 + 1)
    words = max(len(far_lat), len(far_lon))
    reach = {}
    for x in range(nx):
        for y in range(ny):
            reach[x, y] = {((x + dx) % nx, y + dy) for dx in (-1, 0, 1) for dy in (-1, 0, 1) if 0 <= y + dy < ny}
    near = {place: set(known) for place, known in reach.items()}

    def peers(x, y, n):
        out = []
        if n < len(far_lat):
            out += [(x, y + d) for d in (-far_lat[n], far_lat[n]) if 0 <= y + d < ny]
        if n < len(far_lon):
            out += [((x + d) % nx, y) for d in (-far_lon[n], far_lon[n])]
        return out

    told = None
    for n in range(BLOCKS):
        before = reach
        reach = {place: set().union(*(before[other] for other in near[place])) for place in before}
        if told is not None:
            reach = {place: known.union(*(told[other] for other in peers(*place, n - 1))) for place, known in reach.items()}
        told = reach
    if any(len(known) < nx * ny for known in reach.values()):
        far_lon = far_lon + [nx // 2] * (max(BLOCKS, words + 1) - len(far_lon))
    return far_lat, far_lon


def kernel(nx, ny, f_hbm, d_hbm, c_hbm, wl_hbm, wa_hbm, padded, splats,
           diag, coef, block, single, side_in, side_out, band, fixed_in, fixed_out, corner_in, corner_out,
           gram_acc, slots, c_ref, wl_ref, wa_ref, wind_in, kx_in, turned,
           in_sem, wind_sem, lat_send, lat_recv, lon_send, lon_recv, turn_send, turn_recv, fix_send, fix_recv, red_send, red_recv, word):
    channels, lat, lon = f_hbm.shape
    tiles = lon // 128
    basis = padded.at[:, :, pl.ds(0, channels), :]
    total = nx * ny
    ix, iy = lax.axis_index("gx"), lax.axis_index("gy")
    me = ix * ny + iy
    east, west = lax.rem(ix + 1, nx), lax.rem(ix + nx - 1, nx)

    small = [pltpu.make_async_copy(src, dst, wind_sem.at[n])
             for n, (src, dst) in enumerate(((wl_hbm, wl_ref), (wa_hbm, wa_ref), (c_hbm, c_ref)))]
    for copy in small:
        copy.start()
    loads = [[], []]
    for q, (src, dst, off) in enumerate(((f_hbm, basis.at[0], HALO), (d_hbm, diag, 2))):
        for c in range(channels):
            copy = pltpu.make_async_copy(src.at[c], dst.at[pl.ds(off, lat), c, :], in_sem.at[q, c])
            copy.start()
            loads[q].append(copy)

    barrier = pltpu.get_barrier_semaphore()

    def greet(to, sem=barrier):
        pl.semaphore_signal(sem, inc=1, device_id=to, device_id_type=MESH)

    greet((east, iy))
    greet((west, iy))

    def greet_lat(to):
        greet((ix, to))
        greet((east, to))
        greet((west, to))

    @pl.when(iy > 0)
    def _():
        greet_lat(iy - 1)

    @pl.when(iy < ny - 1)
    def _():
        greet_lat(iy + 1)

    far_lat, far_lon = word_plan(nx, ny)

    def spread_word(n):
        if n < len(far_lat):
            d = far_lat[n]

            @pl.when(iy >= d)
            def _():
                greet((ix, iy - d), word.at[n])

            @pl.when(iy + d < ny)
            def _():
                greet((ix, iy + d), word.at[n])

        if n < len(far_lon):
            greet((lax.rem(ix + far_lon[n], nx), iy), word.at[n])
            greet((lax.rem(ix + nx - far_lon[n], nx), iy), word.at[n])

    def hear_word(n):
        count = 2 if n < len(far_lon) else 0
        if n < len(far_lat):
            d = far_lat[n]
            count = count + jnp.where(iy >= d, 1, 0) + jnp.where(iy + d < ny, 1, 0)
        pl.semaphore_wait(word.at[n], count)

    words = max(len(far_lat), len(far_lon))

    scale = 1.0 / WIDTH
    size = GROUP * channels

    def spread(n):
        row = lax.broadcasted_iota(jnp.int32, (n, channels), 0)
        col = lax.broadcasted_iota(jnp.int32, (n, channels), 1)
        return jnp.where(lax.rem(row, channels) == col, 1.0, 0.0).astype(jnp.float32)

    def widen(tall, n):
        wide = lax.dot_general(tall, spread(3 * n), (((1,), (1,)), ((), ())), precision=HI,
                               preferred_element_type=jnp.float32) * (COUPLE * scale)
        across = lax.broadcasted_iota(jnp.int32, wide.shape, 1)
        high = wide.astype(jnp.bfloat16).astype(jnp.float32)
        return jnp.where(across < 2 * n, high, wide - high), across

    def blank(at):
        for b in range(BLOCKS):
            basis[2 * b, pl.ds(HALO + lat if at else 0, HALO)] = jnp.zeros((HALO, channels, lon), jnp.float32)
        diag[pl.ds(lat + 2 if at else 0, 2)] = jnp.zeros((2, channels, lon), jnp.float32)
        coef[pl.ds(lat + 2 if at else 0, 2)] = jnp.zeros((2, 8, lon), jnp.float32)
        corner_in[:, 0 if at else 2] = jnp.zeros((BLOCKS, 2, 128), jnp.float32)
        corner_in[:, 1 if at else 3] = jnp.zeros((BLOCKS, 2, 128), jnp.float32)

    @pl.when(iy == 0)
    def _():
        blank(0)

    @pl.when(iy == ny - 1)
    def _():
        blank(1)

    def fill_coef(wl, wa, kx, at):
        wl, wa = wl * (scale / 12.0), wa * (scale / 12.0)
        kx = jnp.concatenate([kx] * tiles, axis=1)
        planes = (8.0 * wl - kx, -8.0 * wl - kx, wl, 8.0 * wa - DIFF_LAT * scale, -8.0 * wa - DIFF_LAT * scale, wa,
                  2.0 * kx + (1.0 + 2.0 * DIFF_LAT) * scale, jnp.zeros_like(kx))
        for q, plane in enumerate(planes):
            for r in range(wl.shape[0]):
                coef[r + at, q:q + 1, :] = plane[r:r + 1, :]

    def pack(read, far, n, picked=None):
        lane = lax.broadcasted_iota(jnp.int32, (n, 128), 1)
        to_west = to_east = jnp.zeros((n, 128), jnp.float32)
        for r in picked or range(lat):
            head = read(r, slice(0, 128))
            tail = read(r, slice(lon - 128, lon))
            here = (lane >= 2 * r) & (lane < 2 * r + 2)
            to_west = jnp.where(here, pltpu.roll(head, 2 * r, 1) if r else head, to_west)
            to_east = jnp.where(here, pltpu.roll(tail, (2 * r + 2) % 128, 1), to_east)
            if far:
                here = (lane >= 64 + 2 * r) & (lane < 64 + 2 * r + 2)
                to_west = jnp.where(here, pltpu.roll(head, (62 + 2 * r) % 128, 1), to_west)
                to_east = jnp.where(here, pltpu.roll(tail, (68 + 2 * r) % 128, 1), to_east)
        return to_west, to_east

    lane = lax.broadcasted_iota(jnp.int32, (channels, 128), 1)
    spot = lax.broadcasted_iota(jnp.int32, (8, 128), 1)
    deep = lax.broadcasted_iota(jnp.int32, (8, 128), 0)

    def copy_to(src, dst, send, recv, to):
        return pltpu.make_async_remote_copy(src_ref=src, dst_ref=dst, send_sem=send, recv_sem=recv,
                                            device_id=to, device_id_type=MESH)

    def lat_to(way):
        return iy + 1 if way else iy - 1

    def lat_copy(b, way, near):
        if way:
            src, dst = HALO + lat - (2 if near else 4), 2 if near else 0
        else:
            src, dst = HALO + (0 if near else 2), HALO + lat + (0 if near else 2)
        return copy_to(basis.at[2 * b, pl.ds(src, 2)], basis.at[2 * b, pl.ds(dst, 2)], lat_send.at[b, way, near],
                       lat_recv.at[b, way, near], (ix, lat_to(way)))

    def diag_copy(way):
        src = pl.ds(lat, 2) if way else pl.ds(2, 2)
        dst = pl.ds(0, 2) if way else pl.ds(lat + 2, 2)
        return copy_to(diag.at[src], diag.at[dst], fix_send.at[0, way], fix_recv.at[0, way], (ix, lat_to(way)))

    def wind_copies(way):
        src = pl.ds(lat - 2, 2) if way else pl.ds(0, 2)
        return [copy_to(ref.at[src], wind_in.at[n, way], fix_send.at[1 + n, way], fix_recv.at[1 + n, way], (ix, lat_to(way)))
                for n, ref in enumerate((wl_ref, wa_ref))]

    def fix_side(way):
        return copy_to(fixed_out.at[way], fixed_in.at[way], fix_send.at[3, way], fix_recv.at[3, way],
                       (east if way else west, iy))

    def lon_copy(b, part, way):
        return copy_to(side_out.at[b, part, way], side_in.at[b, part, way], lon_send.at[b, part, way],
                       lon_recv.at[b, part, way], (east if way else west, iy))

    sided = (list(range(4, lat - 4)), list(range(4)) + list(range(lat - 4, lat)))

    def turn_copy(b, up, way):
        n = 2 * up + way
        return copy_to(corner_out.at[b], corner_in.at[b, n], turn_send.at[b, n], turn_recv.at[b, n],
                       (east if way else west, lat_to(up)))

    def each_lat(act):
        @pl.when(iy < ny - 1)
        def _():
            act(1)

        @pl.when(iy > 0)
        def _():
            act(0)

    def arrive_lat(act):
        @pl.when(iy > 0)
        def _():
            act(1)

        @pl.when(iy < ny - 1)
        def _():
            act(0)

    def send_corners(b):
        k = 2 * b
        small = jnp.zeros((8, 128), jnp.float32)
        for up in range(2):
            for way in range(2):
                for h in range(channels // 8):
                    for j in range(2):
                        at = 16 * up + 8 * way + 4 * h + 2 * j
                        here = (spot >= at) & (spot < at + 2)
                        cut = slice(lon - 128, lon) if way else slice(0, 128)
                        part = basis[k, HALO + (lat - 2 if up else 0) + j, 8 * h:8 * h + 8, cut]
                        move = (at - (126 if way else 0)) % 128
                        small = jnp.where(here, pltpu.roll(part, move, 1) if move else part, small)
        dense = small
        for g in range(1, 4):
            moved = pltpu.roll(pltpu.roll(small, 8 - 2 * g, 0), 32 * g, 1)
            dense = jnp.where(spot // 32 == g, moved, dense)
        corner_out[b] = dense[0:2, :]

        def go(up):
            turn_copy(b, up, 0).start()
            turn_copy(b, up, 1).start()

        each_lat(go)

    def send_sides(b, part):
        k = 2 * b
        to_west, to_east = pack(lambda r, cut: basis[k, r + HALO, :, cut], True, channels, sided[part])
        side_out[b, part, 0] = to_west
        side_out[b, part, 1] = to_east
        lon_copy(b, part, 0).start()
        lon_copy(b, part, 1).start()

    def take_corners(b):
        got = jnp.zeros((2, 128), jnp.float32)
        sub = lax.rem(lax.broadcasted_iota(jnp.int32, (2, 128), 1), 32) // 8
        for n in range(4):
            got = jnp.where(sub == n, corner_in[b, n], got)
        got = jnp.concatenate([got] * 4, axis=0)
        small = got
        for g in range(1, 4):
            small = jnp.where(deep // 2 == g, pltpu.roll(got, 128 - 32 * g, 1), small)
        parts = []
        for h in range(channels // 8):
            part = jnp.zeros((8, 128), jnp.float32)
            for up in range(2):
                for way in range(2):
                    at = 16 * up + 8 * way + 4 * h
                    want = (64 if way else 0) + (2 * lat - 4 if up else 0)
                    here = (spot >= want) & (spot < want + 4)
                    part = jnp.where(here, pltpu.roll(small, (want - at) % 128, 1) if want != at else small, part)
            parts.append(part)
        return jnp.concatenate(parts, axis=0)

    def theta_of(k):
        theta = jnp.float32(THETA[0] * scale)
        for i in range(1, ITERS):
            theta = jnp.where(k == i, jnp.float32(THETA[i] * scale), theta)
        return theta

    def products(pairs, places, accs):
        for r in places:
            for h in range(channels // 8):
                for t in range(tiles):
                    at = (r + HALO, slice(8 * h, 8 * h + 8), slice(128 * t, 128 * t + 128))
                    held = {}

                    def read(k):
                        if id(k) not in held:
                            held[id(k)] = basis[(k,) + at]
                        return held[id(k)]

                    for n, (k, i) in enumerate(pairs):
                        m = (2 * h + t) % 2
                        accs[2 * n + m] = accs[2 * n + m] + read(k) * read(i)
        return accs

    def keep(k, i, acc, more):
        at = lax.div(k * (k + 1), 2) + i
        gram_acc[at] = gram_acc[at] + acc if more else acc

    def dots(pairs, first, count, more=False):
        zero = jnp.zeros((8, 128), jnp.float32)
        if count == 8:
            accs = products(pairs, [(j + first) % lat for j in range(8)],
                            [zero] * (2 * len(pairs)))
        else:
            def part(b, accs):
                return tuple(products(pairs, [b * 8 + j + first for j in range(8)], list(accs)))

            accs = lax.fori_loop(0, count // 8, part, (zero,) * (2 * len(pairs)))
        for n, (k, i) in enumerate(pairs):
            keep(k, i, accs[2 * n] + accs[2 * n + 1], more)

    def dots_two(k, first, count, more=False):
        def one(i, _):
            before = k - 1
            dots([(before, i), (k, i)], first, count, more)
            return 0

        lax.fori_loop(0, k, one, 0)
        dots([(k, k)], first, count, more)

    def split(stack):
        high = stack.astype(jnp.bfloat16)
        low = (stack - high.astype(jnp.float32)).astype(jnp.bfloat16)
        return jnp.concatenate([high, low, high], axis=0)

    def rows(k, picked, theta, beside, bare=False):
        stack = jnp.concatenate([basis[k, r + HALO] for r in picked], axis=0)
        mixed = lax.dot_general(block[...], split(stack), (((1,), (0,)), ((), ())), preferred_element_type=jnp.float32)
        for j, r in enumerate(picked):
            inside = 0 <= r < lat
            source = beside
            left = 2 * r if inside else 64 + 2 * (r % lat)
            right = 64 + 2 * r if inside else 2 * (r % lat)

            def turn(v, shift):
                return pltpu.roll(v, shift % 128, 1) if shift % 128 else v

            x = [basis[k, r + HALO, :, 128 * t:128 * t + 128] for t in range(tiles)]
            if source is None:
                ends = [jnp.zeros_like(lane, jnp.float32)] * 4
            else:
                ends = [turn(source, shift) for shift in (127 - right, 126 - right, -left - 1, -left)]
            fwd1 = [pltpu.roll(v, 127, 1) for v in x] + [ends[0]]
            fwd2 = [pltpu.roll(v, 126, 1) for v in x] + [ends[1]]
            bwd1 = [ends[2]] + [pltpu.roll(v, 1, 1) for v in x]
            bwd2 = [ends[3]] + [pltpu.roll(v, 2, 1) for v in x]
            for t in range(tiles):
                cut = slice(128 * t, 128 * t + 128)
                e1 = jnp.where(lane < 127, fwd1[t], fwd1[t + 1])
                e2 = jnp.where(lane < 126, fwd2[t], fwd2[t + 1])
                w1 = jnp.where(lane >= 1, bwd1[t + 1], bwd1[t])
                w2 = jnp.where(lane >= 2, bwd2[t + 1], bwd2[t])

                def weight(q):
                    return coef[r + 2, q:q + 1, cut]

                def near(d):
                    return basis[k, r + HALO + d, :, cut]

                def has(d):
                    return not bare or 0 <= r + d < lat

                value = (diag[r + 2, :, cut] - theta) * x[t] + mixed[channels * j:channels * (j + 1), cut]
                value = value + (weight(0) * e1 + weight(1) * w1 + weight(2) * (w2 - e2))
                if has(1):
                    value = value + weight(3) * near(1)
                if has(-1):
                    value = value + weight(4) * near(-1)
                if has(2) and has(-2):
                    value = value + weight(5) * (near(-2) - near(2))
                elif has(2):
                    value = value - weight(5) * near(2)
                else:
                    value = value + weight(5) * near(-2)
                basis[k + 1, r + HALO, :, cut] = value

    def middle(got):
        return jnp.where(lane < 64, got[1], pltpu.roll(got[0], 64, 1))

    def both(ref, b, part):
        return [ref[b, 0, way] + ref[b, 1, way] if part else ref[b, 0, way] for way in range(2)]

    row = lax.rem(lane, 64) // 2
    even = lax.rem(lane, 2) == 0

    def edge_coef(q):
        return jnp.where(spot[0:1] < 64, fixed_in[1, channels + q:channels + q + 1, :],
                         pltpu.roll(fixed_in[0, channels + q:channels + q + 1, :], 64, 1))

    def edge_band(got, given, theta, centre):
        from_east, from_west = got
        to_west, to_east = given
        low = jnp.where(lane < 64, pltpu.roll(from_west, 64, 1), pltpu.roll(to_east, 64, 1))
        high = jnp.where(lane < 64, to_west, from_east)
        e1 = jnp.where(even, pltpu.roll(centre, 127, 1), pltpu.roll(high, 1, 1))
        w1 = jnp.where(even, pltpu.roll(low, 127, 1), pltpu.roll(centre, 1, 1))
        n1 = jnp.where(row < lat - 1, pltpu.roll(centre, 126, 1), 0.0)
        n2 = jnp.where(row < lat - 2, pltpu.roll(centre, 124, 1), 0.0)
        s1 = jnp.where(row >= 1, pltpu.roll(centre, 2, 1), 0.0)
        s2 = jnp.where(row >= 2, pltpu.roll(centre, 4, 1), 0.0)
        mixed = lax.dot_general(single[...], split(centre), (((1,), (0,)), ((), ())), preferred_element_type=jnp.float32)
        own = jnp.where(lane < 64, fixed_in[1, 0:channels, :], pltpu.roll(fixed_in[0, 0:channels, :], 64, 1))
        value = (own - theta) * centre + mixed
        value = value + (edge_coef(0) * e1 + edge_coef(1) * w1 + edge_coef(2) * (low - high))
        return value + (edge_coef(3) * n1 + edge_coef(4) * s1 + edge_coef(5) * (s2 - n2))

    def edge_turn(corners):
        n1 = jnp.where(row < lat - 1, 0.0, pltpu.roll(corners, 126, 1))
        n2 = jnp.where(row < lat - 2, 0.0, pltpu.roll(corners, 124, 1))
        s1 = jnp.where(row >= 1, 0.0, pltpu.roll(corners, 2, 1))
        s2 = jnp.where(row >= 2, 0.0, pltpu.roll(corners, 4, 1))
        return edge_coef(3) * n1 + edge_coef(4) * s1 + edge_coef(5) * (s2 - n2)

    def add_sides(k, centre, picked):
        def own(q):
            return jnp.where(spot[0:1] < 64, fixed_out[0, channels + q:channels + q + 1, :],
                             pltpu.roll(fixed_out[1, channels + q:channels + q + 1, :], 64, 1))

        from_west = own(2) * centre + jnp.where(even, own(1) * pltpu.roll(centre, 127, 1), 0.0)
        from_east = jnp.where(even, 0.0, own(0) * pltpu.roll(centre, 1, 1)) - own(2) * centre
        for r in picked:
            left = pltpu.roll(from_west, (128 - 2 * r) % 128, 1) if r else from_west
            right = pltpu.roll(from_east, (62 - 2 * r) % 128, 1) if 2 * r != 62 else from_east
            basis[k + 1, r + HALO, :, 0:128] += jnp.where(lane < 2, left, 0.0)
            basis[k + 1, r + HALO, :, lon - 128:lon] += jnp.where(lane >= 126, right, 0.0)

    def stage(b, _):
        k = 2 * b
        theta, after = theta_of(k), theta_of(k + 1)
        for g in range((lat - 4) // GROUP):
            rows(k, [2 + GROUP * g + j for j in range(GROUP)], theta, None)
        rows(k, (0, 1, lat - 2, lat - 1), theta, None, bare=True)

        dots_two(k, 0, lat)
        more = b + 1 < BLOCKS
        for part in range(2):
            lon_copy(b, part, 0).wait()
            lon_copy(b, part, 1).wait()
            if part == 0:
                @pl.when(b == 0)
                def _():
                    fix_side(0).wait()
                    fix_side(1).wait()

            got = both(side_in, b, part)
            centre = middle(got)
            add_sides(k, centre, sided[part])
            band[...] = edge_band(got, both(side_out, b, part), theta, centre)
            beside = band[...]
            if part:
                rows(k + 1, (4, 5, lat - 6, lat - 5), after, beside)
            else:
                for g in range((lat - 12) // GROUP):
                    rows(k + 1, [6 + GROUP * g + j for j in range(GROUP)], after, beside)

        @pl.when(more)
        def _():
            send_sides(b + 1, 0)

        @pl.when(b + 1 == BLOCKS)
        def _():
            dots_two(k + 2, 4, lat - 8)

        def corners_in(way):
            turn_copy(b, way, 0).wait_recv()
            turn_copy(b, way, 1).wait_recv()

            @pl.when(b == 0)
            def _():
                for copy in wind_copies(way):
                    copy.wait_recv()
                fill_coef(wind_in[0, way], wind_in[1, way], kx_in[way, 6:8] if way else kx_in[way, 0:2], 0 if way else lat + 2)

        arrive_lat(lambda way: lat_copy(b, way, 1).wait_recv())
        beside = band[...]
        south, north = basis[k, HALO - 1], basis[k, HALO + lat]
        basis[k + 1, HALO] += coef[2, 4:5, :] * south + coef[2, 5:6, :] * basis[k, HALO - 2]
        basis[k + 1, HALO + 1] += coef[3, 5:6, :] * south
        basis[k + 1, HALO + lat - 1] += coef[lat + 1, 3:4, :] * north - coef[lat + 1, 5:6, :] * basis[k, HALO + lat + 1]
        basis[k + 1, HALO + lat - 2] -= coef[lat, 5:6, :] * north
        rows(k + 1, (2, 3, lat - 4, lat - 3), after, beside)

        @pl.when(more)
        def _():
            each_lat(lambda way: lat_copy(b + 1, way, 0).start())

        arrive_lat(corners_in)
        turned[0] = take_corners(b)
        turned[1] = band[...] + edge_turn(turned[0])

        def far_in(way):
            lat_copy(b, way, 0).wait_recv()

            @pl.when(b == 0)
            def _():
                diag_copy(way).wait_recv()

        arrive_lat(far_in)
        rows(k, (-2, -1, lat, lat + 1), theta, turned[0])
        rows(k + 1, (0, 1, lat - 2, lat - 1), after, turned[1])

        @pl.when(more)
        def _():
            send_corners(b + 1)
            each_lat(lambda way: lat_copy(b + 1, way, 1).start())
            send_sides(b + 1, 1)

        for n in range(min(words, BLOCKS)):
            @pl.when(b == n)
            def _():
                if n:
                    hear_word(n - 1)
                spread_word(n)

        if words < BLOCKS:
            @pl.when(b == words)
            def _():
                hear_word(words - 1)

        def sent(way):
            lat_copy(b, way, 0).wait_send()
            lat_copy(b, way, 1).wait_send()
            turn_copy(b, way, 0).wait_send()
            turn_copy(b, way, 1).wait_send()

            @pl.when(b == 0)
            def _():
                for copy in wind_copies(way) + [diag_copy(way)]:
                    copy.wait_send()

        each_lat(sent)
        return 0

    for copy in loads[0]:
        copy.wait()
    pl.semaphore_wait(barrier, 2 + jnp.where(iy > 0, 3, 0) + jnp.where(iy < ny - 1, 3, 0))
    def first_rows(way):
        lat_copy(0, way, 1).start()
        lat_copy(0, way, 0).start()

    each_lat(first_rows)
    send_corners(0)
    send_sides(0, 0)
    send_sides(0, 1)
    for copy in small:
        copy.wait()

    def first_winds(way):
        for copy in wind_copies(way):
            copy.start()

    each_lat(first_winds)
    place = (lax.broadcasted_iota(jnp.int32, (lat + 16, 128), 0) + iy * lat - 8).astype(jnp.float32)
    phi = -math.pi / 2 + (place + 0.5) * (math.pi / (lat * ny))
    kx = (DIFF_LON * scale) / (jnp.cos(phi) ** 2 + 0.1)
    kx_in[0] = kx[lat + 8:lat + 16]
    kx_in[1] = kx[0:8]
    fill_coef(wl_ref[...], wa_ref[...], kx[8:lat + 8], 2)
    for copy in loads[1]:
        copy.wait()

    def prepare(r, _):
        diag[r + 2] = diag[r + 2] * scale + coef[r + 2, 6:7, :]
        return 0

    for r in (0, 1, lat - 2, lat - 1):
        prepare(r, 0)
    each_lat(lambda way: diag_copy(way).start())
    lax.fori_loop(2, lat - 2, prepare, 0)
    fixed = [pack(lambda r, cut: diag[r + 2, :, cut], False, channels), pack(lambda r, cut: coef[r + 2, :, cut], False, 8)]
    for way in range(2):
        fixed_out[way, 0:channels, :] = fixed[0][way]
        fixed_out[way, channels:channels + 8, :] = fixed[1][way]
    fix_side(0).start()
    fix_side(1).start()
    single[...] = widen(c_ref[...], channels)[0].astype(jnp.bfloat16)
    tall = lax.dot_general(spread(size), c_ref[...], (((1,), (0,)), ((), ())), precision=HI,
                           preferred_element_type=jnp.float32)
    wide, across = widen(tall, size)
    down = lax.broadcasted_iota(jnp.int32, (size, 3 * size), 0)
    block[...] = jnp.where(down // channels == lax.rem(across, size) // channels, wide, 0.0).astype(jnp.bfloat16)
    lax.fori_loop(0, BLOCKS, stage, 0)
    for n in range(BLOCKS, words + 1):
        hear_word(n - 1)
        if n < words:
            spread_word(n)
    dots_two(ITERS, lat - 4, 8, True)

    sums = jnp.concatenate(
        [jnp.sum(gram_acc[n], axis=0, keepdims=True) for n in range(len(PAIRS))]
        + [jnp.zeros((128 - len(PAIRS), 128), jnp.float32)], axis=0)
    flat = lax.dot_general(jnp.ones((8, 128), jnp.float32), sums, (((1,), (1,)), ((), ())), precision=HI,
                           preferred_element_type=jnp.float32)
    slots[me] = flat[0:1, :]

    def share(to):
        return copy_to(slots.at[me], slots.at[me], red_send.at[0], red_recv.at[0], to)

    def wrap(v, n):
        return jnp.where(v >= n, v - n, v)

    for dx in range(nx):
        for dy in range(ny):
            if dx or dy:
                share((wrap(ix + dx, nx), wrap(iy + dy, ny))).start()
    others = slots.at[pl.ds(0, total - 1)]
    everyone = copy_to(others, others, red_send.at[0], red_recv.at[0], (east, iy))
    everyone.wait_recv()
    everyone.wait_send()
    whole = tree([slots[n] for n in range(total)])
    gram = [[None] * (ITERS + 1) for _ in range(ITERS + 1)]
    for n, (k, i) in enumerate(PAIRS):
        gram[k][i] = gram[i][k] = jnp.broadcast_to(whole[:, n:n + 1], (8, 128))
    answer, applied = small_solve(gram)
    for k in range(ITERS):
        splats[k] = answer[k]
    for k in range(ITERS + 1):
        splats[ITERS + k] = applied[k]


def finish(b_ref, w_ref, sol_hbm, res_hbm, outs, out_sem):
    channels, lat, lon = sol_hbm.shape
    stores = []
    for part in range(lat // 8):
        def one(j, _):
            r = 8 * part + j
            for h in range(channels // 8):
                for t in range(lon // 128):
                    at = (slice(8 * h, 8 * h + 8), slice(128 * t, 128 * t + 128))
                    x = b_ref[0, r + HALO, at[0], at[1]]
                    best = w_ref[0] * x
                    rest = x - w_ref[ITERS] * x
                    for k in range(1, ITERS + 1):
                        x = b_ref[k, r + HALO, at[0], at[1]]
                        if k < ITERS:
                            best = best + w_ref[k] * x
                        rest = rest - w_ref[ITERS + k] * x
                    outs[0, r, at[0], at[1]] = best
                    outs[1, r, at[0], at[1]] = rest
            return 0

        lax.fori_loop(0, 8, one, 0)
        for q, dst in enumerate((sol_hbm, res_hbm)):
            for c in range(channels):
                copy = pltpu.make_async_copy(outs.at[q, pl.ds(8 * part, 8), c, :], dst.at[c, pl.ds(8 * part, 8), :],
                                             out_sem.at[part, q, c])
                copy.start()
                stores.append(copy)
    for copy in stores:
        copy.wait()


def solution(mesh):
    nx, ny = mesh.shape["gx"], mesh.shape["gy"]

    def per_device(forcing, damping, coupling, wind_lon, wind_lat):
        channels, lat, lon = forcing.shape
        f32 = jnp.float32
        vmem = pl.BlockSpec(memory_space=pltpu.VMEM)
        hbm = pl.BlockSpec(memory_space=pltpu.HBM)
        dma = pltpu.SemaphoreType.DMA

        def keep(v):
            return pltpu.with_memory_space_constraint(v, pltpu.HBM)

        basis, weights = pl.pallas_call(
            functools.partial(kernel, nx, ny),
            out_shape=(pltpu.VMEM((ITERS + 1, lat + 2 * HALO + 1, channels + 8, lon), f32), pltpu.VMEM((2 * ITERS + 1, 8, 128), f32)),
            in_specs=[hbm] * 5,
            out_specs=(vmem, vmem),
            scratch_shapes=[
                pltpu.VMEM((lat + 4, channels, lon), f32),
                pltpu.VMEM((lat + 4, 8, lon), f32),
                pltpu.VMEM((GROUP * channels, 3 * GROUP * channels), jnp.bfloat16),
                pltpu.VMEM((channels, 3 * channels), jnp.bfloat16),
                pltpu.VMEM((BLOCKS, 2, 2, channels, 128), f32),
                pltpu.VMEM((BLOCKS, 2, 2, channels, 128), f32),
                pltpu.VMEM((channels, 128), f32),
                pltpu.VMEM((2, channels + 8, 128), f32),
                pltpu.VMEM((2, channels + 8, 128), f32),
                pltpu.VMEM((BLOCKS, 4, 2, 128), f32),
                pltpu.VMEM((BLOCKS, 2, 128), f32),
                pltpu.VMEM((len(PAIRS), 8, 128), f32),
                pltpu.VMEM((nx * ny, 1, 128), f32),
                pltpu.VMEM((channels, channels), f32), pltpu.VMEM((lat, lon), f32), pltpu.VMEM((lat, lon), f32),
                pltpu.VMEM((2, 2, 2, lon), f32), pltpu.VMEM((2, 8, 128), f32), pltpu.VMEM((2, channels, 128), f32),
                dma((2, channels)), dma((3,)),
                dma((BLOCKS, 2, 2)), dma((BLOCKS, 2, 2)), dma((BLOCKS, 2, 2)), dma((BLOCKS, 2, 2)),
                dma((BLOCKS, 4)), dma((BLOCKS, 4)), dma((4, 2)), dma((4, 2)),
                dma((1,)), dma((1,)), pltpu.SemaphoreType.REGULAR((8,)),
            ],
            compiler_params=pltpu.CompilerParams(
                collective_id=0, has_side_effects=True, vmem_limit_bytes=24 * 1024 * 1024),
        )(*map(keep, (forcing, damping, coupling, wind_lon, wind_lat)))
        shape = jax.ShapeDtypeStruct((channels, lat, lon), f32)
        return pl.pallas_call(
            finish,
            out_shape=(shape, shape),
            in_specs=[vmem, vmem],
            out_specs=(hbm, hbm),
            scratch_shapes=[pltpu.VMEM((2, lat, channels, lon), f32), dma((lat // 8, 2, channels))],
            compiler_params=pltpu.CompilerParams(vmem_limit_bytes=24 * 1024 * 1024),
        )(basis, weights)

    return jax.shard_map(
        per_device,
        mesh=mesh,
        in_specs=(P(None, "gy", "gx"), P(None, "gy", "gx"), P(), P("gy", "gx"), P("gy", "gx")),
        out_specs=(P(None, "gy", "gx"), P(None, "gy", "gx")),
        check_vma=False,
    )
```

```python
import functools
import math

import jax
import jax.numpy as jnp
from jax import lax
from jax.experimental import pallas as pl
from jax.experimental.pallas import tpu as pltpu
from jax.sharding import PartitionSpec as P

ITERS = 8
COUPLE = 0.25
DIFF_LAT = 0.5
DIFF_LON = 0.5
GUARD = 1.0
MESH = pl.DeviceIdType.MESH
HI = lax.Precision.HIGHEST

MIDDLE = 9.0
RADIUS = 6.0
WIDTH = 3.0
THETA = [MIDDLE + RADIUS * math.cos(math.pi * (2 * k + 1) / (2 * ITERS)) for k in (7, 0, 4, 2, 6, 1, 5, 3)]
PAIRS = [(k, i) for k in range(ITERS + 1) for i in range(k + 1)]
GROUP = 4
HALO = 4
BLOCKS = ITERS // 2


def apply_to(coords):
    out = [None] * (len(coords) + 1)
    for k, value in enumerate(coords):
        low = THETA[k] * value if k < ITERS else value
        out[k] = low if out[k] is None else out[k] + low
        out[k + 1] = WIDTH * value
    return out


def tree(terms):
    while len(terms) > 1:
        terms = [a + b for a, b in zip(terms[::2], terms[1::2])] + ([terms[-1]] if len(terms) % 2 else [])
    return terms[0]


def small_solve(gram):
    first = jnp.sqrt(gram[0][0] + GUARD)
    coords = [[1.0 / first]]
    images = [[gram[i][0] * coords[0][0] for i in range(ITERS + 1)]]
    heights = []
    for j in range(ITERS):
        moved = apply_to(coords[j])
        column = []
        for i in range(j + 1):
            column.append(tree([images[i][k] * moved[k] for k in range(j + 2)]))
        left = list(moved)
        for k in range(j + 1):
            left[k] = left[k] - tree([column[i] * coords[i][k] for i in range(k, j + 1)])
        image = [
            tree([gram[r][k] * left[k] for k in range(j + 2)])
            for r in range(ITERS + 1)
        ]
        norm_sq = tree([image[k] * left[k] for k in range(j + 2)])
        subdiag = jnp.sqrt(jnp.maximum(norm_sq, 0.0) + GUARD)
        column.append(subdiag)
        heights.append(column)
        inverse = 1.0 / subdiag
        coords.append([v * inverse for v in left])
        images.append([v * inverse for v in image])
    cosines, sines, target, rotated = [], [], [first], []
    for j in range(ITERS):
        column = list(heights[j])
        for e in range(j):
            upper, lower = column[e], column[e + 1]
            column[e] = cosines[e] * upper + sines[e] * lower
            column[e + 1] = cosines[e] * lower - sines[e] * upper
        upper, lower = column[j], column[j + 1]
        radius = jnp.sqrt(upper * upper + lower * lower)
        inverse = 1.0 / radius
        cosine, sine = upper * inverse, lower * inverse
        column[j] = radius
        kept = target[j]
        target[j] = cosine * kept
        target.append(-sine * kept)
        cosines.append(cosine)
        sines.append(sine)
        rotated.append(column)
    weights = [None] * ITERS
    for j in reversed(range(ITERS)):
        value = target[j]
        for later in range(j + 1, ITERS):
            value = value - rotated[later][j] * weights[later]
        weights[j] = value / rotated[j][j]
    answer = [None] * ITERS
    for j in range(ITERS):
        for k in range(j + 1):
            term = weights[j] * coords[j][k]
            answer[k] = term if answer[k] is None else answer[k] + term
    return answer, apply_to(answer)


def word_plan(nx, ny):
    def doubled(n):
        out = [2]
        while out[-1] < n:
            out.append(2 * out[-1])
        return out[:-1]

    far_lat, far_lon = doubled(ny), doubled(nx // 2 + 1)
    words = max(len(far_lat), len(far_lon))
    reach = {}
    for x in range(nx):
        for y in range(ny):
            reach[x, y] = {((x + dx) % nx, y + dy) for dx in (-1, 0, 1) for dy in (-1, 0, 1) if 0 <= y + dy < ny}
    near = {place: set(known) for place, known in reach.items()}

    def peers(x, y, n):
        out = []
        if n < len(far_lat):
            out += [(x, y + d) for d in (-far_lat[n], far_lat[n]) if 0 <= y + d < ny]
        if n < len(far_lon):
            out += [((x + d) % nx, y) for d in (-far_lon[n], far_lon[n])]
        return out

    told = None
    for n in range(BLOCKS):
        before = reach
        reach = {place: set().union(*(before[other] for other in near[place])) for place in before}
        if told is not None:
            reach = {place: known.union(*(told[other] for other in peers(*place, n - 1))) for place, known in reach.items()}
        told = reach
    if any(len(known) < nx * ny for known in reach.values()):
        far_lon = far_lon + [nx // 2] * (max(BLOCKS, words + 1) - len(far_lon))
    return far_lat, far_lon


def kernel(nx, ny, f_hbm, d_hbm, c_hbm, wl_hbm, wa_hbm, padded, splats,
           diag, coef, block, single, side_in, side_out, band, fixed_in, fixed_out, corner_in, corner_out,
           gram_acc, slots, c_ref, wl_ref, wa_ref, wind_in, kx_in, turned,
           in_sem, wind_sem, lat_send, lat_recv, lon_send, lon_recv, turn_send, turn_recv, fix_send, fix_recv, red_send, red_recv, word):
    channels, lat, lon = f_hbm.shape
    tiles = lon // 128
    basis = padded.at[:, :, pl.ds(0, channels), :]
    total = nx * ny
    ix, iy = lax.axis_index("gx"), lax.axis_index("gy")
    me = ix * ny + iy
    east, west = lax.rem(ix + 1, nx), lax.rem(ix + nx - 1, nx)

    small = [pltpu.make_async_copy(src, dst, wind_sem.at[n])
             for n, (src, dst) in enumerate(((wl_hbm, wl_ref), (wa_hbm, wa_ref), (c_hbm, c_ref)))]
    for copy in small:
        copy.start()
    loads = [[], []]
    for q, (src, dst, off) in enumerate(((f_hbm, basis.at[0], HALO), (d_hbm, diag, 2))):
        for c in range(channels):
            copy = pltpu.make_async_copy(src.at[c], dst.at[pl.ds(off, lat), c, :], in_sem.at[q, c])
            copy.start()
            loads[q].append(copy)

    barrier = pltpu.get_barrier_semaphore()

    def greet(to, sem=barrier):
        pl.semaphore_signal(sem, inc=1, device_id=to, device_id_type=MESH)

    greet((east, iy))
    greet((west, iy))

    def greet_lat(to):
        greet((ix, to))
        greet((east, to))
        greet((west, to))

    @pl.when(iy > 0)
    def _():
        greet_lat(iy - 1)

    @pl.when(iy < ny - 1)
    def _():
        greet_lat(iy + 1)

    far_lat, far_lon = word_plan(nx, ny)

    def spread_word(n):
        if n < len(far_lat):
            d = far_lat[n]

            @pl.when(iy >= d)
            def _():
                greet((ix, iy - d), word.at[n])

            @pl.when(iy + d < ny)
            def _():
                greet((ix, iy + d), word.at[n])

        if n < len(far_lon):
            greet((lax.rem(ix + far_lon[n], nx), iy), word.at[n])
            greet((lax.rem(ix + nx - far_lon[n], nx), iy), word.at[n])

    def hear_word(n):
        count = 2 if n < len(far_lon) else 0
        if n < len(far_lat):
            d = far_lat[n]
            count = count + jnp.where(iy >= d, 1, 0) + jnp.where(iy + d < ny, 1, 0)
        pl.semaphore_wait(word.at[n], count)

    words = max(len(far_lat), len(far_lon))

    scale = 1.0 / WIDTH
    size = GROUP * channels

    def spread(n):
        row = lax.broadcasted_iota(jnp.int32, (n, channels), 0)
        col = lax.broadcasted_iota(jnp.int32, (n, channels), 1)
        return jnp.where(lax.rem(row, channels) == col, 1.0, 0.0).astype(jnp.float32)

    def widen(tall, n):
        wide = lax.dot_general(tall, spread(3 * n), (((1,), (1,)), ((), ())), precision=HI,
                               preferred_element_type=jnp.float32) * (COUPLE * scale)
        across = lax.broadcasted_iota(jnp.int32, wide.shape, 1)
        high = wide.astype(jnp.bfloat16).astype(jnp.float32)
        return jnp.where(across < 2 * n, high, wide - high), across

    def blank(at):
        for b in range(BLOCKS):
            basis[2 * b, pl.ds(HALO + lat if at else 0, HALO)] = jnp.zeros((HALO, channels, lon), jnp.float32)
        diag[pl.ds(lat + 2 if at else 0, 2)] = jnp.zeros((2, channels, lon), jnp.float32)
        coef[pl.ds(lat + 2 if at else 0, 2)] = jnp.zeros((2, 8, lon), jnp.float32)
        corner_in[:, 0 if at else 2] = jnp.zeros((BLOCKS, 2, 128), jnp.float32)
        corner_in[:, 1 if at else 3] = jnp.zeros((BLOCKS, 2, 128), jnp.float32)

    @pl.when(iy == 0)
    def _():
        blank(0)

    @pl.when(iy == ny - 1)
    def _():
        blank(1)

    def fill_coef(wl, wa, kx, at):
        wl, wa = wl * (scale / 12.0), wa * (scale / 12.0)
        kx = jnp.concatenate([kx] * tiles, axis=1)
        planes = (8.0 * wl - kx, -8.0 * wl - kx, wl, 8.0 * wa - DIFF_LAT * scale, -8.0 * wa - DIFF_LAT * scale, wa,
                  2.0 * kx + (1.0 + 2.0 * DIFF_LAT) * scale, jnp.zeros_like(kx))
        for q, plane in enumerate(planes):
            for r in range(wl.shape[0]):
                coef[r + at, q:q + 1, :] = plane[r:r + 1, :]

    def pack(read, far, n, picked=None):
        lane = lax.broadcasted_iota(jnp.int32, (n, 128), 1)
        to_west = to_east = jnp.zeros((n, 128), jnp.float32)
        for r in picked or range(lat):
            head = read(r, slice(0, 128))
            tail = read(r, slice(lon - 128, lon))
            here = (lane >= 2 * r) & (lane < 2 * r + 2)
            to_west = jnp.where(here, pltpu.roll(head, 2 * r, 1) if r else head, to_west)
            to_east = jnp.where(here, pltpu.roll(tail, (2 * r + 2) % 128, 1), to_east)
            if far:
                here = (lane >= 64 + 2 * r) & (lane < 64 + 2 * r + 2)
                to_west = jnp.where(here, pltpu.roll(head, (62 + 2 * r) % 128, 1), to_west)
                to_east = jnp.where(here, pltpu.roll(tail, (68 + 2 * r) % 128, 1), to_east)
        return to_west, to_east

    lane = lax.broadcasted_iota(jnp.int32, (channels, 128), 1)
    spot = lax.broadcasted_iota(jnp.int32, (8, 128), 1)
    deep = lax.broadcasted_iota(jnp.int32, (8, 128), 0)

    def copy_to(src, dst, send, recv, to):
        return pltpu.make_async_remote_copy(src_ref=src, dst_ref=dst, send_sem=send, recv_sem=recv,
                                            device_id=to, device_id_type=MESH)

    def lat_to(way):
        return iy + 1 if way else iy - 1

    def lat_copy(b, way, near):
        if way:
            src, dst = HALO + lat - (2 if near else 4), 2 if near else 0
        else:
            src, dst = HALO + (0 if near else 2), HALO + lat + (0 if near else 2)
        return copy_to(basis.at[2 * b, pl.ds(src, 2)], basis.at[2 * b, pl.ds(dst, 2)], lat_send.at[b, way, near],
                       lat_recv.at[b, way, near], (ix, lat_to(way)))

    def diag_copy(way):
        src = pl.ds(lat, 2) if way else pl.ds(2, 2)
        dst = pl.ds(0, 2) if way else pl.ds(lat + 2, 2)
        return copy_to(diag.at[src], diag.at[dst], fix_send.at[0, way], fix_recv.at[0, way], (ix, lat_to(way)))

    def wind_copies(way):
        src = pl.ds(lat - 2, 2) if way else pl.ds(0, 2)
        return [copy_to(ref.at[src], wind_in.at[n, way], fix_send.at[1 + n, way], fix_recv.at[1 + n, way], (ix, lat_to(way)))
                for n, ref in enumerate((wl_ref, wa_ref))]

    def fix_side(way):
        return copy_to(fixed_out.at[way], fixed_in.at[way], fix_send.at[3, way], fix_recv.at[3, way],
                       (east if way else west, iy))

    def lon_copy(b, part, way):
        return copy_to(side_out.at[b, part, way], side_in.at[b, part, way], lon_send.at[b, part, way],
                       lon_recv.at[b, part, way], (east if way else west, iy))

    sided = (list(range(4, lat - 4)), list(range(4)) + list(range(lat - 4, lat)))

    def turn_copy(b, up, way):
        n = 2 * up + way
        return copy_to(corner_out.at[b], corner_in.at[b, n], turn_send.at[b, n], turn_recv.at[b, n],
                       (east if way else west, lat_to(up)))

    def each_lat(act):
        @pl.when(iy < ny - 1)
        def _():
            act(1)

        @pl.when(iy > 0)
        def _():
            act(0)

    def arrive_lat(act):
        @pl.when(iy > 0)
        def _():
            act(1)

        @pl.when(iy < ny - 1)
        def _():
            act(0)

    def send_corners(b):
        k = 2 * b
        small = jnp.zeros((8, 128), jnp.float32)
        for up in range(2):
            for way in range(2):
                for h in range(channels // 8):
                    for j in range(2):
                        at = 16 * up + 8 * way + 4 * h + 2 * j
                        here = (spot >= at) & (spot < at + 2)
                        cut = slice(lon - 128, lon) if way else slice(0, 128)
                        part = basis[k, HALO + (lat - 2 if up else 0) + j, 8 * h:8 * h + 8, cut]
                        move = (at - (126 if way else 0)) % 128
                        small = jnp.where(here, pltpu.roll(part, move, 1) if move else part, small)
        dense = small
        for g in range(1, 4):
            moved = pltpu.roll(pltpu.roll(small, 8 - 2 * g, 0), 32 * g, 1)
            dense = jnp.where(spot // 32 == g, moved, dense)
        corner_out[b] = dense[0:2, :]

        def go(up):
            turn_copy(b, up, 0).start()
            turn_copy(b, up, 1).start()

        each_lat(go)

    def send_sides(b, part):
        k = 2 * b
        to_west, to_east = pack(lambda r, cut: basis[k, r + HALO, :, cut], True, channels, sided[part])
        side_out[b, part, 0] = to_west
        side_out[b, part, 1] = to_east
        lon_copy(b, part, 0).start()
        lon_copy(b, part, 1).start()

    def take_corners(b):
        got = jnp.zeros((2, 128), jnp.float32)
        sub = lax.rem(lax.broadcasted_iota(jnp.int32, (2, 128), 1), 32) // 8
        for n in range(4):
            got = jnp.where(sub == n, corner_in[b, n], got)
        got = jnp.concatenate([got] * 4, axis=0)
        small = got
        for g in range(1, 4):
            small = jnp.where(deep // 2 == g, pltpu.roll(got, 128 - 32 * g, 1), small)
        parts = []
        for h in range(channels // 8):
            part = jnp.zeros((8, 128), jnp.float32)
            for up in range(2):
                for way in range(2):
                    at = 16 * up + 8 * way + 4 * h
                    want = (64 if way else 0) + (2 * lat - 4 if up else 0)
                    here = (spot >= want) & (spot < want + 4)
                    part = jnp.where(here, pltpu.roll(small, (want - at) % 128, 1) if want != at else small, part)
            parts.append(part)
        return jnp.concatenate(parts, axis=0)

    def theta_of(k):
        theta = jnp.float32(THETA[0] * scale)
        for i in range(1, ITERS):
            theta = jnp.where(k == i, jnp.float32(THETA[i] * scale), theta)
        return theta

    def products(pairs, places, accs):
        for r in places:
            for h in range(channels // 8):
                for t in range(tiles):
                    at = (r + HALO, slice(8 * h, 8 * h + 8), slice(128 * t, 128 * t + 128))
                    held = {}

                    def read(k):
                        if id(k) not in held:
                            held[id(k)] = basis[(k,) + at]
                        return held[id(k)]

                    for n, (k, i) in enumerate(pairs):
                        m = (2 * h + t) % 2
                        accs[2 * n + m] = accs[2 * n + m] + read(k) * read(i)
        return accs

    def keep(k, i, acc, more):
        at = lax.div(k * (k + 1), 2) + i
        gram_acc[at] = gram_acc[at] + acc if more else acc

    def dots(pairs, first, count, more=False):
        zero = jnp.zeros((8, 128), jnp.float32)
        if count == 8:
            accs = products(pairs, [(j + first) % lat for j in range(8)],
                            [zero] * (2 * len(pairs)))
        else:
            def part(b, accs):
                return tuple(products(pairs, [b * 8 + j + first for j in range(8)], list(accs)))

            accs = lax.fori_loop(0, count // 8, part, (zero,) * (2 * len(pairs)))
        for n, (k, i) in enumerate(pairs):
            keep(k, i, accs[2 * n] + accs[2 * n + 1], more)

    def dots_two(k, first, count, more=False):
        def one(i, _):
            before = k - 1
            dots([(before, i), (k, i)], first, count, more)
            return 0

        lax.fori_loop(0, k, one, 0)
        dots([(k, k)], first, count, more)

    def split(stack):
        high = stack.astype(jnp.bfloat16)
        low = (stack - high.astype(jnp.float32)).astype(jnp.bfloat16)
        return jnp.concatenate([high, low, high], axis=0)

    def rows(k, picked, theta, beside, bare=False):
        stack = jnp.concatenate([basis[k, r + HALO] for r in picked], axis=0)
        mixed = lax.dot_general(block[...], split(stack), (((1,), (0,)), ((), ())), preferred_element_type=jnp.float32)
        for j, r in enumerate(picked):
            inside = 0 <= r < lat
            source = beside
            left = 2 * r if inside else 64 + 2 * (r % lat)
            right = 64 + 2 * r if inside else 2 * (r % lat)

            def turn(v, shift):
                return pltpu.roll(v, shift % 128, 1) if shift % 128 else v

            x = [basis[k, r + HALO, :, 128 * t:128 * t + 128] for t in range(tiles)]
            if source is None:
                ends = [jnp.zeros_like(lane, jnp.float32)] * 4
            else:
                ends = [turn(source, shift) for shift in (127 - right, 126 - right, -left - 1, -left)]
            fwd1 = [pltpu.roll(v, 127, 1) for v in x] + [ends[0]]
            fwd2 = [pltpu.roll(v, 126, 1) for v in x] + [ends[1]]
            bwd1 = [ends[2]] + [pltpu.roll(v, 1, 1) for v in x]
            bwd2 = [ends[3]] + [pltpu.roll(v, 2, 1) for v in x]
            for t in range(tiles):
                cut = slice(128 * t, 128 * t + 128)
                e1 = jnp.where(lane < 127, fwd1[t], fwd1[t + 1])
                e2 = jnp.where(lane < 126, fwd2[t], fwd2[t + 1])
                w1 = jnp.where(lane >= 1, bwd1[t + 1], bwd1[t])
                w2 = jnp.where(lane >= 2, bwd2[t + 1], bwd2[t])

                def weight(q):
                    return coef[r + 2, q:q + 1, cut]

                def near(d):
                    return basis[k, r + HALO + d, :, cut]

                def has(d):
                    return not bare or 0 <= r + d < lat

                value = (diag[r + 2, :, cut] - theta) * x[t] + mixed[channels * j:channels * (j + 1), cut]
                value = value + (weight(0) * e1 + weight(1) * w1 + weight(2) * (w2 - e2))
                if has(1):
                    value = value + weight(3) * near(1)
                if has(-1):
                    value = value + weight(4) * near(-1)
                if has(2) and has(-2):
                    value = value + weight(5) * (near(-2) - near(2))
                elif has(2):
                    value = value - weight(5) * near(2)
                else:
                    value = value + weight(5) * near(-2)
                basis[k + 1, r + HALO, :, cut] = value

    def middle(got):
        return jnp.where(lane < 64, got[1], pltpu.roll(got[0], 64, 1))

    def both(ref, b, part):
        return [ref[b, 0, way] + ref[b, 1, way] if part else ref[b, 0, way] for way in range(2)]

    row = lax.rem(lane, 64) // 2
    even = lax.rem(lane, 2) == 0

    def edge_coef(q):
        return jnp.where(spot[0:1] < 64, fixed_in[1, channels + q:channels + q + 1, :],
                         pltpu.roll(fixed_in[0, channels + q:channels + q + 1, :], 64, 1))

    def edge_band(got, given, theta, centre):
        from_east, from_west = got
        to_west, to_east = given
        low = jnp.where(lane < 64, pltpu.roll(from_west, 64, 1), pltpu.roll(to_east, 64, 1))
        high = jnp.where(lane < 64, to_west, from_east)
        e1 = jnp.where(even, pltpu.roll(centre, 127, 1), pltpu.roll(high, 1, 1))
        w1 = jnp.where(even, pltpu.roll(low, 127, 1), pltpu.roll(centre, 1, 1))
        n1 = jnp.where(row < lat - 1, pltpu.roll(centre, 126, 1), 0.0)
        n2 = jnp.where(row < lat - 2, pltpu.roll(centre, 124, 1), 0.0)
        s1 = jnp.where(row >= 1, pltpu.roll(centre, 2, 1), 0.0)
        s2 = jnp.where(row >= 2, pltpu.roll(centre, 4, 1), 0.0)
        mixed = lax.dot_general(single[...], split(centre), (((1,), (0,)), ((), ())), preferred_element_type=jnp.float32)
        own = jnp.where(lane < 64, fixed_in[1, 0:channels, :], pltpu.roll(fixed_in[0, 0:channels, :], 64, 1))
        value = (own - theta) * centre + mixed
        value = value + (edge_coef(0) * e1 + edge_coef(1) * w1 + edge_coef(2) * (low - high))
        return value + (edge_coef(3) * n1 + edge_coef(4) * s1 + edge_coef(5) * (s2 - n2))

    def edge_turn(corners):
        n1 = jnp.where(row < lat - 1, 0.0, pltpu.roll(corners, 126, 1))
        n2 = jnp.where(row < lat - 2, 0.0, pltpu.roll(corners, 124, 1))
        s1 = jnp.where(row >= 1, 0.0, pltpu.roll(corners, 2, 1))
        s2 = jnp.where(row >= 2, 0.0, pltpu.roll(corners, 4, 1))
        return edge_coef(3) * n1 + edge_coef(4) * s1 + edge_coef(5) * (s2 - n2)

    def add_sides(k, centre, picked):
        def own(q):
            return jnp.where(spot[0:1] < 64, fixed_out[0, channels + q:channels + q + 1, :],
                             pltpu.roll(fixed_out[1, channels + q:channels + q + 1, :], 64, 1))

        from_west = own(2) * centre + jnp.where(even, own(1) * pltpu.roll(centre, 127, 1), 0.0)
        from_east = jnp.where(even, 0.0, own(0) * pltpu.roll(centre, 1, 1)) - own(2) * centre
        for r in picked:
            left = pltpu.roll(from_west, (128 - 2 * r) % 128, 1) if r else from_west
            right = pltpu.roll(from_east, (62 - 2 * r) % 128, 1) if 2 * r != 62 else from_east
            basis[k + 1, r + HALO, :, 0:128] += jnp.where(lane < 2, left, 0.0)
            basis[k + 1, r + HALO, :, lon - 128:lon] += jnp.where(lane >= 126, right, 0.0)

    def stage(b, _):
        k = 2 * b
        theta, after = theta_of(k), theta_of(k + 1)
        for g in range((lat - 4) // GROUP):
            rows(k, [2 + GROUP * g + j for j in range(GROUP)], theta, None)
        rows(k, (0, 1, lat - 2, lat - 1), theta, None, bare=True)

        dots_two(k, 0, lat)
        more = b + 1 < BLOCKS
        for part in range(2):
            lon_copy(b, part, 0).wait()
            lon_copy(b, part, 1).wait()
            if part == 0:
                @pl.when(b == 0)
                def _():
                    fix_side(0).wait()
                    fix_side(1).wait()

            got = both(side_in, b, part)
            centre = middle(got)
            add_sides(k, centre, sided[part])
            band[...] = edge_band(got, both(side_out, b, part), theta, centre)
            beside = band[...]
            if part:
                rows(k + 1, (4, 5, lat - 6, lat - 5), after, beside)
            else:
                for g in range((lat - 12) // GROUP):
                    rows(k + 1, [6 + GROUP * g + j for j in range(GROUP)], after, beside)

        @pl.when(more)
        def _():
            send_sides(b + 1, 0)

        @pl.when(b + 1 == BLOCKS)
        def _():
            dots_two(k + 2, 4, lat - 8)

        def corners_in(way):
            turn_copy(b, way, 0).wait_recv()
            turn_copy(b, way, 1).wait_recv()

            @pl.when(b == 0)
            def _():
                for copy in wind_copies(way):
                    copy.wait_recv()
                fill_coef(wind_in[0, way], wind_in[1, way], kx_in[way, 6:8] if way else kx_in[way, 0:2], 0 if way else lat + 2)

        arrive_lat(lambda way: lat_copy(b, way, 1).wait_recv())
        beside = band[...]
        south, north = basis[k, HALO - 1], basis[k, HALO + lat]
        basis[k + 1, HALO] += coef[2, 4:5, :] * south + coef[2, 5:6, :] * basis[k, HALO - 2]
        basis[k + 1, HALO + 1] += coef[3, 5:6, :] * south
        basis[k + 1, HALO + lat - 1] += coef[lat + 1, 3:4, :] * north - coef[lat + 1, 5:6, :] * basis[k, HALO + lat + 1]
        basis[k + 1, HALO + lat - 2] -= coef[lat, 5:6, :] * north
        rows(k + 1, (2, 3, lat - 4, lat - 3), after, beside)

        @pl.when(more)
        def _():
            each_lat(lambda way: lat_copy(b + 1, way, 0).start())

        arrive_lat(corners_in)
        turned[0] = take_corners(b)
        turned[1] = band[...] + edge_turn(turned[0])

        def far_in(way):
            lat_copy(b, way, 0).wait_recv()

            @pl.when(b == 0)
            def _():
                diag_copy(way).wait_recv()

        arrive_lat(far_in)
        rows(k, (-2, -1, lat, lat + 1), theta, turned[0])
        rows(k + 1, (0, 1, lat - 2, lat - 1), after, turned[1])

        @pl.when(more)
        def _():
            each_lat(lambda way: lat_copy(b + 1, way, 1).start())
            send_corners(b + 1)
            send_sides(b + 1, 1)

        for n in range(min(words, BLOCKS)):
            @pl.when(b == n)
            def _():
                if n:
                    hear_word(n - 1)
                spread_word(n)

        if words < BLOCKS:
            @pl.when(b == words)
            def _():
                hear_word(words - 1)

        def sent(way):
            lat_copy(b, way, 0).wait_send()
            lat_copy(b, way, 1).wait_send()
            turn_copy(b, way, 0).wait_send()
            turn_copy(b, way, 1).wait_send()

            @pl.when(b == 0)
            def _():
                for copy in wind_copies(way) + [diag_copy(way)]:
                    copy.wait_send()

        each_lat(sent)
        return 0

    for copy in loads[0]:
        copy.wait()
    pl.semaphore_wait(barrier, 2 + jnp.where(iy > 0, 3, 0) + jnp.where(iy < ny - 1, 3, 0))
    def first_rows(way):
        lat_copy(0, way, 1).start()
        lat_copy(0, way, 0).start()

    each_lat(first_rows)
    send_corners(0)
    send_sides(0, 0)
    send_sides(0, 1)
    for copy in small:
        copy.wait()

    def first_winds(way):
        for copy in wind_copies(way):
            copy.start()

    each_lat(first_winds)
    place = (lax.broadcasted_iota(jnp.int32, (lat + 16, 128), 0) + iy * lat - 8).astype(jnp.float32)
    phi = -math.pi / 2 + (place + 0.5) * (math.pi / (lat * ny))
    kx = (DIFF_LON * scale) / (jnp.cos(phi) ** 2 + 0.1)
    kx_in[0] = kx[lat + 8:lat + 16]
    kx_in[1] = kx[0:8]
    fill_coef(wl_ref[...], wa_ref[...], kx[8:lat + 8], 2)
    for copy in loads[1]:
        copy.wait()

    def prepare(r, _):
        diag[r + 2] = diag[r + 2] * scale + coef[r + 2, 6:7, :]
        return 0

    for r in (0, 1, lat - 2, lat - 1):
        prepare(r, 0)
    each_lat(lambda way: diag_copy(way).start())
    lax.fori_loop(2, lat - 2, prepare, 0)
    fixed = [pack(lambda r, cut: diag[r + 2, :, cut], False, channels), pack(lambda r, cut: coef[r + 2, :, cut], False, 8)]
    for way in range(2):
        fixed_out[way, 0:channels, :] = fixed[0][way]
        fixed_out[way, channels:channels + 8, :] = fixed[1][way]
    fix_side(0).start()
    fix_side(1).start()
    single[...] = widen(c_ref[...], channels)[0].astype(jnp.bfloat16)
    tall = lax.dot_general(spread(size), c_ref[...], (((1,), (0,)), ((), ())), precision=HI,
                           preferred_element_type=jnp.float32)
    wide, across = widen(tall, size)
    down = lax.broadcasted_iota(jnp.int32, (size, 3 * size), 0)
    block[...] = jnp.where(down // channels == lax.rem(across, size) // channels, wide, 0.0).astype(jnp.bfloat16)
    lax.fori_loop(0, BLOCKS, stage, 0)
    for n in range(BLOCKS, words + 1):
        hear_word(n - 1)
        if n < words:
            spread_word(n)
    dots_two(ITERS, lat - 4, 8, True)

    sums = jnp.concatenate(
        [jnp.sum(gram_acc[n], axis=0, keepdims=True) for n in range(len(PAIRS))]
        + [jnp.zeros((128 - len(PAIRS), 128), jnp.float32)], axis=0)
    flat = lax.dot_general(jnp.ones((8, 128), jnp.float32), sums, (((1,), (1,)), ((), ())), precision=HI,
                           preferred_element_type=jnp.float32)
    slots[me] = flat[0:1, :]

    def share(to):
        return copy_to(slots.at[me], slots.at[me], red_send.at[0], red_recv.at[0], to)

    def wrap(v, n):
        return jnp.where(v >= n, v - n, v)

    for dx in range(nx):
        for dy in range(ny):
            if dx or dy:
                share((wrap(ix + dx, nx), wrap(iy + dy, ny))).start()
    others = slots.at[pl.ds(0, total - 1)]
    everyone = copy_to(others, others, red_send.at[0], red_recv.at[0], (east, iy))
    everyone.wait_recv()
    everyone.wait_send()
    whole = tree([slots[n] for n in range(total)])
    gram = [[None] * (ITERS + 1) for _ in range(ITERS + 1)]
    for n, (k, i) in enumerate(PAIRS):
        gram[k][i] = gram[i][k] = jnp.broadcast_to(whole[:, n:n + 1], (8, 128))
    answer, applied = small_solve(gram)
    for k in range(ITERS):
        splats[k] = answer[k]
    for k in range(ITERS + 1):
        splats[ITERS + k] = applied[k]


def finish(b_ref, w_ref, sol_hbm, res_hbm, outs, out_sem):
    channels, lat, lon = sol_hbm.shape
    stores = []
    for part in range(lat // 8):
        def one(j, _):
            r = 8 * part + j
            for h in range(channels // 8):
                for t in range(lon // 128):
                    at = (slice(8 * h, 8 * h + 8), slice(128 * t, 128 * t + 128))
                    x = b_ref[0, r + HALO, at[0], at[1]]
                    best = w_ref[0] * x
                    rest = x - w_ref[ITERS] * x
                    for k in range(1, ITERS + 1):
                        x = b_ref[k, r + HALO, at[0], at[1]]
                        if k < ITERS:
                            best = best + w_ref[k] * x
                        rest = rest - w_ref[ITERS + k] * x
                    outs[0, r, at[0], at[1]] = best
                    outs[1, r, at[0], at[1]] = rest
            return 0

        lax.fori_loop(0, 8, one, 0)
        for q, dst in enumerate((sol_hbm, res_hbm)):
            for c in range(channels):
                copy = pltpu.make_async_copy(outs.at[q, pl.ds(8 * part, 8), c, :], dst.at[c, pl.ds(8 * part, 8), :],
                                             out_sem.at[part, q, c])
                copy.start()
                stores.append(copy)
    for copy in stores:
        copy.wait()


def solution(mesh):
    nx, ny = mesh.shape["gx"], mesh.shape["gy"]

    def per_device(forcing, damping, coupling, wind_lon, wind_lat):
        channels, lat, lon = forcing.shape
        f32 = jnp.float32
        vmem = pl.BlockSpec(memory_space=pltpu.VMEM)
        hbm = pl.BlockSpec(memory_space=pltpu.HBM)
        dma = pltpu.SemaphoreType.DMA

        def keep(v):
            return pltpu.with_memory_space_constraint(v, pltpu.HBM)

        basis, weights = pl.pallas_call(
            functools.partial(kernel, nx, ny),
            out_shape=(pltpu.VMEM((ITERS + 1, lat + 2 * HALO + 1, channels + 8, lon), f32), pltpu.VMEM((2 * ITERS + 1, 8, 128), f32)),
            in_specs=[hbm] * 5,
            out_specs=(vmem, vmem),
            scratch_shapes=[
                pltpu.VMEM((lat + 4, channels, lon), f32),
                pltpu.VMEM((lat + 4, 8, lon), f32),
                pltpu.VMEM((GROUP * channels, 3 * GROUP * channels), jnp.bfloat16),
                pltpu.VMEM((channels, 3 * channels), jnp.bfloat16),
                pltpu.VMEM((BLOCKS, 2, 2, channels, 128), f32),
                pltpu.VMEM((BLOCKS, 2, 2, channels, 128), f32),
                pltpu.VMEM((channels, 128), f32),
                pltpu.VMEM((2, channels + 8, 128), f32),
                pltpu.VMEM((2, channels + 8, 128), f32),
                pltpu.VMEM((BLOCKS, 4, 2, 128), f32),
                pltpu.VMEM((BLOCKS, 2, 128), f32),
                pltpu.VMEM((len(PAIRS), 8, 128), f32),
                pltpu.VMEM((nx * ny, 1, 128), f32),
                pltpu.VMEM((channels, channels), f32), pltpu.VMEM((lat, lon), f32), pltpu.VMEM((lat, lon), f32),
                pltpu.VMEM((2, 2, 2, lon), f32), pltpu.VMEM((2, 8, 128), f32), pltpu.VMEM((2, channels, 128), f32),
                dma((2, channels)), dma((3,)),
                dma((BLOCKS, 2, 2)), dma((BLOCKS, 2, 2)), dma((BLOCKS, 2, 2)), dma((BLOCKS, 2, 2)),
                dma((BLOCKS, 4)), dma((BLOCKS, 4)), dma((4, 2)), dma((4, 2)),
                dma((1,)), dma((1,)), pltpu.SemaphoreType.REGULAR((8,)),
            ],
            compiler_params=pltpu.CompilerParams(
                collective_id=0, has_side_effects=True, vmem_limit_bytes=24 * 1024 * 1024),
        )(*map(keep, (forcing, damping, coupling, wind_lon, wind_lat)))
        shape = jax.ShapeDtypeStruct((channels, lat, lon), f32)
        return pl.pallas_call(
            finish,
            out_shape=(shape, shape),
            in_specs=[vmem, vmem],
            out_specs=(hbm, hbm),
            scratch_shapes=[pltpu.VMEM((2, lat, channels, lon), f32), dma((lat // 8, 2, channels))],
            compiler_params=pltpu.CompilerParams(vmem_limit_bytes=24 * 1024 * 1024),
        )(basis, weights)

    return jax.shard_map(
        per_device,
        mesh=mesh,
        in_specs=(P(None, "gy", "gx"), P(None, "gy", "gx"), P(), P("gy", "gx"), P("gy", "gx")),
        out_specs=(P(None, "gy", "gx"), P(None, "gy", "gx")),
        check_vma=False,
    )
```
